32 devices in a mesh: data: 2 (over x), col: 4 (over z), row: 4 (over y, core).
Axes of the slice: x: 2, y: 2, z: 4, core: 2. Of those that a mesh axis runs over, the one named last changes fastest.
Arguments:
- image: bfloat16 [256, 128, 4], P(('data', 'row'), 'col'), parts along dimension 0
- w_enc1a: bfloat16 [3, 3, 4, 320], replicated
- b_enc1a: float32 [320], replicated
- w_enc1b: bfloat16 [3, 3, 320, 320], replicated
- b_enc1b: float32 [320], replicated
- w_enc2a: bfloat16 [3, 3, 320, 640], replicated
- b_enc2a: float32 [640], replicated
- w_enc2b: bfloat16 [3, 3, 640, 640], replicated
- b_enc2b: float32 [640], replicated
- w_mid_a: bfloat16 [3, 3, 640, 1280], replicated
- b_mid_a: float32 [1280], replicated
- w_mid_b: bfloat16 [3, 3, 1280, 1280], replicated
- b_mid_b: float32 [1280], replicated
- w_up2: bfloat16 [2, 2, 1280, 640], replicated
- w_dec2a: bfloat16 [3, 3, 1280, 640], replicated
- b_dec2a: float32 [640], replicated
- w_dec2b: bfloat16 [3, 3, 640, 640], replicated
- b_dec2b: float32 [640], replicated
- w_up1: bfloat16 [2, 2, 640, 320], replicated
- w_dec1a: bfloat16 [3, 3, 640, 320], replicated
- b_dec1a: float32 [320], replicated
- w_dec1b: bfloat16 [3, 3, 320, 320], replicated
- b_dec1b: float32 [320], replicated
- w_head: bfloat16 [320, 4], replicated
- b_head: float32 [4], replicated
Outputs:
- output: float32 [256, 128, 4], P(('data', 'row'), 'col'), parts along dimension 0
There are 2 independent parts. The reference program is written for one: setup_inputs(seed, part) draws one part's arguments, and reference() takes and returns one part's arrays. A program takes and returns all parts, laid end to end along the dimension named above; an argument that names none is the same for every part.
All inputs are finite; a program needn't handle non-finite values.
Results may differ from the reference program's by a relative error of at most 0.0170829.
Values are sent between devices in bfloat16 or wider.
A program may use at most 1 GiB of HBM per device.

```python
import jax
import jax.numpy as jnp
from jax import lax

IN_CH = 4
BASE_CH = 320
OUT_CH = 4
IMG_ROWS = 128
IMG_COLS = 128


def weight_specs():
    ch_one = BASE_CH
    ch_two = 2 * BASE_CH
    ch_four = 4 * BASE_CH
    bias_gain = 0.0625
    return [
        ("w_enc1a", (3, 3, IN_CH, ch_one), 9 * IN_CH, 2.0, jnp.bfloat16),
        ("b_enc1a", (ch_one,), 1, bias_gain, jnp.float32),
        ("w_enc1b", (3, 3, ch_one, ch_one), 9 * ch_one, 2.0, jnp.bfloat16),
        ("b_enc1b", (ch_one,), 1, bias_gain, jnp.float32),
        ("w_enc2a", (3, 3, ch_one, ch_two), 9 * ch_one, 2.0, jnp.bfloat16),
        ("b_enc2a", (ch_two,), 1, bias_gain, jnp.float32),
        ("w_enc2b", (3, 3, ch_two, ch_two), 9 * ch_two, 2.0, jnp.bfloat16),
        ("b_enc2b", (ch_two,), 1, bias_gain, jnp.float32),
        ("w_mid_a", (3, 3, ch_two, ch_four), 9 * ch_two, 2.0, jnp.bfloat16),
        ("b_mid_a", (ch_four,), 1, bias_gain, jnp.float32),
        ("w_mid_b", (3, 3, ch_four, ch_four), 9 * ch_four, 2.0, jnp.bfloat16),
        ("b_mid_b", (ch_four,), 1, bias_gain, jnp.float32),
        ("w_up2", (2, 2, ch_four, ch_two), ch_four, 1.0, jnp.bfloat16),
        ("w_dec2a", (3, 3, ch_four, ch_two), 9 * ch_four, 2.0, jnp.bfloat16),
        ("b_dec2a", (ch_two,), 1, bias_gain, jnp.float32),
        ("w_dec2b", (3, 3, ch_two, ch_two), 9 * ch_two, 2.0, jnp.bfloat16),
        ("b_dec2b", (ch_two,), 1, bias_gain, jnp.float32),
        ("w_up1", (2, 2, ch_two, ch_one), ch_two, 1.0, jnp.bfloat16),
        ("w_dec1a", (3, 3, ch_two, ch_one), 9 * ch_two, 2.0, jnp.bfloat16),
        ("b_dec1a", (ch_one,), 1, bias_gain, jnp.float32),
        ("w_dec1b", (3, 3, ch_one, ch_one), 9 * ch_one, 2.0, jnp.bfloat16),
        ("b_dec1b", (ch_one,), 1, bias_gain, jnp.float32),
        ("w_head", (ch_one, OUT_CH), ch_one, 1.0, jnp.bfloat16),
        ("b_head", (OUT_CH,), 1, bias_gain, jnp.float32),
    ]


def setup_inputs(seed: int = 0, part: int = 0) -> dict:
    root = jax.random.key(seed)
    image_key = jax.random.fold_in(jax.random.fold_in(root, 1000), part)
    pixels = jax.random.normal(image_key, (IMG_ROWS, IMG_COLS, IN_CH), jnp.float32)
    result = {"image": pixels.astype(jnp.bfloat16)}
    for index, spec in enumerate(weight_specs()):
        name, shape, fan_in, gain, dtype = spec
        values = jax.random.normal(jax.random.fold_in(root, index), shape, jnp.float32)
        result[name] = (values * (gain / fan_in) ** 0.5).astype(dtype)
    return result


def conv_relu(hidden, weight, bias):
    conv_out = lax.conv_general_dilated(hidden.astype(jnp.float32)[None], weight.astype(jnp.float32), (1, 1), "SAME", dimension_numbers=("NHWC", "HWIO", "NHWC"))[0]
    return jax.nn.relu(conv_out + bias).astype(jnp.bfloat16)


def double_conv(hidden, w_first, b_first, w_second, b_second):
    return conv_relu(conv_relu(hidden, w_first, b_first), w_second, b_second)


def max_pool(hidden):
    height, width, channels = hidden.shape
    return hidden.reshape(height // 2, 2, width // 2, 2, channels).max(axis=(1, 3))


def up_conv(hidden, weight):
    height = hidden.shape[0]
    width = hidden.shape[1]
    summed = jnp.einsum("ijc,abco->iajbo", hidden.astype(jnp.float32), weight.astype(jnp.float32))
    return summed.astype(jnp.bfloat16).reshape(2 * height, 2 * width, weight.shape[3])


def reference(image, w_enc1a, b_enc1a, w_enc1b, b_enc1b, w_enc2a, b_enc2a, w_enc2b, b_enc2b, w_mid_a, b_mid_a, w_mid_b, b_mid_b, w_up2, w_dec2a, b_dec2a, w_dec2b, b_dec2b, w_up1, w_dec1a, b_dec1a, w_dec1b, b_dec1b, w_head, b_head):
    skip_one = double_conv(image, w_enc1a, b_enc1a, w_enc1b, b_enc1b)
    skip_two = double_conv(max_pool(skip_one), w_enc2a, b_enc2a, w_enc2b, b_enc2b)
    middle = double_conv(max_pool(skip_two), w_mid_a, b_mid_a, w_mid_b, b_mid_b)
    hidden = double_conv(jnp.concatenate([up_conv(middle, w_up2), skip_two], axis=2), w_dec2a, b_dec2a, w_dec2b, b_dec2b)
    hidden = double_conv(jnp.concatenate([up_conv(hidden, w_up1), skip_one], axis=2), w_dec1a, b_dec1a, w_dec1b, b_dec1b)
    flat = hidden.reshape(-1, hidden.shape[2])
    head_out = jnp.dot(flat, w_head, preferred_element_type=jnp.float32) + b_head
    return head_out.reshape(hidden.shape[0], hidden.shape[1], w_head.shape[1])
```

```python
import jax
import jax.numpy as jnp
from jax import lax
from jax.experimental import pallas as pl
from jax.experimental.pallas import tpu as pltpu
from jax.sharding import PartitionSpec as P

F32 = jnp.float32
BF16 = jnp.bfloat16
STRIPS = 16
LAST = STRIPS - 1
SIDE = 4
SUB, LANE = 8, 128
TILE, HALF = 2 * LANE, LANE // 2
C1, C2, C3, C1P = 320, 640, 1280, 384
W3 = 32
END = SUB + TILE
MARGIN = END + SUB
TAPS = range(3)
TAP9 = 9
A_D2A = 17
A_REFILL = 27
A_D2B = 35
A_END = 44
B_END = 27
NOT = jnp.logical_not
AND = jnp.logical_and
OR = jnp.logical_or
RING_A = 18
RING_B = 10
MESH_ID = pl.DeviceIdType.MESH


def dot(lhs, rhs):
    return jnp.dot(lhs, rhs, preferred_element_type=F32)


def sum_of(parts):
    first, *rest = parts
    for part in rest:
        first = first + part
    return first


def relu(value):
    return jnp.maximum(value, 0.0)


def lane_mask(shape, below):
    return lax.broadcasted_iota(jnp.int32, shape, 1) < below


def column_index(rows, width):
    return lax.rem(lax.broadcasted_iota(jnp.int32, (rows, LANE), 0), width)


def kernel(x_ref, w_e1a, bias, w_head, h_e1b, h_e2a, h_e2b, h_ma, h_mb, h_up2, h_d2a, h_d2b, h_up1, h_d1a, h_d1b,
           out_ref,
           xb, xh, z, act1, s1, p1, act2, s2, p2, act3, mid, u2, act4, d2, u1, act5,
           v_e1b, v_d1a, v_d1b, v_up1, v_e2a, t_e1b, t_d1a, t_d1b, ring_a, ring_b,
           pm, pt, pl2, pl3, pool, up_f32, ys, ysend, yrecv,
           sem_w, sem_a, sem_b, x_send, x_recv, h_send, h_recv, e_send, e_recv, y_send, y_recv):
    col = lax.axis_index("col")
    row = lax.axis_index("row")
    data = lax.axis_index("data")

    def owner(strip):
        strip_col = strip // 4
        k = strip % 4
        return strip_col, k + (strip_col % 2) * (3 - 2 * k)

    def device(strip_col, strip_row):
        return (data, strip_col, strip_row)

    k_me = row + (col % 2) * (3 - 2 * row)
    me = 4 * col + k_me

    def whole(src, dst, index):
        return pltpu.make_async_copy(src, dst, sem_w.at[index])

    cp_e1b = whole(h_e1b, v_e1b, 0)
    cp_e2a = whole(h_e2a, v_e2a, 1)
    cp_up1 = whole(h_up1, v_up1, 2)
    cp_d1a = whole(h_d1a, v_d1a, 3)
    cp_d1b = whole(h_d1b, v_d1b, 4)

    def unit_a(unit):
        slot = unit % RING_A
        if unit < TAP9:
            src = h_e2b.at[unit]
        elif unit < A_D2A:
            src = h_up2.at[(unit - TAP9) // 2, pl.ds(((unit - TAP9) % 2) * C2, C2)]
        elif unit < A_D2B:
            local = unit - A_D2A
            dx, rest = local // 6, local % 6
            src = h_d2a.at[(rest // 2) * 3 + dx, pl.ds((rest % 2) * C2, C2)]
        else:
            local = unit - A_D2B
            src = h_d2b.at[(local % 3) * 3 + local // 3]
        return pltpu.make_async_copy(src, ring_a.at[slot], sem_a.at[slot])

    def wait_a(unit):
        slot = unit % RING_A
        pltpu.make_async_copy(h_e2b.at[0], ring_a.at[slot], sem_a.at[slot]).wait()

    def unit_b(unit):
        slot = unit % RING_B
        if unit < TAP9:
            src = h_ma.at[unit]
        else:
            local = unit - TAP9
            order = (3, 4, 5, 0, 1, 2, 6, 7, SUB)[local // 2]
            src = h_mb.at[order, pl.ds((local % 2) * C2, C2)]
        return pltpu.make_async_copy(src, ring_b.at[slot], sem_b.at[slot])

    def wait_b(unit):
        slot = unit % RING_B
        pltpu.make_async_copy(h_ma.at[0], ring_b.at[slot], sem_b.at[slot]).wait()

    cp_e1b.start()
    cp_e2a.start()
    for unit in range(TAP9):
        unit_a(unit).start()
    for unit in range(RING_B):
        unit_b(unit).start()
    for unit in range(TAP9, RING_A):
        unit_a(unit).start()

    barrier = pltpu.get_barrier_semaphore()
    for strip in range(1, STRIPS):
        other = (me + strip) % STRIPS
        other_col, other_row = owner(other)
        pl.semaphore_signal(barrier, inc=1, device_id=device(other_col, other_row), device_id_type=MESH_ID)
    pl.semaphore_wait(barrier, LAST)

    def is_me(strip_col, strip_row):
        return AND(strip_col == col, strip_row == row)

    def remote(src, dst, send, recv, strip_col, strip_row):
        return pltpu.make_async_remote_copy(src_ref=src, dst_ref=dst, send_sem=send, recv_sem=recv,
                                            device_id=device(strip_col, strip_row), device_id_type=MESH_ID)

    for k in range(SIDE):
        to_col, to_row = owner(4 * row + k)
        here = is_me(to_col, to_row)
        copy = remote(x_ref.at[pl.ds(SUB * k, STRIPS)], xb.at[col], x_send.at[k], x_recv.at[col], to_col, to_row)

        @pl.when(NOT(here))
        def _():
            copy.start()

        @pl.when(here)
        def _():
            xb[pl.ds(col, 1)] = x_ref[SUB * k:SUB * k + STRIPS][None]

    def halo_target(strip):
        return owner(jnp.clip(strip, 0, LAST))

    for side, (strip, allowed, first) in enumerate(((4 * row - 1, row > 0, 0), (4 * row + 4, row < 3, W3))):
        to_col, to_row = halo_target(strip)
        here = is_me(to_col, to_row)
        copy = remote(x_ref.at[pl.ds(first, SUB)], xh.at[col], h_send.at[side], h_recv.at[col], to_col, to_row)

        @pl.when(AND(allowed, NOT(here)))
        def _():
            copy.start()

        @pl.when(AND(allowed, here))
        def _():
            xh[pl.ds(col, 1)] = x_ref[first:first + SUB][None]

    for c in range(SIDE):
        @pl.when(NOT(is_me(c, row) & (row == col)))
        def _():
            remote(x_ref.at[pl.ds(0, STRIPS)], xb.at[c], x_send.at[0], x_recv.at[c], col, row).wait_recv()

    has_top = AND(k_me == 0, col > 0)
    has_bottom = AND(k_me == 3, col < 3)
    halo_row = jnp.where(has_top, col - 1, col + 1)
    for c in range(SIDE):
        own = AND(c == col, row == halo_row)

        @pl.when(AND(OR(has_top, has_bottom), NOT(own)))
        def _():
            remote(x_ref.at[pl.ds(0, SUB)], xh.at[c], h_send.at[0], h_recv.at[c], col, row).wait_recv()

    for k in range(SIDE):
        to_col, to_row = owner(4 * row + k)

        @pl.when(NOT(is_me(to_col, to_row)))
        def _():
            remote(x_ref.at[pl.ds(SUB * k, STRIPS)], xb.at[col], x_send.at[k], x_recv.at[col], to_col, to_row).wait_send()

    for side, (strip, allowed, first) in enumerate(((4 * row - 1, row > 0, 0), (4 * row + 4, row < 3, W3))):
        to_col, to_row = halo_target(strip)

        @pl.when(AND(allowed, NOT(is_me(to_col, to_row))))
        def _():
            remote(x_ref.at[pl.ds(first, SUB)], xh.at[col], h_send.at[side], h_recv.at[col], to_col, to_row).wait_send()

    lanes16 = lax.broadcasted_iota(jnp.int32, (STRIPS, LANE), 1)
    rows16 = lax.broadcasted_iota(jnp.int32, (STRIPS, LANE), 0)
    planes = [jnp.zeros((STRIPS, LANE), F32) for _ in range(SIDE)]
    for c in range(SIDE):
        halo = xh[c]
        both = jnp.concatenate([halo, halo], axis=0)
        top_rows = AND(has_top, rows16 < 2)
        bottom_rows = AND(has_bottom, AND(rows16 >= 10, rows16 < 12))
        block = jnp.where(OR(top_rows, bottom_rows), both, xb[c])
        inside = AND(lanes16 >= W3 * c, lanes16 < W3 * c + W3)
        for channel in range(SIDE):
            shift = (W3 * c - W3 * channel) % LANE
            moved = block if shift == 0 else pltpu.roll(block, shift, 1)
            planes[channel] = jnp.where(inside, moved, planes[channel])
    z[...] = jnp.zeros_like(z)
    for dx in TAPS:
        for channel in range(SIDE):
            plane = planes[channel]
            if dx == 0:
                plane = jnp.where(lanes16 == 0, 0.0, pltpu.roll(plane, 1, 1))
            elif dx == 2:
                plane = jnp.where(lanes16 == 127, 0.0, pltpu.roll(plane, 127, 1))
            z[pl.ds(dx * 4 + channel, STRIPS, stride=STRIPS), :] = plane

    def first_conv(j, carry):
        start = pl.multiple_of(j * STRIPS, STRIPS)
        taps = z[pl.ds(start, 48), :].astype(BF16)
        value = lax.dot_general(taps, w_e1a[...], (((0,), (0,)), ((), ())), preferred_element_type=F32)
        value = relu(value + bias[:1, :C1P])
        outside = OR(AND(me == 0, j == 0), AND(me == LAST, j == 9))
        value = jnp.where(outside, 0.0, value)
        act1[pl.ds(pl.multiple_of(j * LANE, LANE), LANE), :] = value.astype(BF16)
        return carry

    lax.fori_loop(0, 10, first_conv, 0)

    up_col, up_row = owner(jnp.maximum(me - 1, 0))
    down_col, down_row = owner(jnp.minimum(me + 1, LAST))

    def halo_copies(ref, width, height, index):
        to_up = remote(ref.at[pl.ds(width, width)], ref.at[pl.ds((height + 1) * width, width)],
                       e_send.at[index, 0], e_recv.at[index, 0], up_col, up_row)
        to_down = remote(ref.at[pl.ds(height * width, width)], ref.at[pl.ds(0, width)],
                         e_send.at[index, 1], e_recv.at[index, 1], down_col, down_row)
        return to_up, to_down

    def halo_start(ref, width, height, index):
        to_up, to_down = halo_copies(ref, width, height, index)

        @pl.when(me > 0)
        def _():
            to_up.start()

        @pl.when(me < LAST)
        def _():
            to_down.start()

        @pl.when(me == 0)
        def _():
            ref[:width, :] = jnp.zeros((width, ref.shape[1]), BF16)

        @pl.when(me == LAST)
        def _():
            ref[(height + 1) * width:(height + 2) * width, :] = jnp.zeros((width, ref.shape[1]), BF16)

    def halo_wait(ref, width, height, index):
        to_up, to_down = halo_copies(ref, width, height, index)

        @pl.when(me > 0)
        def _():
            to_down.wait_recv()
            to_up.wait_send()

        @pl.when(me < LAST)
        def _():
            to_up.wait_recv()
            to_down.wait_send()

    def build_tail(weights, base, tail):
        def body(dy, carry):
            parts = [weights[dy * 3 + dx, base:base + C1, TILE:C1].astype(F32) for dx in TAPS]
            zero = jnp.zeros((C1, HALF), F32)
            pair = jnp.concatenate([parts[0], parts[1]], axis=1)
            last = jnp.concatenate([parts[2], zero], axis=1)
            tail[dy, :, :LANE] = pair.astype(BF16)
            tail[dy, :, LANE:TILE] = last.astype(BF16)
            return carry

        lax.fori_loop(0, 3, body, 0)

    def narrow_lhs(ref, start, rows, width):
        mains = [ref[pl.ds(start + dy * width, rows), :TILE] for dy in TAPS]
        tails = [ref[pl.ds(start + dy * width, rows), TILE:C1P] for dy in TAPS]
        pair = (tails[0].astype(F32) + pltpu.roll(tails[1].astype(F32), HALF, 1)).astype(BF16)
        return jnp.concatenate(mains + [pair, tails[2][:, :HALF]], axis=1)

    def narrow_rhs(load):
        return jnp.concatenate([load(dy, 0, TILE) for dy in TAPS] + [load(dy, TILE, C1) for dy in TAPS], axis=0)

    x_index = column_index(TILE, LANE)
    not_first = x_index > 0
    not_last = x_index < 127

    def conv_level1(blocks, bias_row, finish):
        def chunk(i, carry):
            start = pl.multiple_of(i * TILE, TILE)
            lefts = [narrow_lhs(ref, start, TILE, LANE) for ref, _, _, _ in blocks]
            for dx in TAPS:
                pm[dx, SUB:END, :] = sum_of(
                    dot(left, narrow_rhs(lambda dy, a, b: weights[dy * 3 + dx, base + a:base + b, :TILE]))
                    for left, (_, weights, base, _) in zip(lefts, blocks))
            pt[SUB:END, :] = sum_of(dot(left, narrow_rhs(lambda dy, a, b: tail[dy, a:b, :]))
                                    for left, (_, _, _, tail) in zip(lefts, blocks))
            pieces = []
            for block in range(2):
                lanes = slice(block * LANE, block * LANE + LANE)
                value = pm[1, SUB:END, lanes] + jnp.where(not_first, pm[0, 7:263, lanes], 0.0)
                value = value + jnp.where(not_last, pm[2, 9:265, lanes], 0.0)
                pieces.append(relu(value + bias[bias_row:bias_row + 1, lanes]))
            value = pltpu.roll(pt[SUB:END, :LANE], HALF, 1) + jnp.where(not_first, pt[7:263, :LANE], 0.0)
            value = value + jnp.where(not_last, pt[9:265, LANE:TILE], 0.0)
            value = relu(value + bias[bias_row:bias_row + 1, TILE:C1P])
            pieces.append(jnp.where(lane_mask((TILE, LANE), HALF), value, 0.0))
            finish(i, pieces)
            return carry

        lax.fori_loop(0, 4, chunk, 0)

    def store_level1(ref):
        def finish(i, pieces):
            start = pl.multiple_of(LANE + i * TILE, LANE)
            for block in range(3):
                ref[pl.ds(start, TILE), block * LANE:block * LANE + LANE] = pieces[block].astype(BF16)
        return finish

    def finish_s1(i, pieces):
        store_level1(s1)(i, pieces)
        start = pl.multiple_of(HALF + i * HALF, HALF)
        for block in range(3):
            pool[:LANE, :] = jnp.maximum(pieces[block][:LANE], pieces[block][LANE:TILE])
            pooled = jnp.maximum(pool[pl.ds(0, HALF, stride=2), :], pool[pl.ds(1, HALF, stride=2), :])
            p1[pl.ds(start, HALF), block * LANE:block * LANE + LANE] = pooled.astype(BF16)

    cp_e1b.wait()
    build_tail(v_e1b, 0, t_e1b)
    conv_level1([(act1, v_e1b, 0, t_e1b)], 1, finish_s1)
    halo_start(p1, HALF, 4, 0)
    halo_start(s1, LANE, SUB, 1)

    x_index2 = column_index(TILE, HALF)
    not_first2 = x_index2 > 0
    not_last2 = x_index2 < 63

    def finish_level2(bias_row, store):
        def body(block, carry):
            lanes = pl.ds(pl.multiple_of(block * LANE, LANE), LANE)
            value = pl2[1, SUB:END, lanes] + jnp.where(not_first2, pl2[0, 7:263, lanes], 0.0)
            value = value + jnp.where(not_last2, pl2[2, 9:265, lanes], 0.0)
            store(lanes, relu(value + bias[bias_row:bias_row + 1, lanes]))
            return carry

        lax.fori_loop(0, 5, body, 0)

    def store_level2(ref, start):
        def store(lanes, value):
            ref[start:start + TILE, lanes] = value.astype(BF16)
        return store

    def store_s2(lanes, value):
        s2[HALF:C1, lanes] = value.astype(BF16)
        for i in range(2):
            pool[:HALF, :] = jnp.maximum(value[LANE * i:LANE * i + HALF], value[LANE * i + HALF:LANE * i + LANE])
            pooled = jnp.maximum(pool[pl.ds(0, W3, stride=2), :], pool[pl.ds(1, W3, stride=2), :])
            p2[W3 + W3 * i:HALF + W3 * i, lanes] = pooled.astype(BF16)

    NTILES = ((0, TILE), (TILE, 512), (512, C2))

    def stack_rows(ref, rows, width):
        return jnp.concatenate([ref[dy * width:dy * width + rows, :] for dy in TAPS], axis=1)

    halo_wait(p1, HALF, 4, 0)
    cp_e2a.wait()

    def enc2a(dx, carry):
        left = narrow_lhs(p1, 0, TILE, HALF)
        for a, b in NTILES:
            right = narrow_rhs(lambda dy, r0, r1: v_e2a[dy * 3 + dx, r0:r1, a:b])
            pl2[dx, SUB:END, a:b] = dot(left, right)
        return carry

    lax.fori_loop(0, 3, enc2a, 0)
    finish_level2(2, store_level2(act2, HALF))
    halo_start(act2, HALF, 4, 2)

    for unit in range(TAP9):
        wait_a(unit)
    halo_wait(act2, HALF, 4, 2)

    def conv640(ref, slots):
        def body(dx, carry):
            left = stack_rows(ref, TILE, HALF)
            picks = slots(dx)
            for a, b in NTILES:
                right = jnp.concatenate([ring_a[pick, :, a:b] for pick in picks], axis=0)
                pl2[dx, SUB:END, a:b] = dot(left, right)
            return carry

        lax.fori_loop(0, 3, body, 0)

    conv640(act2, lambda dx: [dy * 3 + dx for dy in TAPS])
    finish_level2(3, store_s2)
    halo_start(p2, W3, 2, 3)
    halo_start(s2, HALF, 4, 4)
    for unit in range(RING_A, A_REFILL):
        unit_a(unit).start()

    x_index3 = column_index(HALF, W3)
    not_first3 = x_index3 > 0
    not_last3 = x_index3 < 31

    def finish_level3(bias_row, ref, start):
        def body(block, carry):
            lanes = pl.ds(pl.multiple_of(block * LANE, LANE), LANE)
            value = pl3[1, SUB:72, lanes] + jnp.where(not_first3, pl3[0, 7:71, lanes], 0.0)
            value = value + jnp.where(not_last3, pl3[2, 9:73, lanes], 0.0)
            ref[start:start + HALF, lanes] = relu(value + bias[bias_row:bias_row + 1, lanes]).astype(BF16)
            return carry

        lax.fori_loop(0, 10, body, 0)

    for unit in range(TAP9):
        wait_b(unit)
    halo_wait(p2, W3, 2, 3)

    def mid_a(dx, carry):
        left = stack_rows(p2, HALF, W3)
        for n in range(5):
            right = jnp.concatenate([ring_b[dy * 3 + dx, :, n * TILE:n * TILE + TILE] for dy in TAPS], axis=0)
            pl3[dx, SUB:72, n * TILE:n * TILE + TILE] = dot(left, right)
        return carry

    lax.fori_loop(0, 3, mid_a, 0)
    finish_level3(4, act3, W3)
    halo_start(act3, W3, 2, 5)
    for unit in range(RING_B, RING_B + TAP9):
        unit_b(unit).start()
    cp_up1.start()
    cp_d1a.start()
    cp_d1b.start()
    halo_wait(act3, W3, 2, 5)

    def mid_b_tap(tap):
        dy = (1, 0, 2)[tap // 3]
        dx = tap % 3
        first = 9 + 2 * tap
        wait_b(first)
        wait_b(first + 1)
        left = act3[dy * W3:dy * W3 + HALF, :]

        def body(n, carry):
            lanes = pl.ds(pl.multiple_of(n * TILE, TILE), TILE)
            right = jnp.concatenate([ring_b[(first + half) % RING_B, :, lanes] for half in range(2)], axis=0)
            part = dot(left, right)
            if tap < 3:
                pl3[dx, SUB:72, lanes] = part
            else:
                pl3[dx, SUB:72, lanes] = pl3[dx, SUB:72, lanes] + part
            return carry

        lax.fori_loop(0, 5, body, 0)
        for unit in (first + RING_B, first + 1 + RING_B):
            if RING_B + TAP9 <= unit < B_END:
                unit_b(unit).start()

    for tap in range(TAP9):
        mid_b_tap(tap)
    finish_level3(5, mid, 0)

    for unit in range(TAP9, A_D2A):
        wait_a(unit)
    for tap in range(SIDE):
        p, q = tap // 2, tap % 2
        left = mid[...]
        for a, b in NTILES:
            right = jnp.concatenate([ring_a[(9 + 2 * tap + half) % RING_A, :, a:b] for half in range(2)], axis=0)
            part = dot(left, right)
            for i in range(2):
                for c0 in range(a, b, LANE):
                    up_f32[pl.ds(c0 * 2 + (2 * i + p) * HALF + q, W3, stride=2), :] = part[W3 * i:W3 * i + W3, c0 - a:c0 - a + LANE]
    for block in range(5):
        u2[HALF:C1, block * LANE:block * LANE + LANE] = up_f32[block * TILE:block * TILE + TILE, :].astype(BF16)
    halo_start(u2, HALF, 4, 6)
    for unit in range(A_REFILL, A_D2B):
        unit_a(unit).start()
    halo_wait(s2, HALF, 4, 4)
    halo_wait(u2, HALF, 4, 6)
    for unit in range(A_D2A, A_D2B):
        wait_a(unit)

    def dec2a(dx, carry):
        lefts = [stack_rows(u2, TILE, HALF), stack_rows(s2, TILE, HALF)]
        for a, b in NTILES:
            pl2[dx, SUB:END, a:b] = sum_of(
                dot(left, jnp.concatenate([ring_a[lax.rem(A_D2A + dx * 6 + dy * 2 + half, RING_A), :, a:b] for dy in TAPS], axis=0))
                for half, left in enumerate(lefts))
        return carry

    lax.fori_loop(0, 3, dec2a, 0)
    for unit in range(A_D2B, A_END):
        unit_a(unit).start()
    finish_level2(6, store_level2(act4, HALF))
    halo_start(act4, HALF, 4, 7)
    for unit in range(A_D2B, A_END):
        wait_a(unit)
    halo_wait(act4, HALF, 4, 7)
    conv640(act4, lambda dx: [lax.rem(A_D2B + dx * 3 + dy, RING_A) for dy in TAPS])
    finish_level2(7, store_level2(d2, 0))

    cp_up1.wait()
    for tap in range(SIDE):
        p, q = tap // 2, tap % 2
        left = d2[...]
        for a, b in ((0, TILE), (TILE, C1)):
            part = dot(left, v_up1[tap, :, a:b])
            for i in range(SIDE):
                for c0 in range(a, b, LANE):
                    c1 = min(b, c0 + LANE)
                    up_f32[pl.ds(c0 * SUB + (2 * i + p) * LANE + q, HALF, stride=2), :c1 - c0] = part[HALF * i:HALF * i + HALF, c0 - a:c1 - a]
    for block in range(3):
        value = up_f32[block * 1024:block * 1024 + 1024, :]
        if block == 2:
            value = jnp.where(lane_mask((1024, LANE), HALF), value, 0.0)
        u1[LANE:1152, block * LANE:block * LANE + LANE] = value.astype(BF16)
    halo_start(u1, LANE, SUB, SUB)
    cp_d1a.wait()
    build_tail(v_d1a, 0, t_d1a.at[0])
    build_tail(v_d1a, C1, t_d1a.at[1])
    halo_wait(s1, LANE, SUB, 1)
    halo_wait(u1, LANE, SUB, SUB)
    conv_level1([(u1, v_d1a, 0, t_d1a.at[0]), (s1, v_d1a, C1, t_d1a.at[1])], SUB, store_level1(act5))
    halo_start(act5, LANE, SUB, 9)
    cp_d1b.wait()
    build_tail(v_d1b, 0, t_d1b)
    halo_wait(act5, LANE, SUB, 9)

    def finish_head(i, pieces):
        value = jnp.concatenate([piece.astype(BF16) for piece in pieces], axis=1)
        head = lax.dot_general(w_head[...], value, (((1,), (1,)), ((), ())), preferred_element_type=F32)
        ys[pl.ds(i, 1)] = head[None]

    conv_level1([(act5, v_d1b, 0, t_d1b)], 9, finish_head)

    lanes8 = lax.broadcasted_iota(jnp.int32, (SUB, LANE), 1)
    sub8 = lax.broadcasted_iota(jnp.int32, (SUB, LANE), 0)
    for c in range(SIDE):
        packed = jnp.zeros((SUB, LANE), F32)
        for y in range(SUB):
            line = ys[y // 2, :, (y % 2) * LANE:(y % 2) * LANE + LANE]
            slot = y % 4
            shift = (W3 * slot - W3 * c) % LANE
            line = line if shift == 0 else pltpu.roll(line, shift, 1)
            if y >= 4:
                line = pltpu.roll(line, 4, 0)
            place = AND(AND(lanes8 >= W3 * slot, lanes8 < W3 * slot + W3), (sub8 >= 4) if y >= 4 else (sub8 < 4))
            packed = jnp.where(place, line, packed)
        ysend[c] = packed

    def y_copy(c):
        return remote(ysend.at[c], yrecv.at[k_me], y_send.at[c], y_recv.at[k_me], c, col)

    for c in range(SIDE):
        here = is_me(c, col)

        @pl.when(NOT(here))
        def _():
            y_copy(c).start()

        @pl.when(here)
        def _():
            yrecv[pl.ds(k_me, 1)] = ysend[c][None]

    for k in range(SIDE):
        from_col, from_row = owner(4 * row + k)

        @pl.when(NOT(is_me(from_col, from_row)))
        def _():
            remote(ysend.at[0], yrecv.at[k], y_send.at[0], y_recv.at[k], col, row).wait_recv()

    for c in range(SIDE):
        @pl.when(NOT(is_me(c, col)))
        def _():
            y_copy(c).wait_send()

    out_ref[...] = yrecv[...]


def network(x, w_e1a, bias, w_head, *weights):
    vmem = pl.BlockSpec(memory_space=pltpu.VMEM)
    hbm = pl.BlockSpec(memory_space=pl.ANY)
    dma = pltpu.SemaphoreType.DMA
    scratch = [
        pltpu.VMEM((4, STRIPS, LANE), F32), pltpu.VMEM((4, SUB, LANE), F32), pltpu.VMEM((TILE, LANE), F32),
        pltpu.VMEM((C3, C1P), BF16), pltpu.VMEM((C3, C1P), BF16), pltpu.VMEM((C1P, C1P), BF16),
        pltpu.VMEM((C1P, C2), BF16), pltpu.VMEM((C1P, C2), BF16), pltpu.VMEM((LANE, C2), BF16),
        pltpu.VMEM((LANE, C3), BF16), pltpu.VMEM((HALF, C3), BF16), pltpu.VMEM((C1P, C2), BF16),
        pltpu.VMEM((C1P, C2), BF16), pltpu.VMEM((TILE, C2), BF16), pltpu.VMEM((C3, C1P), BF16), pltpu.VMEM((C3, C1P), BF16),
        pltpu.VMEM((9, C1, C1), BF16), pltpu.VMEM((9, C2, C1), BF16), pltpu.VMEM((9, C1, C1), BF16),
        pltpu.VMEM((4, C2, C1), BF16), pltpu.VMEM((9, C1, C2), BF16),
        pltpu.VMEM((3, C1, TILE), BF16), pltpu.VMEM((2, 3, C1, TILE), BF16), pltpu.VMEM((3, C1, TILE), BF16),
        pltpu.VMEM((RING_A, C2, C2), BF16), pltpu.VMEM((RING_B, C2, C3), BF16),
        pltpu.VMEM((3, MARGIN, TILE), F32), pltpu.VMEM((MARGIN, TILE), F32), pltpu.VMEM((3, MARGIN, C2), F32), pltpu.VMEM((3, 80, C3), F32),
        pltpu.VMEM((LANE, LANE), F32), pltpu.VMEM((3072, LANE), F32), pltpu.VMEM((4, SUB, TILE), F32),
        pltpu.VMEM((4, SUB, LANE), F32), pltpu.VMEM((4, SUB, LANE), F32),
        dma((5,)), dma((RING_A,)), dma((RING_B,)), dma((4,)), dma((4,)), dma((2,)), dma((4,)),
        dma((10, 2)), dma((10, 2)), dma((4,)), dma((4,)),
    ]
    return pl.pallas_call(
        kernel,
        out_shape=jax.ShapeDtypeStruct((4, SUB, LANE), F32),
        in_specs=[vmem] * 4 + [hbm] * 11,
        out_specs=vmem,
        scratch_shapes=scratch,
        compiler_params=pltpu.CompilerParams(collective_id=0, has_side_effects=True, vmem_limit_bytes=66 * 1000 * 1000),
        name="unet",
    )(x, w_e1a, bias, w_head, *weights)


def solution(mesh):
    tile_spec = P(("data", "row"), "col", None)

    def device_body(tile, *params):
        (w_enc1a, b_enc1a, w_enc1b, b_enc1b, w_enc2a, b_enc2a, w_enc2b, b_enc2b,
         w_mid_a, b_mid_a, w_mid_b, b_mid_b, w_up2, w_dec2a, b_dec2a, w_dec2b, b_dec2b,
         w_up1, w_dec1a, b_dec1a, w_dec1b, b_dec1b, w_head, b_head) = params
        x = jnp.transpose(tile, (0, 2, 1)).reshape(W3, LANE).astype(F32)
        x = jnp.pad(x, ((2, 6), (0, 0)))
        first = jnp.pad(w_enc1a.reshape(3, 12, C1), ((0, 0), (0, 4), (0, HALF))).reshape(48, C1P)
        biases = (b_enc1a, b_enc1b, b_enc2a, b_enc2b, b_mid_a, b_mid_b, b_dec2a, b_dec2b, b_dec1a, b_dec1b)
        bias = jnp.stack([jnp.pad(b, (0, C3 - b.shape[0])) for b in biases])
        head = jnp.pad(w_head.T, ((0, 4), (0, HALF)))

        def taps(weight):
            return weight.reshape(-1, weight.shape[2], weight.shape[3])

        weights = [taps(w) for w in (w_enc1b, w_enc2a, w_enc2b, w_mid_a, w_mid_b, w_up2, w_dec2a, w_dec2b, w_up1, w_dec1a, w_dec1b)]
        packed = network(x, first, bias, head, *weights)
        out = packed.reshape(4, 2, 4, 4, W3).transpose(0, 1, 3, 4, 2).reshape(W3, W3, 4)
        return out + b_head

    def program(image, *params):
        mapped = jax.shard_map(device_body, mesh=mesh, in_specs=(tile_spec,) + tuple([P()] * len(params)), out_specs=tile_spec, check_vma=False)
        return mapped(image, *params)

    return program
```

```python
import jax
import jax.numpy as jnp
from jax import lax
from jax.experimental import pallas as pl
from jax.experimental.pallas import tpu as pltpu
from jax.sharding import PartitionSpec as P

F32 = jnp.float32
BF16 = jnp.bfloat16
STRIPS = 16
LAST = STRIPS - 1
SIDE = 4
SUB, LANE = 8, 128
TILE, HALF = 2 * LANE, LANE // 2
C1, C2, C3, C1P = 320, 640, 1280, 384
W3 = 32
END = SUB + TILE
MARGIN = END + SUB
TAPS = range(3)
TAP9 = 9
RING = 50
E2B, MA, MB, UP2, D2A, D2B, UP1, D1A, UNITS = 0, 9, 27, 63, 71, 89, 98, 100, 105
ROWS = (1, 0, 2)
NOT = jnp.logical_not
AND = jnp.logical_and
OR = jnp.logical_or
MESH_ID = pl.DeviceIdType.MESH


def dot(lhs, rhs):
    return jnp.dot(lhs, rhs, preferred_element_type=F32)


def sum_of(parts):
    first, *rest = parts
    for part in rest:
        first = first + part
    return first


def relu(value):
    return jnp.maximum(value, 0.0)


def lane_mask(shape, below):
    return lax.broadcasted_iota(jnp.int32, shape, 1) < below


def column_index(rows, width):
    return lax.rem(lax.broadcasted_iota(jnp.int32, (rows, LANE), 0), width)


def kernel(x_ref, w_e1a, w_head, *refs):
    biases, refs = refs[:10], refs[10:]
    (h_e1b, h_e2a, h_e2b, h_ma, h_mb, h_up2, h_d2a, h_d2b, h_up1, h_d1a, h_d1b,
     out_ref,
     xb, xh, z, act1, cat1, p1, act2, s2, p2, act3, mid, u2, act4, d2, act5,
     v_e1b, v_e2a, t_e1b, ring, bias, w_first, w_out,
     pm, pt, pl2, pl3, pd1, pool, up_f32, ys, ysend, yrecv,
     sem_w, sem_r, x_send, x_recv, h_send, h_recv, e_send, e_recv, y_send, y_recv) = refs
    col = lax.axis_index("col")
    row = lax.axis_index("row")
    data = lax.axis_index("data")

    def owner(strip):
        strip_col = strip // 4
        k = strip % 4
        return strip_col, k + (strip_col % 2) * (3 - 2 * k)

    def device(strip_col, strip_row):
        return (data, strip_col, strip_row)

    k_me = row + (col % 2) * (3 - 2 * row)
    me = 4 * col + k_me

    def whole(src, dst, index):
        return pltpu.make_async_copy(src, dst, sem_w.at[index])

    cp_e1b = whole(h_e1b, v_e1b, 0)
    cp_e2a = whole(h_e2a, v_e2a, 1)
    cp_d1b = whole(h_d1b, v_e1b, 2)

    def half(index):
        return pl.ds((index % 2) * C2, C2)

    def unit(index):
        slot = index % RING
        dst = ring.at[slot]
        if index < MA:
            src = h_e2b.at[index]
        elif index < MB:
            tap = (index - MA) // 2
            src = h_ma.at[ROWS[tap // 3] * 3 + tap % 3, :, half(index - MA)]
        elif index < UP2:
            local = index - MB
            tap = local // 4
            src = h_mb.at[ROWS[tap // 3] * 3 + tap % 3, half(local // 2), half(local)]
        elif index < D2A:
            local = index - UP2
            src = h_up2.at[local // 2, half(local)]
        elif index < D2B:
            local = (index - D2A) % TAP9
            src = h_d2a.at[(local % 3) * 3 + local // 3, half((D2B - 1 - index) // TAP9)]
        elif index < UP1:
            local = index - D2B
            src = h_d2b.at[(local % 3) * 3 + local // 3]
        elif index < D1A:
            src = h_up1.at[pl.ds((index - UP1) * C2, C2)]
        elif index < UNITS - 1:
            src = h_d1a.at[pl.ds((index - D1A) * C2, C2)]
        else:
            src = h_d1a.at[pl.ds((index - D1A) * C2, C1)]
            dst = ring.at[slot, pl.ds(0, C1)]
        return pltpu.make_async_copy(src, dst, sem_r.at[slot])

    def wait_units(first, last):
        for index in range(first, last):
            unit(index).wait()

    def refill(done):
        for index in range(done[0] + RING, min(done[1] + RING, UNITS)):
            unit(index).start()

    cp_e1b.start()
    cp_e2a.start()
    for index in range(RING):
        unit(index).start()

    bias[...] = jnp.zeros_like(bias)
    for index, ref in enumerate(biases):
        bias[index:index + 1, :ref.shape[0]] = ref[...].reshape(1, ref.shape[0])
    w_first[...] = jnp.zeros_like(w_first)
    for tap in range(TAP9):
        at = (tap // 3) * STRIPS + (tap % 3) * SIDE
        w_first[at:at + SIDE, :C1] = w_e1a[tap].astype(F32)
    w_out[...] = jnp.zeros_like(w_out)
    w_out[:SIDE, :C1] = w_head[...].astype(F32)

    barrier = pltpu.get_barrier_semaphore()
    for strip in range(1, STRIPS):
        other = (me + strip) % STRIPS
        other_col, other_row = owner(other)
        pl.semaphore_signal(barrier, inc=1, device_id=device(other_col, other_row), device_id_type=MESH_ID)
    pl.semaphore_wait(barrier, LAST)

    def is_me(strip_col, strip_row):
        return AND(strip_col == col, strip_row == row)

    def remote(src, dst, send, recv, strip_col, strip_row):
        return pltpu.make_async_remote_copy(src_ref=src, dst_ref=dst, send_sem=send, recv_sem=recv,
                                            device_id=device(strip_col, strip_row), device_id_type=MESH_ID)

    for k in range(SIDE):
        to_col, to_row = owner(4 * row + k)
        here = is_me(to_col, to_row)
        copy = remote(x_ref.at[pl.ds(SUB * k, STRIPS)], xb.at[col], x_send.at[k], x_recv.at[col], to_col, to_row)

        @pl.when(NOT(here))
        def _():
            copy.start()

        @pl.when(here)
        def _():
            xb[pl.ds(col, 1)] = x_ref[SUB * k:SUB * k + STRIPS][None]

    def halo_target(strip):
        return owner(jnp.clip(strip, 0, LAST))

    for side, (strip, allowed, first) in enumerate(((4 * row - 1, row > 0, 0), (4 * row + 4, row < 3, W3))):
        to_col, to_row = halo_target(strip)
        here = is_me(to_col, to_row)
        copy = remote(x_ref.at[pl.ds(first, SUB)], xh.at[col], h_send.at[side], h_recv.at[col], to_col, to_row)

        @pl.when(AND(allowed, NOT(here)))
        def _():
            copy.start()

        @pl.when(AND(allowed, here))
        def _():
            xh[pl.ds(col, 1)] = x_ref[first:first + SUB][None]

    for c in range(SIDE):
        @pl.when(NOT(is_me(c, row) & (row == col)))
        def _():
            remote(x_ref.at[pl.ds(0, STRIPS)], xb.at[c], x_send.at[0], x_recv.at[c], col, row).wait_recv()

    has_top = AND(k_me == 0, col > 0)
    has_bottom = AND(k_me == 3, col < 3)
    halo_row = jnp.where(has_top, col - 1, col + 1)
    for c in range(SIDE):
        own = AND(c == col, row == halo_row)

        @pl.when(AND(OR(has_top, has_bottom), NOT(own)))
        def _():
            remote(x_ref.at[pl.ds(0, SUB)], xh.at[c], h_send.at[0], h_recv.at[c], col, row).wait_recv()

    for k in range(SIDE):
        to_col, to_row = owner(4 * row + k)

        @pl.when(NOT(is_me(to_col, to_row)))
        def _():
            remote(x_ref.at[pl.ds(SUB * k, STRIPS)], xb.at[col], x_send.at[k], x_recv.at[col], to_col, to_row).wait_send()

    for side, (strip, allowed, first) in enumerate(((4 * row - 1, row > 0, 0), (4 * row + 4, row < 3, W3))):
        to_col, to_row = halo_target(strip)

        @pl.when(AND(allowed, NOT(is_me(to_col, to_row))))
        def _():
            remote(x_ref.at[pl.ds(first, SUB)], xh.at[col], h_send.at[side], h_recv.at[col], to_col, to_row).wait_send()

    lanes16 = lax.broadcasted_iota(jnp.int32, (STRIPS, LANE), 1)
    rows16 = lax.broadcasted_iota(jnp.int32, (STRIPS, LANE), 0)
    planes = [jnp.zeros((STRIPS, LANE), F32) for _ in range(SIDE)]
    for c in range(SIDE):
        halo = xh[c]
        both = jnp.concatenate([halo, halo], axis=0)
        top_rows = AND(has_top, rows16 < 2)
        bottom_rows = AND(has_bottom, AND(rows16 >= 10, rows16 < 12))
        block = jnp.where(OR(top_rows, bottom_rows), both, xb[c])
        inside = AND(lanes16 >= W3 * c, lanes16 < W3 * c + W3)
        for channel in range(SIDE):
            shift = (W3 * c - W3 * channel) % LANE
            moved = block if shift == 0 else pltpu.roll(block, shift, 1)
            planes[channel] = jnp.where(inside, moved, planes[channel])
    z[...] = jnp.zeros_like(z)
    for dx in TAPS:
        for channel in range(SIDE):
            plane = planes[channel]
            if dx == 0:
                plane = jnp.where(lanes16 == 0, 0.0, pltpu.roll(plane, 1, 1))
            elif dx == 2:
                plane = jnp.where(lanes16 == 127, 0.0, pltpu.roll(plane, 127, 1))
            z[pl.ds(dx * 4 + channel, STRIPS, stride=STRIPS), :] = plane

    def first_conv(pair, carry):
        weights = w_first[...].astype(BF16)
        for j in (2 * pair, 2 * pair + 1):
            taps = z[pl.ds(pl.multiple_of(j * STRIPS, STRIPS), 48), :].astype(BF16)
            value = lax.dot_general(taps, weights, (((0,), (0,)), ((), ())), preferred_element_type=F32)
            value = relu(value + bias[:1, :C1P])
            outside = OR(AND(me == 0, j == 0), AND(me == LAST, j == TAP9))
            value = jnp.where(outside, 0.0, value)
            act1[pl.ds(pl.multiple_of(j * LANE, LANE), LANE), :] = value.astype(BF16)
        return carry

    lax.fori_loop(0, 5, first_conv, 0)

    up_col, up_row = owner(jnp.maximum(me - 1, 0))
    down_col, down_row = owner(jnp.minimum(me + 1, LAST))

    def clear_borders(ref, width, height):
        @pl.when(me == 0)
        def _():
            ref[:width, :] = jnp.zeros((width, ref.shape[1]), BF16)

        @pl.when(me == LAST)
        def _():
            ref[(height + 1) * width:(height + 2) * width, :] = jnp.zeros((width, ref.shape[1]), BF16)

    for ref, width, height in ((cat1, LANE, SUB), (act5, LANE, SUB), (p1, HALF, SIDE), (act2, HALF, SIDE), (s2, HALF, SIDE),
                               (u2, HALF, SIDE), (act4, HALF, SIDE), (p2, W3, 2), (act3, W3, 2)):
        clear_borders(ref, width, height)

    def halo_copies(ref, width, height, index, lanes):
        to_up = remote(ref.at[pl.ds(width, width), lanes], ref.at[pl.ds((height + 1) * width, width), lanes],
                       e_send.at[index, 0], e_recv.at[index, 0], up_col, up_row)
        to_down = remote(ref.at[pl.ds(height * width, width), lanes], ref.at[pl.ds(0, width), lanes],
                         e_send.at[index, 1], e_recv.at[index, 1], down_col, down_row)
        return to_up, to_down

    def halo_start(ref, width, height, index, lanes=slice(None)):
        to_up, to_down = halo_copies(ref, width, height, index, lanes)

        @pl.when(me > 0)
        def _():
            to_up.start()

        @pl.when(me < LAST)
        def _():
            to_down.start()

    def halo_wait(ref, width, height, index, lanes=slice(None)):
        to_up, to_down = halo_copies(ref, width, height, index, lanes)

        @pl.when(me > 0)
        def _():
            to_down.wait_recv()
            to_up.wait_send()

        @pl.when(me < LAST)
        def _():
            to_up.wait_recv()
            to_down.wait_send()

    def build_tail(weights, base, tail):
        def body(dy, carry):
            parts = [weights[dy * 3 + dx, base:base + C1, TILE:C1].astype(F32) for dx in TAPS]
            zero = jnp.zeros((C1, HALF), F32)
            pair = jnp.concatenate([parts[0], parts[1]], axis=1)
            last = jnp.concatenate([parts[2], zero], axis=1)
            tail[dy, :, :LANE] = pair.astype(BF16)
            tail[dy, :, LANE:TILE] = last.astype(BF16)
            return carry

        lax.fori_loop(0, 3, body, 0)

    def narrow_lhs(ref, start, rows, width):
        mains = [ref[pl.ds(start + dy * width, rows), :TILE] for dy in TAPS]
        tails = [ref[pl.ds(start + dy * width, rows), TILE:C1P] for dy in TAPS]
        pair = (tails[0].astype(F32) + pltpu.roll(tails[1].astype(F32), HALF, 1)).astype(BF16)
        return jnp.concatenate(mains + [pair, tails[2][:, :HALF]], axis=1)

    def narrow_rhs(load):
        return jnp.concatenate([load(dy, 0, TILE) for dy in TAPS] + [load(dy, TILE, C1) for dy in TAPS], axis=0)

    x_index = column_index(TILE, LANE)
    not_first = x_index > 0
    not_last = x_index < 127

    low_half = lane_mask((TILE, LANE), HALF)

    def shifted(ref, plane, left, right):
        first = left + jnp.where(not_first, ref[plane(0) + (slice(7, 263), right[0])], 0.0)
        return first + jnp.where(not_last, ref[plane(2) + (slice(9, 265), right[1])], 0.0)

    def blocks_of(block):
        return slice(block * LANE, block * LANE + LANE)

    def conv_narrow(ref, bias_row, finish, chunks):
        def chunk(step, carry):
            i = chunks[0] + step * chunks[1]
            start = pl.multiple_of(i * TILE, TILE)
            left = narrow_lhs(ref, start, TILE, LANE)
            for dx in TAPS:
                pm[dx, SUB:END, :] = dot(left, narrow_rhs(lambda dy, a, b: v_e1b[dy * 3 + dx, a:b, :TILE]))
            pt[SUB:END, :] = dot(left, narrow_rhs(lambda dy, a, b: t_e1b[dy, a:b, :]))
            pieces = []
            for block in range(2):
                lanes = blocks_of(block)
                value = shifted(pm, lambda dx: (dx,), pm[1, SUB:END, lanes], (lanes, lanes))
                pieces.append(relu(value + bias[bias_row:bias_row + 1, lanes]))
            value = shifted(pt, lambda dx: (), pltpu.roll(pt[SUB:END, :LANE], HALF, 1), (blocks_of(0), blocks_of(1)))
            value = relu(value + bias[bias_row:bias_row + 1, TILE:C1P])
            pieces.append(jnp.where(low_half, value, 0.0))
            finish(i, pieces)
            return carry

        lax.fori_loop(0, 2, chunk, 0)

    def conv_cat(bias_row, finish, chunks):
        def chunk(step, carry):
            i = chunks[0] + step * chunks[1]
            start = pl.multiple_of(i * TILE, TILE)
            left = jnp.concatenate([cat1[pl.ds(start + dy * LANE, TILE), :] for dy in TAPS], axis=1)
            right = jnp.concatenate([jnp.concatenate([d1a_tap(dy * 3 + dx) for dx in TAPS], axis=0) for dy in TAPS], axis=1)
            pd1[SUB:END, :960] = lax.dot_general(left, right, (((1,), (1,)), ((), ())), preferred_element_type=F32)
            turned = [pltpu.roll(pd1[SUB:END, blocks_of(2 + block)], HALF, 1) for block in TAPS]
            pieces = []
            for block in TAPS:
                middle = turned[block] if block == 2 else jnp.where(low_half, turned[block], turned[block + 1])
                value = shifted(pd1, lambda dx: (), middle, (blocks_of(block), blocks_of(5 + block) if block < 2 else slice(896, 1024)))
                value = relu(value + bias[bias_row:bias_row + 1, blocks_of(block)])
                pieces.append(value if block < 2 else jnp.where(low_half, value, 0.0))
            finish(i, pieces)
            return carry

        lax.fori_loop(0, 2, chunk, 0)

    def store_level1(ref):
        def finish(i, pieces):
            start = pl.multiple_of(LANE + i * TILE, LANE)
            for block in range(3):
                ref[pl.ds(start, TILE), block * LANE:block * LANE + LANE] = pieces[block].astype(BF16)
        return finish

    def finish_s1(i, pieces):
        at = pl.ds(pl.multiple_of(LANE + i * TILE, LANE), TILE)
        turned = [pltpu.roll(piece, HALF, 1) for piece in pieces]
        cat1[at, TILE:C1P] = jnp.where(low_half, 0.0, turned[0]).astype(BF16)
        for block in range(2):
            cat1[at, blocks_of(3 + block)] = jnp.where(low_half, turned[block], turned[block + 1]).astype(BF16)
        start = pl.multiple_of(HALF + i * HALF, HALF)
        for block in range(3):
            pool[:LANE, :] = jnp.maximum(pieces[block][:LANE], pieces[block][LANE:TILE])
            pooled = jnp.maximum(pool[pl.ds(0, HALF, stride=2), :], pool[pl.ds(1, HALF, stride=2), :])
            p1[pl.ds(start, HALF), block * LANE:block * LANE + LANE] = pooled.astype(BF16)

    S1_LANES = pl.ds(C1P, TILE)
    U1_LANES = pl.ds(0, C1P)
    cp_e1b.wait()
    build_tail(v_e1b, 0, t_e1b)
    conv_narrow(act1, 1, finish_s1, (0, 3))
    halo_start(p1, HALF, SIDE, 0)
    halo_start(cat1, LANE, SUB, 1, S1_LANES)
    conv_narrow(act1, 1, finish_s1, (1, 1))
    cp_d1b.start()

    x_index2 = column_index(TILE, HALF)
    not_first2 = x_index2 > 0
    not_last2 = x_index2 < 63

    def finish_level2(bias_row, store):
        def body(block, carry):
            lanes = pl.ds(pl.multiple_of(block * LANE, LANE), LANE)
            value = pl2[1, SUB:END, lanes] + jnp.where(not_first2, pl2[0, 7:263, lanes], 0.0)
            value = value + jnp.where(not_last2, pl2[2, 9:265, lanes], 0.0)
            store(lanes, relu(value + bias[bias_row:bias_row + 1, lanes]))
            return carry

        lax.fori_loop(0, 5, body, 0)

    def store_level2(ref, start):
        def store(lanes, value):
            ref[start:start + TILE, lanes] = value.astype(BF16)
        return store

    def store_s2(lanes, value):
        s2[HALF:C1, lanes] = value.astype(BF16)
        for i in range(2):
            pool[:HALF, :] = jnp.maximum(value[LANE * i:LANE * i + HALF], value[LANE * i + HALF:LANE * i + LANE])
            pooled = jnp.maximum(pool[pl.ds(0, W3, stride=2), :], pool[pl.ds(1, W3, stride=2), :])
            p2[W3 + W3 * i:HALF + W3 * i, lanes] = pooled.astype(BF16)

    NTILES = ((0, TILE), (TILE, 512), (512, C2))

    def stack_rows(ref, rows, width):
        return jnp.concatenate([ref[dy * width:dy * width + rows, :] for dy in TAPS], axis=1)

    halo_wait(p1, HALF, 4, 0)
    cp_e2a.wait()

    def enc2a(dx, carry):
        left = narrow_lhs(p1, 0, TILE, HALF)
        for a, b in NTILES:
            right = narrow_rhs(lambda dy, r0, r1: v_e2a[dy * 3 + dx, r0:r1, a:b])
            pl2[dx, SUB:END, a:b] = dot(left, right)
        return carry

    lax.fori_loop(0, 3, enc2a, 0)
    finish_level2(2, store_level2(act2, HALF))
    halo_start(act2, HALF, 4, 2)

    wait_units(E2B, MA)
    halo_wait(act2, HALF, 4, 2)

    def conv640(ref, slots):
        def body(dx, carry):
            left = stack_rows(ref, TILE, HALF)
            picks = slots(dx)
            for a, b in NTILES:
                right = jnp.concatenate([ring[pick, :, a:b] for pick in picks], axis=0)
                pl2[dx, SUB:END, a:b] = dot(left, right)
            return carry

        lax.fori_loop(0, 3, body, 0)

    conv640(act2, lambda dx: [dy * 3 + dx for dy in TAPS])
    finish_level2(3, store_s2)
    halo_start(p2, W3, 2, 3)
    halo_start(s2, HALF, 4, 4)
    refill((E2B, MA))

    x_index3 = column_index(HALF, W3)
    not_first3 = x_index3 > 0
    not_last3 = x_index3 < 31

    def finish_level3(bias_row, ref, start):
        def body(block, carry):
            lanes = pl.ds(pl.multiple_of(block * LANE, LANE), LANE)
            value = pl3[1, SUB:72, lanes] + jnp.where(not_first3, pl3[0, 7:71, lanes], 0.0)
            value = value + jnp.where(not_last3, pl3[2, 9:73, lanes], 0.0)
            ref[start:start + HALF, lanes] = relu(value + bias[bias_row:bias_row + 1, lanes]).astype(BF16)
            return carry

        lax.fori_loop(0, 10, body, 0)

    def slot_of(index):
        return lax.rem(index, RING)

    def wide(first):
        return jnp.concatenate([ring[slot_of(first)], ring[slot_of(first + 1)]], axis=1)

    def add_rows(dx, value):
        pl3[dx, SUB:72, :] = pl3[dx, SUB:72, :] + value

    def mid_a_own(dx, carry):
        pl3[dx, SUB:72, :] = dot(p2[W3:3 * W3, :], wide(MA + 2 * dx))
        return carry

    def mid_a_halo(dx, carry):
        left = jnp.concatenate([p2[:HALF, :], p2[HALF:LANE, :]], axis=1)
        add_rows(dx, dot(left, jnp.concatenate([wide(MA + 6 + 2 * dx), wide(MA + 12 + 2 * dx)], axis=0)))
        return carry

    wait_units(MA, MB)
    lax.fori_loop(0, 3, mid_a_own, 0)
    halo_wait(p2, W3, 2, 3)
    lax.fori_loop(0, 3, mid_a_halo, 0)
    finish_level3(4, act3, W3)
    halo_start(act3, W3, 2, 5)
    refill((MA, MB))

    for group, dy in enumerate(ROWS):
        def mid_b(dx, carry):
            first = MB + (group * 3 + dx) * SIDE
            for part in range(SIDE):
                slot = slot_of(first + part)
                pltpu.make_async_copy(h_e2b.at[0], ring.at[slot], sem_r.at[slot]).wait()
            value = dot(act3[dy * W3:dy * W3 + HALF, :], jnp.concatenate([wide(first), wide(first + 2)], axis=0))
            if group:
                add_rows(dx, value)
            else:
                pl3[dx, SUB:72, :] = value
            return carry

        if group == 1:
            halo_wait(act3, W3, 2, 5)
        lax.fori_loop(0, 3, mid_b, 0)
        refill((MB + group * 12, MB + group * 12 + 12))
    finish_level3(5, mid, 0)

    wait_units(UP2, D2A)
    for tap in range(SIDE):
        p, q = tap // 2, tap % 2
        left = mid[...]
        for a, b in NTILES:
            right = jnp.concatenate([ring[(UP2 + 2 * tap + part) % RING, :, a:b] for part in range(2)], axis=0)
            part = dot(left, right)
            for i in range(2):
                for c0 in range(a, b, LANE):
                    up_f32[pl.ds(c0 * 2 + (2 * i + p) * HALF + q, W3, stride=2), :] = part[W3 * i:W3 * i + W3, c0 - a:c0 - a + LANE]
    for block in range(5):
        u2[HALF:C1, block * LANE:block * LANE + LANE] = up_f32[block * TILE:block * TILE + TILE, :].astype(BF16)
    halo_start(u2, HALF, 4, 6)
    refill((UP2, D2A))
    halo_wait(s2, HALF, SIDE, 4)

    def dec2a(ref, first, dx):
        left = stack_rows(ref, TILE, HALF)
        for a, b in NTILES:
            right = jnp.concatenate([ring[slot_of(first + dx * 3 + dy), :, a:b] for dy in TAPS], axis=0)
            yield a, b, dot(left, right)

    def dec2a_skip(dx, carry):
        for a, b, value in dec2a(s2, D2A, dx):
            pl2[dx, SUB:END, a:b] = value
        return carry

    def dec2a_up(dx, carry):
        for a, b, value in dec2a(u2, D2A + TAP9, dx):
            pl2[dx, SUB:END, a:b] = pl2[dx, SUB:END, a:b] + value
        return carry

    wait_units(D2A, D2A + TAP9)
    lax.fori_loop(0, 3, dec2a_skip, 0)
    refill((D2A, D2A + TAP9))
    wait_units(D2A + TAP9, D2B)
    halo_wait(u2, HALF, SIDE, 6)
    lax.fori_loop(0, 3, dec2a_up, 0)
    refill((D2A + TAP9, D2B))
    finish_level2(6, store_level2(act4, HALF))
    halo_start(act4, HALF, 4, 7)
    wait_units(D2B, UP1)
    halo_wait(act4, HALF, 4, 7)
    conv640(act4, lambda dx: [slot_of(D2B + dx * 3 + dy) for dy in TAPS])
    finish_level2(7, store_level2(d2, 0))

    def half1(tap):
        return slice((tap % 2) * C1, (tap % 2) * C1 + C1)

    refill((D2B, UP1))
    wait_units(UP1, D1A)
    for tap in range(SIDE):
        p, q = tap // 2, tap % 2
        left = d2[...]
        up = lax.dot_general(left, ring[(UP1 + tap // 2) % RING, half1(tap), :], (((1,), (1,)), ((), ())), preferred_element_type=F32)
        for a, b in ((0, TILE), (TILE, C1)):
            part = up[:, a:b]
            for i in range(SIDE):
                for c0 in range(a, b, LANE):
                    c1 = min(b, c0 + LANE)
                    up_f32[pl.ds(c0 * SUB + (2 * i + p) * LANE + q, HALF, stride=2), :c1 - c0] = part[HALF * i:HALF * i + HALF, c0 - a:c1 - a]
    for block in TAPS:
        value = up_f32[block * 1024:block * 1024 + 1024, :].astype(BF16)
        if block < 2:
            cat1[LANE:TILE + 7 * LANE, blocks_of(block)] = value
        else:
            cat1[LANE:TILE + 7 * LANE, TILE:C1] = value[:, :HALF]
    halo_start(cat1, LANE, SUB, 8, U1_LANES)

    def d1a_tap(tap):
        return ring[(D1A + tap // 2) % RING, half1(tap), :]

    wait_units(D1A, UNITS)
    conv_cat(8, store_level1(act5), (1, 1))
    halo_wait(cat1, LANE, SUB, 1, S1_LANES)
    halo_wait(cat1, LANE, SUB, 8, U1_LANES)
    conv_cat(8, store_level1(act5), (0, 3))
    halo_start(act5, LANE, SUB, 9)
    cp_d1b.wait()
    build_tail(v_e1b, 0, t_e1b)

    def finish_head(i, pieces):
        value = jnp.concatenate([piece.astype(BF16) for piece in pieces], axis=1)
        head = lax.dot_general(w_out[...].astype(BF16), value, (((1,), (1,)), ((), ())), preferred_element_type=F32)
        ys[pl.ds(i, 1)] = head[None]

    conv_narrow(act5, TAP9, finish_head, (1, 1))
    halo_wait(act5, LANE, SUB, 9)
    conv_narrow(act5, TAP9, finish_head, (0, 3))

    lanes8 = lax.broadcasted_iota(jnp.int32, (SUB, LANE), 1)
    sub8 = lax.broadcasted_iota(jnp.int32, (SUB, LANE), 0)
    for c in range(SIDE):
        packed = jnp.zeros((SUB, LANE), F32)
        for y in range(SUB):
            line = ys[y // 2, :, (y % 2) * LANE:(y % 2) * LANE + LANE]
            slot = y % 4
            shift = (W3 * slot - W3 * c) % LANE
            line = line if shift == 0 else pltpu.roll(line, shift, 1)
            if y >= 4:
                line = pltpu.roll(line, 4, 0)
            place = AND(AND(lanes8 >= W3 * slot, lanes8 < W3 * slot + W3), (sub8 >= 4) if y >= 4 else (sub8 < 4))
            packed = jnp.where(place, line, packed)
        ysend[c] = packed

    def y_copy(c):
        return remote(ysend.at[c], yrecv.at[k_me], y_send.at[c], y_recv.at[k_me], c, col)

    for c in range(SIDE):
        here = is_me(c, col)

        @pl.when(NOT(here))
        def _():
            y_copy(c).start()

        @pl.when(here)
        def _():
            yrecv[pl.ds(k_me, 1)] = ysend[c][None]

    for k in range(SIDE):
        from_col, from_row = owner(4 * row + k)

        @pl.when(NOT(is_me(from_col, from_row)))
        def _():
            remote(ysend.at[0], yrecv.at[k], y_send.at[0], y_recv.at[k], col, row).wait_recv()

    for c in range(SIDE):
        @pl.when(NOT(is_me(c, col)))
        def _():
            y_copy(c).wait_send()

    out_ref[...] = yrecv[...]


def network(x, w_e1a, w_head, *rest):
    vmem = pl.BlockSpec(memory_space=pltpu.VMEM)
    hbm = pl.BlockSpec(memory_space=pl.ANY)
    dma = pltpu.SemaphoreType.DMA
    scratch = [pltpu.VMEM(shape, F32) for shape in ((SIDE, STRIPS, LANE), (SIDE, SUB, LANE), (TILE, LANE))]
    level1, level2 = 10 * LANE, 6 * HALF
    scratch += [pltpu.VMEM(shape, BF16) for shape in (
        (level1, C1P), (level1, C2), (level2, C1P), (level2, C2), (level2, C2), (LANE, C2), (LANE, C3), (HALF, C3),
        (level2, C2), (level2, C2), (TILE, C2), (level1, C1P),
        (TAP9, C1, C1), (TAP9, C1, C2), (3, C1, TILE), (RING, C2, C2))]
    scratch += [pltpu.VMEM(shape, F32) for shape in (
        (10, C3), (48, C1P), (SUB, C1P),
        (3, MARGIN, TILE), (MARGIN, TILE), (3, MARGIN, C2), (3, 80, C3), (MARGIN, 1024),
        (LANE, LANE), (3072, LANE), (SIDE, SUB, TILE), (SIDE, SUB, LANE), (SIDE, SUB, LANE))]
    scratch += [dma(shape) for shape in ((3,), (RING,), (SIDE,), (SIDE,), (2,), (SIDE,), (10, 2), (10, 2), (SIDE,), (SIDE,))]
    return pl.pallas_call(
        kernel,
        out_shape=jax.ShapeDtypeStruct((SIDE, SUB, LANE), F32),
        in_specs=[vmem] * 13 + [hbm] * 11,
        out_specs=vmem,
        scratch_shapes=scratch,
        compiler_params=pltpu.CompilerParams(collective_id=0, has_side_effects=True, vmem_limit_bytes=67043328),
        name="unet",
    )(x, w_e1a, w_head, *rest)


def solution(mesh):
    tile_spec = P(("data", "row"), "col", None)

    def device_body(tile, *params):
        (w_enc1a, b_enc1a, w_enc1b, b_enc1b, w_enc2a, b_enc2a, w_enc2b, b_enc2b,
         w_mid_a, b_mid_a, w_mid_b, b_mid_b, w_up2, w_dec2a, b_dec2a, w_dec2b, b_dec2b,
         w_up1, w_dec1a, b_dec1a, w_dec1b, b_dec1b, w_head, b_head) = params
        x = jnp.transpose(tile, (0, 2, 1)).reshape(W3, LANE).astype(F32)
        x = jnp.pad(x, ((2, 6), (0, 0)))
        biases = (b_enc1a, b_enc1b, b_enc2a, b_enc2b, b_mid_a, b_mid_b, b_dec2a, b_dec2b, b_dec1a, b_dec1b)

        def taps(weight):
            return weight.reshape(-1, weight.shape[2], weight.shape[3])

        def turned(weight):
            return jnp.swapaxes(weight, 2, 3).reshape(-1, weight.shape[2])

        weights = [taps(w) for w in (w_enc1b, w_enc2a, w_enc2b, w_mid_a, w_mid_b, w_up2, w_dec2a, w_dec2b)]
        weights += [turned(w_up1), turned(w_dec1a), taps(w_dec1b)]
        packed = network(x, taps(w_enc1a), w_head.T, *biases, *weights)
        out = packed.reshape(4, 2, 4, 4, W3).transpose(0, 1, 3, 4, 2).reshape(W3, W3, 4)
        return out + b_head

    def program(image, *params):
        mapped = jax.shard_map(device_body, mesh=mesh, in_specs=(tile_spec,) + tuple([P()] * len(params)), out_specs=tile_spec, check_vma=False)
        return mapped(image, *params)

    return program
```

```python
import jax
import jax.numpy as jnp
from jax import lax
from jax.experimental import pallas as pl
from jax.experimental.pallas import tpu as pltpu
from jax.sharding import PartitionSpec as P

F32 = jnp.float32
BF16 = jnp.bfloat16
STRIPS = 16
LAST = STRIPS - 1
SIDE = 4
SUB, LANE = 8, 128
TILE, HALF = 2 * LANE, LANE // 2
C1, C2, C3, C1P = 320, 640, 1280, 384
W3 = 32
END = SUB + TILE
MARGIN = END + SUB
TAPS = range(3)
PAIR = range(2)
QUAD = range(SIDE)
TAP9 = 9
RING = 50
E2B, MA, MB, UP2, D2A, D2B, UP1, D1A, UNITS = 0, 9, 27, 63, 71, 89, 98, 100, 105
ROWS = (1, 0, 2)
NOT = jnp.logical_not
AND = jnp.logical_and
OR = jnp.logical_or
MESH_ID = pl.DeviceIdType.MESH


def dot(lhs, rhs):
    return jnp.dot(lhs, rhs, preferred_element_type=F32)


def relu(value):
    return jnp.maximum(value, 0.0)


def dot_t(lhs, rhs):
    return lax.dot_general(lhs, rhs, (((1,), (1,)), ((), ())), preferred_element_type=F32)


def cat_lanes(parts):
    return jnp.concatenate(list(parts), axis=1)


def cat_rows(parts):
    return jnp.concatenate(list(parts), axis=0)


def turn(value, amount=HALF):
    return value if amount == 0 else pltpu.roll(value, amount, 1)


def lane_mask(shape, below):
    return lax.broadcasted_iota(jnp.int32, shape, 1) < below


def column_index(rows, width):
    return lax.rem(lax.broadcasted_iota(jnp.int32, (rows, LANE), 0), width)


def kernel(x_ref, w_e1a, w_head, *refs):
    biases, refs = refs[:10], refs[10:]
    (h_e1b, h_e2a, h_e2b, h_ma, h_mb, h_up2, h_d2a, h_d2b, h_up1, h_d1a, h_d1b,
     out_ref,
     xrows, xs, xb, xh, z, act1, cat1, p1, act2, s2, p2, act3, mid, u2, act4, d2, act5,
     v_e1b, v_e2a, t_e1b, ring, bias, w_first, w_out,
     pm, pt, pl2, pl3, pd1, pool, up_f32, ys, ysend, yrecv,
     sem_w, sem_r, x_send, x_recv, h_send, h_recv, e_send, e_recv, y_send, y_recv) = refs
    col = lax.axis_index("col")
    row = lax.axis_index("row")
    data = lax.axis_index("data")

    def owner(strip):
        strip_col = strip // 4
        k = strip % 4
        return strip_col, k + (strip_col % 2) * (3 - 2 * k)

    def device(strip_col, strip_row):
        return (data, strip_col, strip_row)

    k_me = row + (col % 2) * (3 - 2 * row)
    me = 4 * col + k_me

    barrier = pltpu.get_barrier_semaphore()
    for strip in range(1, STRIPS):
        other_col, other_row = owner((me + strip) % STRIPS)
        pl.semaphore_signal(barrier, inc=1, device_id=device(other_col, other_row), device_id_type=MESH_ID)

    def whole(src, dst, index):
        return pltpu.make_async_copy(src, dst, sem_w.at[index])

    cp_e1b = whole(h_e1b, v_e1b, 0)
    cp_e2a = whole(h_e2a, v_e2a, 1)
    cp_d1b = whole(h_d1b, v_e1b, 2)

    def half(index):
        return pl.ds((index % 2) * C2, C2)

    def unit(index):
        slot = index % RING
        dst = ring.at[slot]
        if index < MA:
            src = h_e2b.at[(index % 3) * 3 + index // 3]
        elif index < MB:
            tap = (index - MA) // 2
            src = h_ma.at[ROWS[tap // 3] * 3 + tap % 3, :, half(index - MA)]
        elif index < UP2:
            local = index - MB
            tap = local // 4
            src = h_mb.at[ROWS[tap // 3] * 3 + tap % 3, half(local // 2), half(local)]
        elif index < D2A:
            local = index - UP2
            src = h_up2.at[local // 2, half(local)]
        elif index < D2B:
            local = (index - D2A) % TAP9
            src = h_d2a.at[(local % 3) * 3 + local // 3, half((D2B - 1 - index) // TAP9)]
        elif index < UP1:
            local = index - D2B
            src = h_d2b.at[(local % 3) * 3 + local // 3]
        elif index < D1A:
            src = h_up1.at[pl.ds((index - UP1) * C2, C2)]
        elif index < UNITS - 1:
            src = h_d1a.at[pl.ds((index - D1A) * C2, C2)]
        else:
            src = h_d1a.at[pl.ds((index - D1A) * C2, C1)]
            dst = ring.at[slot, pl.ds(0, C1)]
        return pltpu.make_async_copy(src, dst, sem_r.at[slot])

    def wait_units(first, last):
        for index in range(first, last):
            unit(index).wait()

    def refill(done):
        for index in range(done[0] + RING, min(done[1] + RING, UNITS)):
            unit(index).start()

    cp_e1b.start()
    cp_e2a.start()
    for index in range(RING):
        unit(index).start()

    bias[...] = jnp.zeros_like(bias)
    for index, ref in enumerate(biases):
        bias[index:index + 1, :ref.shape[0]] = ref[...].reshape(1, ref.shape[0])
    w_first[...] = jnp.zeros_like(w_first)
    for tap in range(TAP9):
        at = (tap // 3) * STRIPS + (tap % 3) * SIDE
        w_first[at:at + SIDE, :C1] = w_e1a[tap].astype(F32)
    w_out[...] = jnp.zeros_like(w_out)
    w_out[:SIDE, :C1] = w_head[...].astype(F32)

    xrows[...] = jnp.zeros_like(xrows)
    xrows[2:2 + W3, :SIDE, :W3] = x_ref[...].astype(F32)

    def pack(group, carry):
        packed = jnp.zeros((SUB, LANE), F32)
        for j in range(SUB):
            line = turn(xrows[group * SUB + j], (j % SIDE) * W3)
            packed = packed + (line if j < SIDE else pltpu.roll(line, SIDE, 0))
        xs[pl.ds(group, 1)] = packed[None]
        return carry

    lax.fori_loop(0, 5, pack, 0)
    pl.semaphore_wait(barrier, LAST)

    def is_me(strip_col, strip_row):
        return AND(strip_col == col, strip_row == row)

    def remote(src, dst, send, recv, strip_col, strip_row):
        return pltpu.make_async_remote_copy(src_ref=src, dst_ref=dst, send_sem=send, recv_sem=recv,
                                            device_id=device(strip_col, strip_row), device_id_type=MESH_ID)

    for k in QUAD:
        to_col, to_row = owner(4 * row + k)
        here = is_me(to_col, to_row)
        copy = remote(xs.at[pl.ds(k, 2)], xb.at[col], x_send.at[k], x_recv.at[col], to_col, to_row)

        @pl.when(NOT(here))
        def _():
            copy.start()

        @pl.when(here)
        def _():
            xb[pl.ds(col, 1)] = xs[k:k + 2][None]

    def halo_target(strip):
        return owner(jnp.clip(strip, 0, LAST))

    for side, (strip, allowed, first) in enumerate(((4 * row - 1, row > 0, 0), (4 * row + 4, row < 3, SIDE))):
        to_col, to_row = halo_target(strip)
        here = is_me(to_col, to_row)
        copy = remote(xs.at[pl.ds(first, 1)], xh.at[col], h_send.at[side], h_recv.at[col], to_col, to_row)

        @pl.when(AND(allowed, NOT(here)))
        def _():
            copy.start()

        @pl.when(AND(allowed, here))
        def _():
            xh[pl.ds(col, 1)] = xs[first:first + 1][None]

    for c in QUAD:
        @pl.when(NOT(is_me(c, row) & (row == col)))
        def _():
            remote(xs.at[pl.ds(0, 2)], xb.at[c], x_send.at[0], x_recv.at[c], col, row).wait_recv()

    has_top = AND(k_me == 0, col > 0)
    has_bottom = AND(k_me == 3, col < 3)
    halo_row = jnp.where(has_top, col - 1, col + 1)
    for c in QUAD:
        own = AND(c == col, row == halo_row)

        @pl.when(AND(OR(has_top, has_bottom), NOT(own)))
        def _():
            remote(xs.at[pl.ds(0, 1)], xh.at[c], h_send.at[0], h_recv.at[c], col, row).wait_recv()

    for k in QUAD:
        to_col, to_row = owner(4 * row + k)

        @pl.when(NOT(is_me(to_col, to_row)))
        def _():
            remote(xs.at[pl.ds(k, 2)], xb.at[col], x_send.at[k], x_recv.at[col], to_col, to_row).wait_send()

    for side, (strip, allowed, first) in enumerate(((4 * row - 1, row > 0, 0), (4 * row + 4, row < 3, SIDE))):
        to_col, to_row = halo_target(strip)

        @pl.when(AND(allowed, NOT(is_me(to_col, to_row))))
        def _():
            remote(xs.at[pl.ds(first, 1)], xh.at[col], h_send.at[side], h_recv.at[col], to_col, to_row).wait_send()

    lanes8 = lax.broadcasted_iota(jnp.int32, (SUB, LANE), 1)
    sub8 = lax.broadcasted_iota(jnp.int32, (SUB, LANE), 0)
    z[...] = jnp.zeros_like(z)
    halo_place = (AND(has_top, lanes8 < HALF), AND(has_bottom, lanes8 >= HALF))
    for part in PAIR:
        place = AND(halo_place[part], sub8 < SIDE)
        blocks = [jnp.where(place, xh[c, 0], xb[c, part]) for c in QUAD]
        for group in QUAD:
            line = jnp.zeros((SUB, LANE), F32)
            for c in QUAD:
                inside = lanes8 // W3 == c
                line = jnp.where(inside, turn(blocks[c], (W3 * (c - group)) % LANE), line)
            for dx in TAPS:
                moved = line
                if dx == 0:
                    moved = jnp.where(lanes8 == 0, 0.0, turn(line, 1))
                elif dx == 2:
                    moved = jnp.where(lanes8 == LANE - 1, 0.0, turn(line, LANE - 1))
                for upper in range(2 - part):
                    at = (part * SUB + group + upper * SIDE) * STRIPS + dx * SIDE
                    z[at:at + SIDE, :] = moved[upper * SIDE:upper * SIDE + SIDE]

    def first_conv(pair, carry):
        weights = w_first[...].astype(BF16)
        for j in (2 * pair, 2 * pair + 1):
            taps = z[pl.ds(pl.multiple_of(j * STRIPS, STRIPS), 48), :].astype(BF16)
            value = lax.dot_general(taps, weights, (((0,), (0,)), ((), ())), preferred_element_type=F32)
            value = relu(value + bias[:1, :C1P])
            outside = OR(AND(me == 0, j == 0), AND(me == LAST, j == TAP9))
            value = jnp.where(outside, 0.0, value)
            act1[pl.ds(pl.multiple_of(j * LANE, LANE), LANE), :] = value.astype(BF16)
        return carry

    lax.fori_loop(0, 5, first_conv, 0)

    up_col, up_row = owner(jnp.maximum(me - 1, 0))
    down_col, down_row = owner(jnp.minimum(me + 1, LAST))

    def clear_borders(ref, width, height):
        @pl.when(me == 0)
        def _():
            ref[:width, :] = jnp.zeros((width, ref.shape[1]), BF16)

        @pl.when(me == LAST)
        def _():
            ref[(height + 1) * width:(height + 2) * width, :] = jnp.zeros((width, ref.shape[1]), BF16)

    for ref, width, height in ((cat1, LANE, SUB), (act5, LANE, SUB), (p1, HALF, SIDE), (act2, HALF, SIDE), (s2, HALF, SIDE),
                               (u2, HALF, SIDE), (act4, HALF, SIDE), (p2, W3, 2), (act3, W3, 2)):
        clear_borders(ref, width, height)

    def halo_copies(ref, width, height, index, lanes):
        to_up = remote(ref.at[pl.ds(width, width), lanes], ref.at[pl.ds((height + 1) * width, width), lanes],
                       e_send.at[index, 0], e_recv.at[index, 0], up_col, up_row)
        to_down = remote(ref.at[pl.ds(height * width, width), lanes], ref.at[pl.ds(0, width), lanes],
                         e_send.at[index, 1], e_recv.at[index, 1], down_col, down_row)
        return to_up, to_down

    def halo_start(ref, width, height, index, lanes=slice(None)):
        to_up, to_down = halo_copies(ref, width, height, index, lanes)

        @pl.when(me > 0)
        def _():
            to_up.start()

        @pl.when(me < LAST)
        def _():
            to_down.start()

    def halo_wait(ref, width, height, index, lanes=slice(None)):
        to_up, to_down = halo_copies(ref, width, height, index, lanes)

        @pl.when(me > 0)
        def _():
            to_down.wait_recv()
            to_up.wait_send()

        @pl.when(me < LAST)
        def _():
            to_up.wait_recv()
            to_down.wait_send()

    def build_tail(weights, base, tail):
        def body(dy, carry):
            parts = [weights[dy * 3 + dx, base:base + C1, TILE:C1].astype(F32) for dx in TAPS]
            zero = jnp.zeros((C1, HALF), F32)
            pair = cat_lanes(parts[:2])
            last = cat_lanes([parts[2], zero])
            tail[dy, :, :LANE] = pair.astype(BF16)
            tail[dy, :, LANE:TILE] = last.astype(BF16)
            return carry

        lax.fori_loop(0, 3, body, 0)

    def narrow_lhs(ref, start, rows, width):
        mains = [ref[pl.ds(start + dy * width, rows), :TILE] for dy in TAPS]
        tails = [ref[pl.ds(start + dy * width, rows), TILE:C1P] for dy in TAPS]
        pair = (tails[0].astype(F32) + turn(tails[1].astype(F32))).astype(BF16)
        return cat_lanes(mains + [pair, tails[2][:, :HALF]])

    def narrow_rhs(load):
        return cat_rows([load(dy, 0, TILE) for dy in TAPS] + [load(dy, TILE, C1) for dy in TAPS])

    x_index = column_index(TILE, LANE)
    not_first = x_index > 0
    not_last = x_index < 127

    low_half = lane_mask((TILE, LANE), HALF)

    def shifted(ref, plane, left, right):
        first = left + jnp.where(not_first, ref[plane(0) + (slice(7, 263), right[0])], 0.0)
        return first + jnp.where(not_last, ref[plane(2) + (slice(9, 265), right[1])], 0.0)

    def blocks_of(block):
        return slice(block * LANE, block * LANE + LANE)

    def conv_narrow(ref, bias_row, finish, chunks):
        def chunk(step, carry):
            i = chunks[0] + step * chunks[1]
            start = pl.multiple_of(i * TILE, TILE)
            left = narrow_lhs(ref, start, TILE, LANE)
            for dx in TAPS:
                pm[dx, SUB:END, :] = dot(left, narrow_rhs(lambda dy, a, b: v_e1b[dy * 3 + dx, a:b, :TILE]))
            pt[SUB:END, :] = dot(left, narrow_rhs(lambda dy, a, b: t_e1b[dy, a:b, :]))
            pieces = []
            for block in PAIR:
                lanes = blocks_of(block)
                value = shifted(pm, lambda dx: (dx,), pm[1, SUB:END, lanes], (lanes, lanes))
                pieces.append(relu(value + bias[bias_row:bias_row + 1, lanes]))
            value = shifted(pt, lambda dx: (), turn(pt[SUB:END, :LANE]), (blocks_of(0), blocks_of(1)))
            value = relu(value + bias[bias_row:bias_row + 1, TILE:C1P])
            pieces.append(jnp.where(low_half, value, 0.0))
            finish(i, pieces)
            return carry

        lax.fori_loop(0, 2, chunk, 0)

    def conv_cat(bias_row, finish, chunks):
        def chunk(step, carry):
            i = chunks[0] + step * chunks[1]
            start = pl.multiple_of(i * TILE, TILE)
            left = cat_lanes(cat1[pl.ds(start + dy * LANE, TILE), :] for dy in TAPS)
            right = cat_lanes(cat_rows(d1a_tap(dy * 3 + dx) for dx in TAPS) for dy in TAPS)
            pd1[SUB:END, :3 * C1] = dot_t(left, right)
            turned = [turn(pd1[SUB:END, blocks_of(2 + block)]) for block in TAPS]
            pieces = []
            for block in TAPS:
                middle = turned[block] if block == 2 else jnp.where(low_half, turned[block], turned[block + 1])
                value = shifted(pd1, lambda dx: (), middle, (blocks_of(block), blocks_of(5 + block) if block < 2 else slice(896, 1024)))
                value = relu(value + bias[bias_row:bias_row + 1, blocks_of(block)])
                pieces.append(value if block < 2 else jnp.where(low_half, value, 0.0))
            finish(i, pieces)
            return carry

        lax.fori_loop(0, 2, chunk, 0)

    def store_level1(ref):
        def finish(i, pieces):
            start = pl.multiple_of(LANE + i * TILE, LANE)
            for block in range(3):
                ref[pl.ds(start, TILE), block * LANE:block * LANE + LANE] = pieces[block].astype(BF16)
        return finish

    def finish_s1(i, pieces):
        at = pl.ds(pl.multiple_of(LANE + i * TILE, LANE), TILE)
        turned = [turn(piece) for piece in pieces]
        cat1[at, TILE:C1P] = jnp.where(low_half, 0.0, turned[0]).astype(BF16)
        for block in PAIR:
            cat1[at, blocks_of(3 + block)] = jnp.where(low_half, turned[block], turned[block + 1]).astype(BF16)
        start = pl.multiple_of(HALF + i * HALF, HALF)
        for block in range(3):
            pool[:LANE, :] = jnp.maximum(pieces[block][:LANE], pieces[block][LANE:TILE])
            pooled = jnp.maximum(pool[pl.ds(0, HALF, stride=2), :], pool[pl.ds(1, HALF, stride=2), :])
            p1[pl.ds(start, HALF), block * LANE:block * LANE + LANE] = pooled.astype(BF16)

    S1_LANES = pl.ds(C1P, TILE)
    U1_LANES = pl.ds(0, C1P)
    cp_e1b.wait()
    build_tail(v_e1b, 0, t_e1b)
    conv_narrow(act1, 1, finish_s1, (0, 3))
    halo_start(p1, HALF, SIDE, 0)
    halo_start(cat1, LANE, SUB, 1, S1_LANES)
    conv_narrow(act1, 1, finish_s1, (1, 1))
    cp_d1b.start()

    x_index2 = column_index(TILE, HALF)
    not_first2 = x_index2 > 0
    not_last2 = x_index2 < 63

    def finish_level2(bias_row, store):
        def body(block, carry):
            lanes = pl.ds(pl.multiple_of(block * LANE, LANE), LANE)
            value = pl2[1, SUB:END, lanes] + jnp.where(not_first2, pl2[0, 7:263, lanes], 0.0)
            value = value + jnp.where(not_last2, pl2[2, 9:265, lanes], 0.0)
            store(lanes, relu(value + bias[bias_row:bias_row + 1, lanes]))
            return carry

        lax.fori_loop(0, 5, body, 0)

    def store_level2(ref, start):
        def store(lanes, value):
            ref[start:start + TILE, lanes] = value.astype(BF16)
        return store

    def store_s2(lanes, value):
        s2[HALF:C1, lanes] = value.astype(BF16)
        for i in PAIR:
            pool[:HALF, :] = jnp.maximum(value[LANE * i:LANE * i + HALF], value[LANE * i + HALF:LANE * i + LANE])
            pooled = jnp.maximum(pool[pl.ds(0, W3, stride=2), :], pool[pl.ds(1, W3, stride=2), :])
            p2[W3 + W3 * i:HALF + W3 * i, lanes] = pooled.astype(BF16)

    NTILES = ((0, TILE), (TILE, 2 * TILE), (2 * TILE, C2))
    TAIL = slice(2 * TILE, C2)

    def stack_rows(ref, rows, width, taps=TAPS):
        return cat_lanes(ref[dy * width:dy * width + rows, :] for dy in taps)

    def level2_taps(left, weights, add=False):
        def put(dx, lanes, value):
            pl2[dx, SUB:END, lanes] = pl2[dx, SUB:END, lanes] + value if add else value

        for dx in TAPS:
            for first, last in NTILES[:2]:
                lanes = slice(first, last)
                put(dx, lanes, dot(left, weights(dx, lanes)))
        pair = dot(left, cat_lanes(weights(dx, TAIL) for dx in PAIR))
        put(0, TAIL, pair[:, :LANE])
        put(1, TAIL, pair[:, LANE:])
        put(2, TAIL, dot(left, weights(2, TAIL)))

    def unit_rows(first, taps=TAPS):
        return lambda dx, lanes: cat_rows(ring[(first + dx * 3 + dy) % RING, :, lanes] for dy in taps)

    halo_wait(p1, HALF, 4, 0)
    cp_e2a.wait()

    level2_taps(narrow_lhs(p1, 0, TILE, HALF),
                lambda dx, lanes: narrow_rhs(lambda dy, r0, r1: v_e2a[dy * 3 + dx, r0:r1, lanes]))
    finish_level2(2, store_level2(act2, HALF))
    halo_start(act2, HALF, 4, 2)

    def conv640(ref, first, index):
        level2_taps(ref[HALF:HALF + TILE, :], unit_rows(first, (1,)))
        halo_wait(ref, HALF, SIDE, index)
        level2_taps(stack_rows(ref, TILE, HALF, (0, 2)), unit_rows(first, (0, 2)), add=True)

    wait_units(E2B, MA)
    conv640(act2, E2B, 2)
    finish_level2(3, store_s2)
    halo_start(p2, W3, 2, 3)
    halo_start(s2, HALF, 4, 4)
    refill((E2B, MA))

    x_index3 = column_index(HALF, W3)
    not_first3 = x_index3 > 0
    not_last3 = x_index3 < 31

    def finish_level3(bias_row, ref, start):
        def body(block, carry):
            lanes = pl.ds(pl.multiple_of(block * LANE, LANE), LANE)
            value = pl3[1, SUB:72, lanes] + jnp.where(not_first3, pl3[0, 7:71, lanes], 0.0)
            value = value + jnp.where(not_last3, pl3[2, 9:73, lanes], 0.0)
            ref[start:start + HALF, lanes] = relu(value + bias[bias_row:bias_row + 1, lanes]).astype(BF16)
            return carry

        lax.fori_loop(0, 10, body, 0)

    def slot_of(index):
        return lax.rem(index, RING)

    def wide(first):
        return cat_lanes([ring[slot_of(first)], ring[slot_of(first + 1)]])

    def add_rows(dx, value):
        pl3[dx, SUB:72, :] = pl3[dx, SUB:72, :] + value

    wait_units(MA, MB)
    for dx in TAPS:
        pl3[dx, SUB:72, :] = dot(p2[W3:3 * W3, :], wide(MA + 2 * dx))
    halo_wait(p2, W3, 2, 3)
    left = cat_lanes([p2[:HALF, :], p2[HALF:LANE, :]])
    for dx in TAPS:
        add_rows(dx, dot(left, cat_rows([wide(MA + 6 + 2 * dx), wide(MA + 12 + 2 * dx)])))
    finish_level3(4, act3, W3)
    halo_start(act3, W3, 2, 5)
    refill((MA, MB))

    for group, dy in enumerate(ROWS):
        def mid_b(dx, carry):
            first = MB + (group * 3 + dx) * SIDE
            for part in QUAD:
                slot = slot_of(first + part)
                pltpu.make_async_copy(h_e2b.at[0], ring.at[slot], sem_r.at[slot]).wait()
            value = dot(act3[dy * W3:dy * W3 + HALF, :], cat_rows([wide(first), wide(first + 2)]))
            if group:
                add_rows(dx, value)
            else:
                pl3[dx, SUB:72, :] = value
            return carry

        if group == 1:
            halo_wait(act3, W3, 2, 5)
        lax.fori_loop(0, 3, mid_b, 0)
        refill((MB + group * 12, MB + group * 12 + 12))
    finish_level3(5, mid, 0)

    wait_units(UP2, D2A)
    for tap in QUAD:
        p, q = tap // 2, tap % 2
        left = mid[...]
        for a, b in NTILES:
            right = cat_rows(ring[(UP2 + 2 * tap + part) % RING, :, a:b] for part in PAIR)
            part = dot(left, right)
            for i in PAIR:
                for c0 in range(a, b, LANE):
                    up_f32[pl.ds(c0 * 2 + (2 * i + p) * HALF + q, W3, stride=2), :] = part[W3 * i:W3 * i + W3, c0 - a:c0 - a + LANE]
    for block in range(5):
        u2[HALF:C1, block * LANE:block * LANE + LANE] = up_f32[block * TILE:block * TILE + TILE, :].astype(BF16)
    halo_start(u2, HALF, 4, 6)
    refill((UP2, D2A))
    halo_wait(s2, HALF, SIDE, 4)

    wait_units(D2A, D2A + TAP9)
    level2_taps(stack_rows(s2, TILE, HALF), unit_rows(D2A))
    refill((D2A, D2A + TAP9))
    wait_units(D2A + TAP9, D2B)
    halo_wait(u2, HALF, SIDE, 6)
    level2_taps(stack_rows(u2, TILE, HALF), unit_rows(D2A + TAP9), add=True)
    refill((D2A + TAP9, D2B))
    finish_level2(6, store_level2(act4, HALF))
    halo_start(act4, HALF, 4, 7)
    wait_units(D2B, UP1)
    conv640(act4, D2B, 7)
    finish_level2(7, store_level2(d2, 0))

    def half1(tap):
        return slice((tap % 2) * C1, (tap % 2) * C1 + C1)

    refill((D2B, UP1))
    wait_units(UP1, D1A)
    for tap in QUAD:
        p, q = tap // 2, tap % 2
        left = d2[...]
        up = dot_t(left, ring[(UP1 + tap // 2) % RING, half1(tap), :])
        for a, b in ((0, TILE), (TILE, C1)):
            part = up[:, a:b]
            for i in QUAD:
                for c0 in range(a, b, LANE):
                    c1 = min(b, c0 + LANE)
                    up_f32[pl.ds(c0 * SUB + (2 * i + p) * LANE + q, HALF, stride=2), :c1 - c0] = part[HALF * i:HALF * i + HALF, c0 - a:c1 - a]
    for block in TAPS:
        value = up_f32[block * 1024:block * 1024 + 1024, :].astype(BF16)
        if block < 2:
            cat1[LANE:TILE + 7 * LANE, blocks_of(block)] = value
        else:
            cat1[LANE:TILE + 7 * LANE, TILE:C1] = value[:, :HALF]
    halo_start(cat1, LANE, SUB, 8, U1_LANES)

    def d1a_tap(tap):
        return ring[(D1A + tap // 2) % RING, half1(tap), :]

    wait_units(D1A, UNITS)
    conv_cat(8, store_level1(act5), (1, 1))
    halo_wait(cat1, LANE, SUB, 1, S1_LANES)
    halo_wait(cat1, LANE, SUB, 8, U1_LANES)
    conv_cat(8, store_level1(act5), (0, 3))
    halo_start(act5, LANE, SUB, 9)
    cp_d1b.wait()
    build_tail(v_e1b, 0, t_e1b)

    def finish_head(i, pieces):
        head = dot_t(w_out[...].astype(BF16), cat_lanes(piece.astype(BF16) for piece in pieces))
        ys[pl.ds(i, 1)] = head[None]

    conv_narrow(act5, TAP9, finish_head, (1, 1))
    halo_wait(act5, LANE, SUB, 9)
    conv_narrow(act5, TAP9, finish_head, (0, 3))

    for c in QUAD:
        packed = jnp.zeros((SUB, LANE), F32)
        for y in range(SUB):
            line = ys[y // 2, :, (y % 2) * LANE:(y % 2) * LANE + LANE]
            slot = y % 4
            shift = (W3 * slot - W3 * c) % LANE
            line = turn(line, shift)
            if y >= 4:
                line = pltpu.roll(line, 4, 0)
            place = AND(AND(lanes8 >= W3 * slot, lanes8 < W3 * slot + W3), (sub8 >= 4) if y >= 4 else (sub8 < 4))
            packed = jnp.where(place, line, packed)
        ysend[c] = packed

    def y_copy(c):
        return remote(ysend.at[c], yrecv.at[k_me], y_send.at[c], y_recv.at[k_me], c, col)

    for c in QUAD:
        here = is_me(c, col)

        @pl.when(NOT(here))
        def _():
            y_copy(c).start()

        @pl.when(here)
        def _():
            yrecv[pl.ds(k_me, 1)] = ysend[c][None]

    for k in QUAD:
        from_col, from_row = owner(4 * row + k)

        @pl.when(NOT(is_me(from_col, from_row)))
        def _():
            remote(ysend.at[0], yrecv.at[k], y_send.at[0], y_recv.at[k], col, row).wait_recv()

    for c in QUAD:
        @pl.when(NOT(is_me(c, col)))
        def _():
            y_copy(c).wait_send()

    for k in QUAD:
        for low in QUAD:
            line = turn(yrecv[k], (LANE - low * W3) % LANE)
            for high in PAIR:
                out_ref[k * SUB + high * SIDE + low] = line[high * SIDE:high * SIDE + SIDE, :W3]


def network(x, w_e1a, w_head, *rest):
    vmem = pl.BlockSpec(memory_space=pltpu.VMEM)
    hbm = pl.BlockSpec(memory_space=pl.ANY)
    dma = pltpu.SemaphoreType.DMA
    scratch = [pltpu.VMEM(shape, F32) for shape in ((5 * SUB, SUB, LANE), (5, SUB, LANE), (SIDE, 2, SUB, LANE), (SIDE, 1, SUB, LANE), (TILE, LANE))]
    level1, level2 = 10 * LANE, 6 * HALF
    scratch += [pltpu.VMEM(shape, BF16) for shape in (
        (level1, C1P), (level1, C2), (level2, C1P), (level2, C2), (level2, C2), (LANE, C2), (LANE, C3), (HALF, C3),
        (level2, C2), (level2, C2), (TILE, C2), (level1, C1P),
        (TAP9, C1, C1), (TAP9, C1, C2), (3, C1, TILE), (RING, C2, C2))]
    scratch += [pltpu.VMEM(shape, F32) for shape in (
        (10, C3), (48, C1P), (SUB, C1P),
        (3, MARGIN, TILE), (MARGIN, TILE), (3, MARGIN, C2), (3, 80, C3), (MARGIN, 1024),
        (LANE, LANE), (3072, LANE), (SIDE, SUB, TILE), (SIDE, SUB, LANE), (SIDE, SUB, LANE))]
    scratch += [dma(shape) for shape in ((3,), (RING,), (SIDE,), (SIDE,), (2,), (SIDE,), (10, 2), (10, 2), (SIDE,), (SIDE,))]
    return pl.pallas_call(
        kernel,
        out_shape=jax.ShapeDtypeStruct((W3, SIDE, W3), F32),
        in_specs=[vmem] * 13 + [hbm] * 11,
        out_specs=vmem,
        scratch_shapes=scratch,
        compiler_params=pltpu.CompilerParams(collective_id=0, has_side_effects=True, vmem_limit_bytes=67043328),
        name="unet",
    )(x, w_e1a, w_head, *rest)


def solution(mesh):
    tile_spec = P(("data", "row"), "col", None)

    def device_body(tile, *params):
        (w_enc1a, b_enc1a, w_enc1b, b_enc1b, w_enc2a, b_enc2a, w_enc2b, b_enc2b,
         w_mid_a, b_mid_a, w_mid_b, b_mid_b, w_up2, w_dec2a, b_dec2a, w_dec2b, b_dec2b,
         w_up1, w_dec1a, b_dec1a, w_dec1b, b_dec1b, w_head, b_head) = params
        biases = (b_enc1a, b_enc1b, b_enc2a, b_enc2b, b_mid_a, b_mid_b, b_dec2a, b_dec2b, b_dec1a, b_dec1b)

        def taps(weight):
            return weight.reshape(-1, weight.shape[2], weight.shape[3])

        def turned(weight):
            return jnp.swapaxes(weight, 2, 3).reshape(-1, weight.shape[2])

        weights = [taps(w) for w in (w_enc1b, w_enc2a, w_enc2b, w_mid_a, w_mid_b, w_up2, w_dec2a, w_dec2b)]
        weights += [turned(w_up1), turned(w_dec1a), taps(w_dec1b)]
        packed = network(jnp.transpose(tile, (0, 2, 1)), taps(w_enc1a), w_head.T, *biases, *weights)
        return jnp.transpose(packed, (0, 2, 1)) + b_head

    def program(image, *params):
        mapped = jax.shard_map(device_body, mesh=mesh, in_specs=(tile_spec,) + tuple([P()] * len(params)), out_specs=tile_spec, check_vma=False)
        return mapped(image, *params)

    return program
```

```python
import jax
import jax.numpy as jnp
from jax import lax
from jax.experimental import pallas as pl
from jax.experimental.pallas import tpu as pltpu
from jax.sharding import PartitionSpec as P

F32 = jnp.float32
BF16 = jnp.bfloat16
STRIPS = 16
LAST = STRIPS - 1
SIDE = 4
SUB, LANE = 8, 128
TILE, HALF = 2 * LANE, LANE // 2
C1, C2, C3, C1P = 320, 640, 1280, 384
W3 = 32
END = SUB + TILE
MARGIN = END + SUB
TAPS = range(3)
PAIR = range(2)
QUAD = range(SIDE)
TAP9 = 9
RING = 47
E2B, MA, MB, UP2, D2A, D2B, UP1, D1A, UNITS = 0, 9, 27, 63, 71, 89, 98, 100, 105
ROWS = (1, 0, 2)
NOT = jnp.logical_not
AND = jnp.logical_and
OR = jnp.logical_or
MESH_ID = pl.DeviceIdType.MESH


def dot(lhs, rhs):
    return jnp.dot(lhs, rhs, preferred_element_type=F32)


def relu(value):
    return jnp.maximum(value, 0.0)


def dot_t(lhs, rhs):
    return lax.dot_general(lhs, rhs, (((1,), (1,)), ((), ())), preferred_element_type=F32)


def cat_lanes(parts):
    return jnp.concatenate(list(parts), axis=1)


def cat_rows(parts):
    return jnp.concatenate(list(parts), axis=0)


def turn(value, amount=HALF):
    return value if amount == 0 else pltpu.roll(value, amount, 1)


def lane_mask(shape, below):
    return lax.broadcasted_iota(jnp.int32, shape, 1) < below


def column_index(rows, width):
    return lax.rem(lax.broadcasted_iota(jnp.int32, (rows, LANE), 0), width)


def kernel(x_ref, w_e1a, w_head, *refs):
    biases, refs = refs[:10], refs[10:]
    (h_e1b, h_e2a, h_e2b, h_ma, h_mb, h_up2, h_d2a, h_d2b, h_up1, h_d1a, h_d1b,
     out_ref,
     xrows, xs, xb, xh, z, act1, cat1, p1, act2, s2, p2, act3, mid, u2, act4, d2, act5,
     v_e1b, v_e2a, t_e1b, ring, bias, w_first, w_out,
     pm, pt, pl2, pl3, pd1, pool, up_f32, ys, ysend, yrecv,
     sem_w, sem_r, x_send, x_recv, h_send, h_recv, e_send, e_recv, y_send, y_recv) = refs
    col = lax.axis_index("col")
    row = lax.axis_index("row")
    data = lax.axis_index("data")

    def owner(strip):
        strip_col = strip // 4
        k = strip % 4
        return strip_col, k + (strip_col % 2) * (3 - 2 * k)

    def device(strip_col, strip_row):
        return (data, strip_col, strip_row)

    k_me = row + (col % 2) * (3 - 2 * row)
    me = 4 * col + k_me

    barrier = pltpu.get_barrier_semaphore()
    for strip in range(1, STRIPS):
        other_col, other_row = owner((me + strip) % STRIPS)
        pl.semaphore_signal(barrier, inc=1, device_id=device(other_col, other_row), device_id_type=MESH_ID)

    def whole(src, dst, index):
        return pltpu.make_async_copy(src, dst, sem_w.at[index])

    cp_e1b = whole(h_e1b, v_e1b, 0)
    cp_e2a = whole(h_e2a, v_e2a, 1)
    cp_d1b = whole(h_d1b, v_e1b, 2)

    def half(index):
        return pl.ds((index % 2) * C2, C2)

    def unit(index):
        slot = index % RING
        dst = ring.at[slot]
        if index < MA:
            src = h_e2b.at[(index % 3) * 3 + index // 3]
        elif index < MB:
            tap = (index - MA) // 2
            src = h_ma.at[ROWS[tap // 3] * 3 + tap % 3, :, half(index - MA)]
        elif index < UP2:
            local = index - MB
            tap = local // 4
            src = h_mb.at[ROWS[tap // 3] * 3 + tap % 3, half(local // 2), half(local)]
        elif index < D2A:
            local = index - UP2
            src = h_up2.at[local // 2, half(local)]
        elif index < D2B:
            local = (index - D2A) % TAP9
            src = h_d2a.at[(local % 3) * 3 + local // 3, half((D2B - 1 - index) // TAP9)]
        elif index < UP1:
            local = index - D2B
            src = h_d2b.at[(local % 3) * 3 + local // 3]
        elif index < D1A:
            src = h_up1.at[pl.ds((index - UP1) * C2, C2)]
        elif index < UNITS - 1:
            src = h_d1a.at[pl.ds((index - D1A) * C2, C2)]
        else:
            src = h_d1a.at[pl.ds((index - D1A) * C2, C1)]
            dst = ring.at[slot, pl.ds(0, C1)]
        return pltpu.make_async_copy(src, dst, sem_r.at[slot])

    def wait_units(first, last):
        for index in range(first, last):
            unit(index).wait()

    def refill(done):
        for index in range(done[0] + RING, min(done[1] + RING, UNITS)):
            unit(index).start()

    cp_e1b.start()
    cp_e2a.start()
    for index in range(MA):
        unit(index).start()

    bias[...] = jnp.zeros_like(bias)
    for index, ref in enumerate(biases):
        bias[index:index + 1, :ref.shape[0]] = ref[...].reshape(1, ref.shape[0])
    w_first[...] = jnp.zeros_like(w_first)
    for tap in range(TAP9):
        at = (tap // 3) * STRIPS + (tap % 3) * SIDE
        w_first[at:at + SIDE, :C1] = w_e1a[tap].astype(F32)
    w_out[...] = jnp.zeros_like(w_out)
    w_out[:SIDE, :C1] = w_head[...].astype(F32)

    xrows[...] = jnp.zeros_like(xrows)
    xrows[2:2 + W3, :SIDE, :W3] = x_ref[...].astype(F32)

    def pack(group, carry):
        packed = jnp.zeros((SUB, LANE), F32)
        for j in range(SUB):
            line = turn(xrows[group * SUB + j], (j % SIDE) * W3)
            packed = packed + (line if j < SIDE else pltpu.roll(line, SIDE, 0))
        xs[pl.ds(group, 1)] = packed[None]
        return carry

    lax.fori_loop(0, 5, pack, 0)
    pl.semaphore_wait(barrier, LAST)

    def build_tail(weights, base, tail):
        def body(dy, carry):
            parts = [weights[dy * 3 + dx, base:base + C1, TILE:C1].astype(F32) for dx in TAPS]
            zero = jnp.zeros((C1, HALF), F32)
            pair = cat_lanes(parts[:2])
            last = cat_lanes([parts[2], zero])
            tail[dy, :, :LANE] = pair.astype(BF16)
            tail[dy, :, LANE:TILE] = last.astype(BF16)
            return carry

        lax.fori_loop(0, 3, body, 0)


    def is_me(strip_col, strip_row):
        return AND(strip_col == col, strip_row == row)

    def remote(src, dst, send, recv, strip_col, strip_row):
        return pltpu.make_async_remote_copy(src_ref=src, dst_ref=dst, send_sem=send, recv_sem=recv,
                                            device_id=device(strip_col, strip_row), device_id_type=MESH_ID)

    for k in QUAD:
        to_col, to_row = owner(4 * row + k)
        here = is_me(to_col, to_row)
        copy = remote(xs.at[pl.ds(k, 2)], xb.at[col], x_send.at[k], x_recv.at[col], to_col, to_row)

        @pl.when(NOT(here))
        def _():
            copy.start()

        @pl.when(here)
        def _():
            xb[pl.ds(col, 1)] = xs[k:k + 2][None]

    def halo_target(strip):
        return owner(jnp.clip(strip, 0, LAST))

    for side, (strip, allowed, first) in enumerate(((4 * row - 1, row > 0, 0), (4 * row + 4, row < 3, SIDE))):
        to_col, to_row = halo_target(strip)
        here = is_me(to_col, to_row)
        copy = remote(xs.at[pl.ds(first, 1)], xh.at[col], h_send.at[side], h_recv.at[col], to_col, to_row)

        @pl.when(AND(allowed, NOT(here)))
        def _():
            copy.start()

        @pl.when(AND(allowed, here))
        def _():
            xh[pl.ds(col, 1)] = xs[first:first + 1][None]

    cp_e1b.wait()
    build_tail(v_e1b, 0, t_e1b)
    for index in range(MA, RING):
        unit(index).start()

    for c in QUAD:
        @pl.when(NOT(is_me(c, row) & (row == col)))
        def _():
            remote(xs.at[pl.ds(0, 2)], xb.at[c], x_send.at[0], x_recv.at[c], col, row).wait_recv()

    has_top = AND(k_me == 0, col > 0)
    has_bottom = AND(k_me == 3, col < 3)
    halo_row = jnp.where(has_top, col - 1, col + 1)
    for c in QUAD:
        own = AND(c == col, row == halo_row)

        @pl.when(AND(OR(has_top, has_bottom), NOT(own)))
        def _():
            remote(xs.at[pl.ds(0, 1)], xh.at[c], h_send.at[0], h_recv.at[c], col, row).wait_recv()

    for k in QUAD:
        to_col, to_row = owner(4 * row + k)

        @pl.when(NOT(is_me(to_col, to_row)))
        def _():
            remote(xs.at[pl.ds(k, 2)], xb.at[col], x_send.at[k], x_recv.at[col], to_col, to_row).wait_send()

    for side, (strip, allowed, first) in enumerate(((4 * row - 1, row > 0, 0), (4 * row + 4, row < 3, SIDE))):
        to_col, to_row = halo_target(strip)

        @pl.when(AND(allowed, NOT(is_me(to_col, to_row))))
        def _():
            remote(xs.at[pl.ds(first, 1)], xh.at[col], h_send.at[side], h_recv.at[col], to_col, to_row).wait_send()

    lanes8 = lax.broadcasted_iota(jnp.int32, (SUB, LANE), 1)
    sub8 = lax.broadcasted_iota(jnp.int32, (SUB, LANE), 0)
    z[...] = jnp.zeros_like(z)
    halo_place = (AND(has_top, lanes8 < HALF), AND(has_bottom, lanes8 >= HALF))
    for part in PAIR:
        place = AND(halo_place[part], sub8 < SIDE)
        blocks = [jnp.where(place, xh[c, 0], xb[c, part]) for c in QUAD]
        for group in QUAD:
            line = jnp.zeros((SUB, LANE), F32)
            for c in QUAD:
                inside = lanes8 // W3 == c
                line = jnp.where(inside, turn(blocks[c], (W3 * (c - group)) % LANE), line)
            for dx in TAPS:
                moved = line
                if dx == 0:
                    moved = jnp.where(lanes8 == 0, 0.0, turn(line, 1))
                elif dx == 2:
                    moved = jnp.where(lanes8 == LANE - 1, 0.0, turn(line, LANE - 1))
                for upper in range(2 - part):
                    at = (part * SUB + group + upper * SIDE) * STRIPS + dx * SIDE
                    z[at:at + SIDE, :] = moved[upper * SIDE:upper * SIDE + SIDE]

    def first_conv(pair, carry):
        weights = w_first[...].astype(BF16)
        for j in (2 * pair, 2 * pair + 1):
            taps = z[pl.ds(pl.multiple_of(j * STRIPS, STRIPS), 48), :].astype(BF16)
            value = lax.dot_general(taps, weights, (((0,), (0,)), ((), ())), preferred_element_type=F32)
            value = relu(value + bias[:1, :C1P])
            outside = OR(AND(me == 0, j == 0), AND(me == LAST, j == TAP9))
            value = jnp.where(outside, 0.0, value)
            act1[pl.ds(pl.multiple_of(j * LANE, LANE), LANE), :] = value.astype(BF16)
        return carry

    lax.fori_loop(0, 5, first_conv, 0)

    up_col, up_row = owner(jnp.maximum(me - 1, 0))
    down_col, down_row = owner(jnp.minimum(me + 1, LAST))

    def clear_borders(ref, width, height):
        @pl.when(me == 0)
        def _():
            ref[:width, :] = jnp.zeros((width, ref.shape[1]), BF16)

        @pl.when(me == LAST)
        def _():
            ref[(height + 1) * width:(height + 2) * width, :] = jnp.zeros((width, ref.shape[1]), BF16)

    for ref, width, height in ((cat1, LANE, SUB), (act5, LANE, SUB), (p1, HALF, SIDE), (act2, HALF, SIDE), (s2, HALF, SIDE),
                               (u2, HALF, SIDE), (act4, HALF, SIDE), (p2, W3, 2), (act3, W3, 2)):
        clear_borders(ref, width, height)

    def halo_copies(ref, width, height, index, lanes):
        to_up = remote(ref.at[pl.ds(width, width), lanes], ref.at[pl.ds((height + 1) * width, width), lanes],
                       e_send.at[index, 0], e_recv.at[index, 0], up_col, up_row)
        to_down = remote(ref.at[pl.ds(height * width, width), lanes], ref.at[pl.ds(0, width), lanes],
                         e_send.at[index, 1], e_recv.at[index, 1], down_col, down_row)
        return to_up, to_down

    def halo_start(ref, width, height, index, lanes=slice(None)):
        to_up, to_down = halo_copies(ref, width, height, index, lanes)

        @pl.when(me > 0)
        def _():
            to_up.start()

        @pl.when(me < LAST)
        def _():
            to_down.start()

    def halo_wait(ref, width, height, index, lanes=slice(None)):
        to_up, to_down = halo_copies(ref, width, height, index, lanes)

        @pl.when(me > 0)
        def _():
            to_down.wait_recv()
            to_up.wait_send()

        @pl.when(me < LAST)
        def _():
            to_up.wait_recv()
            to_down.wait_send()

    def narrow_lhs(ref, start, rows, width):
        mains = [ref[pl.ds(start + dy * width, rows), :TILE] for dy in TAPS]
        tails = [ref[pl.ds(start + dy * width, rows), TILE:C1P] for dy in TAPS]
        pair = (tails[0].astype(F32) + turn(tails[1].astype(F32))).astype(BF16)
        return cat_lanes(mains + [pair, tails[2][:, :HALF]])

    def narrow_rhs(load):
        return cat_rows([load(dy, 0, TILE) for dy in TAPS] + [load(dy, TILE, C1) for dy in TAPS])

    x_index = column_index(TILE, LANE)
    not_first = x_index > 0
    not_last = x_index < 127

    low_half = lane_mask((TILE, LANE), HALF)

    def shifted(ref, plane, left, right):
        first = left + jnp.where(not_first, ref[plane(0) + (slice(7, 263), right[0])], 0.0)
        return first + jnp.where(not_last, ref[plane(2) + (slice(9, 265), right[1])], 0.0)

    def blocks_of(block):
        return slice(block * LANE, block * LANE + LANE)

    def conv_narrow(ref, bias_row, finish, chunks):
        for side, i in enumerate(chunks):
            left = narrow_lhs(ref, i * TILE, TILE, LANE)
            for dx in TAPS:
                pm[side, dx, SUB:END, :] = dot(left, narrow_rhs(lambda dy, a, b: v_e1b[dy * 3 + dx, a:b, :TILE]))
            pt[side, SUB:END, :] = dot(left, narrow_rhs(lambda dy, a, b: t_e1b[dy, a:b, :]))
        for side, i in enumerate(chunks):
            pieces = []
            for block in PAIR:
                lanes = blocks_of(block)
                value = shifted(pm, lambda dx: (side, dx), pm[side, 1, SUB:END, lanes], (lanes, lanes))
                pieces.append(relu(value + bias[bias_row:bias_row + 1, lanes]))
            value = shifted(pt, lambda dx: (side,), turn(pt[side, SUB:END, :LANE]), (blocks_of(0), blocks_of(1)))
            value = relu(value + bias[bias_row:bias_row + 1, TILE:C1P])
            pieces.append(jnp.where(low_half, value, 0.0))
            finish(i, pieces)

    def conv_cat(bias_row, finish, chunks):
        for side, i in enumerate(chunks):
            start = i * TILE
            left = cat_lanes(cat1[pl.ds(start + dy * LANE, TILE), :] for dy in TAPS)
            right = cat_lanes(cat_rows(d1a_tap(dy * 3 + dx) for dx in TAPS) for dy in TAPS)
            pd1[side, SUB:END, :3 * C1] = dot_t(left, right)
        for side, i in enumerate(chunks):
            turned = [turn(pd1[side, SUB:END, blocks_of(2 + block)]) for block in TAPS]
            pieces = []
            for block in TAPS:
                middle = turned[block] if block == 2 else jnp.where(low_half, turned[block], turned[block + 1])
                value = shifted(pd1, lambda dx: (side,), middle, (blocks_of(block), blocks_of(5 + block) if block < 2 else slice(896, 1024)))
                value = relu(value + bias[bias_row:bias_row + 1, blocks_of(block)])
                pieces.append(value if block < 2 else jnp.where(low_half, value, 0.0))
            finish(i, pieces)

    def store_level1(ref):
        def finish(i, pieces):
            start = LANE + i * TILE
            for block in range(3):
                ref[pl.ds(start, TILE), block * LANE:block * LANE + LANE] = pieces[block].astype(BF16)
        return finish

    def finish_s1(i, pieces):
        at = pl.ds(LANE + i * TILE, TILE)
        turned = [turn(piece) for piece in pieces]
        cat1[at, TILE:C1P] = jnp.where(low_half, 0.0, turned[0]).astype(BF16)
        for block in PAIR:
            cat1[at, blocks_of(3 + block)] = jnp.where(low_half, turned[block], turned[block + 1]).astype(BF16)
        start = HALF + i * HALF
        for block in range(3):
            pool[:LANE, :] = jnp.maximum(pieces[block][:LANE], pieces[block][LANE:TILE])
            pooled = jnp.maximum(pool[pl.ds(0, HALF, stride=2), :], pool[pl.ds(1, HALF, stride=2), :])
            p1[pl.ds(start, HALF), block * LANE:block * LANE + LANE] = pooled.astype(BF16)

    S1_LANES = pl.ds(C1P, TILE)
    U1_LANES = pl.ds(0, C1P)
    conv_narrow(act1, 1, finish_s1, (0, 3))
    halo_start(p1, HALF, SIDE, 0)
    halo_start(cat1, LANE, SUB, 1, S1_LANES)
    conv_narrow(act1, 1, finish_s1, (1, 2))
    cp_d1b.start()

    x_index2 = column_index(TILE, HALF)
    not_first2 = x_index2 > 0
    not_last2 = x_index2 < 63

    def finish_level2(bias_row, store):
        def body(block, carry):
            lanes = pl.ds(pl.multiple_of(block * LANE, LANE), LANE)
            value = pl2[1, SUB:END, lanes] + jnp.where(not_first2, pl2[0, 7:263, lanes], 0.0)
            value = value + jnp.where(not_last2, pl2[2, 9:265, lanes], 0.0)
            store(lanes, relu(value + bias[bias_row:bias_row + 1, lanes]))
            return carry

        lax.fori_loop(0, 5, body, 0)

    def store_level2(ref, start):
        def store(lanes, value):
            ref[start:start + TILE, lanes] = value.astype(BF16)
        return store

    def store_s2(lanes, value):
        s2[HALF:C1, lanes] = value.astype(BF16)
        for i in PAIR:
            pool[:HALF, :] = jnp.maximum(value[LANE * i:LANE * i + HALF], value[LANE * i + HALF:LANE * i + LANE])
            pooled = jnp.maximum(pool[pl.ds(0, W3, stride=2), :], pool[pl.ds(1, W3, stride=2), :])
            p2[W3 + W3 * i:HALF + W3 * i, lanes] = pooled.astype(BF16)

    NTILES = ((0, TILE), (TILE, 2 * TILE), (2 * TILE, C2))
    TAIL = slice(2 * TILE, C2)

    def stack_rows(ref, rows, width, taps=TAPS):
        return cat_lanes(ref[dy * width:dy * width + rows, :] for dy in taps)

    def level2_taps(left, weights, add=False):
        def put(dx, lanes, value):
            pl2[dx, SUB:END, lanes] = pl2[dx, SUB:END, lanes] + value if add else value

        for dx in TAPS:
            for first, last in NTILES[:2]:
                lanes = slice(first, last)
                put(dx, lanes, dot(left, weights(dx, lanes)))
        pair = dot(left, cat_lanes(weights(dx, TAIL) for dx in PAIR))
        put(0, TAIL, pair[:, :LANE])
        put(1, TAIL, pair[:, LANE:])
        put(2, TAIL, dot(left, weights(2, TAIL)))

    def unit_rows(first, taps=TAPS):
        return lambda dx, lanes: cat_rows(ring[(first + dx * 3 + dy) % RING, :, lanes] for dy in taps)

    halo_wait(p1, HALF, 4, 0)
    cp_e2a.wait()

    level2_taps(narrow_lhs(p1, 0, TILE, HALF),
                lambda dx, lanes: narrow_rhs(lambda dy, r0, r1: v_e2a[dy * 3 + dx, r0:r1, lanes]))
    finish_level2(2, store_level2(act2, HALF))
    halo_start(act2, HALF, 4, 2)

    def conv640(ref, first, index):
        level2_taps(ref[HALF:HALF + TILE, :], unit_rows(first, (1,)))
        halo_wait(ref, HALF, SIDE, index)
        level2_taps(stack_rows(ref, TILE, HALF, (0, 2)), unit_rows(first, (0, 2)), add=True)

    wait_units(E2B, MA)
    conv640(act2, E2B, 2)
    finish_level2(3, store_s2)
    halo_start(p2, W3, 2, 3)
    halo_start(s2, HALF, 4, 4)
    refill((E2B, MA))

    x_index3 = column_index(HALF, W3)
    not_first3 = x_index3 > 0
    not_last3 = x_index3 < 31

    def finish_level3(bias_row, ref, start):
        def body(block, carry):
            lanes = pl.ds(pl.multiple_of(block * LANE, LANE), LANE)
            value = pl3[1, SUB:72, lanes] + jnp.where(not_first3, pl3[0, 7:71, lanes], 0.0)
            value = value + jnp.where(not_last3, pl3[2, 9:73, lanes], 0.0)
            ref[start:start + HALF, lanes] = relu(value + bias[bias_row:bias_row + 1, lanes]).astype(BF16)
            return carry

        lax.fori_loop(0, 10, body, 0)

    def slot_of(index):
        return lax.rem(index, RING)

    def wide(first):
        return cat_lanes([ring[slot_of(first)], ring[slot_of(first + 1)]])

    def add_rows(dx, value):
        pl3[dx, SUB:72, :] = pl3[dx, SUB:72, :] + value

    wait_units(MA, MB)
    for dx in TAPS:
        pl3[dx, SUB:72, :] = dot(p2[W3:3 * W3, :], wide(MA + 2 * dx))
    cp_d1b.wait()
    build_tail(v_e1b, 0, t_e1b)
    halo_wait(p2, W3, 2, 3)
    left = cat_lanes([p2[:HALF, :], p2[HALF:LANE, :]])
    for dx in TAPS:
        add_rows(dx, dot(left, cat_rows([wide(MA + 6 + 2 * dx), wide(MA + 12 + 2 * dx)])))
    finish_level3(4, act3, W3)
    halo_start(act3, W3, 2, 5)
    refill((MA, MB))

    for group, dy in enumerate(ROWS):
        def mid_b(dx, carry):
            first = MB + (group * 3 + dx) * SIDE
            for part in QUAD:
                slot = slot_of(first + part)
                pltpu.make_async_copy(h_e2b.at[0], ring.at[slot], sem_r.at[slot]).wait()
            value = dot(act3[dy * W3:dy * W3 + HALF, :], cat_rows([wide(first), wide(first + 2)]))
            if group:
                add_rows(dx, value)
            else:
                pl3[dx, SUB:72, :] = value
            return carry

        if group == 1:
            halo_wait(act3, W3, 2, 5)
        lax.fori_loop(0, 3, mid_b, 0)
        refill((MB + group * 12, MB + group * 12 + 12))
    finish_level3(5, mid, 0)

    wait_units(UP2, D2A)
    for tap in QUAD:
        p, q = tap // 2, tap % 2
        left = mid[...]
        for a, b in NTILES:
            right = cat_rows(ring[(UP2 + 2 * tap + part) % RING, :, a:b] for part in PAIR)
            part = dot(left, right)
            for i in PAIR:
                for c0 in range(a, b, LANE):
                    up_f32[pl.ds(c0 * 2 + (2 * i + p) * HALF + q, W3, stride=2), :] = part[W3 * i:W3 * i + W3, c0 - a:c0 - a + LANE]
    for block in range(5):
        u2[HALF:C1, block * LANE:block * LANE + LANE] = up_f32[block * TILE:block * TILE + TILE, :].astype(BF16)
    halo_start(u2, HALF, 4, 6)
    refill((UP2, D2A))
    halo_wait(s2, HALF, SIDE, 4)

    wait_units(D2A, D2A + TAP9)
    level2_taps(stack_rows(s2, TILE, HALF), unit_rows(D2A))
    refill((D2A, D2A + TAP9))
    wait_units(D2A + TAP9, D2B)
    halo_wait(u2, HALF, SIDE, 6)
    level2_taps(stack_rows(u2, TILE, HALF), unit_rows(D2A + TAP9), add=True)
    refill((D2A + TAP9, D2B))
    finish_level2(6, store_level2(act4, HALF))
    halo_start(act4, HALF, 4, 7)
    wait_units(D2B, UP1)
    conv640(act4, D2B, 7)
    finish_level2(7, store_level2(d2, 0))

    def half1(tap):
        return slice((tap % 2) * C1, (tap % 2) * C1 + C1)

    refill((D2B, UP1))
    wait_units(UP1, D1A)
    for tap in QUAD:
        p, q = tap // 2, tap % 2
        left = d2[...]
        up = dot_t(left, ring[(UP1 + tap // 2) % RING, half1(tap), :])
        for a, b in ((0, TILE), (TILE, C1)):
            part = up[:, a:b]
            for i in QUAD:
                for c0 in range(a, b, LANE):
                    c1 = min(b, c0 + LANE)
                    up_f32[pl.ds(c0 * SUB + (2 * i + p) * LANE + q, HALF, stride=2), :c1 - c0] = part[HALF * i:HALF * i + HALF, c0 - a:c1 - a]
    for block in TAPS:
        value = up_f32[block * 1024:block * 1024 + 1024, :].astype(BF16)
        if block < 2:
            cat1[LANE:TILE + 7 * LANE, blocks_of(block)] = value
        else:
            cat1[LANE:TILE + 7 * LANE, TILE:C1] = value[:, :HALF]
    halo_start(cat1, LANE, SUB, 8, U1_LANES)

    def d1a_tap(tap):
        return ring[(D1A + tap // 2) % RING, half1(tap), :]

    wait_units(D1A, UNITS)
    conv_cat(8, store_level1(act5), (1, 2))
    halo_wait(cat1, LANE, SUB, 1, S1_LANES)
    halo_wait(cat1, LANE, SUB, 8, U1_LANES)
    conv_cat(8, store_level1(act5), (0, 3))
    halo_start(act5, LANE, SUB, 9)

    def finish_head(i, pieces):
        head = dot_t(w_out[...].astype(BF16), cat_lanes(piece.astype(BF16) for piece in pieces))
        ys[pl.ds(i, 1)] = head[None]

    conv_narrow(act5, TAP9, finish_head, (1, 2))
    halo_wait(act5, LANE, SUB, 9)
    conv_narrow(act5, TAP9, finish_head, (0, 3))

    for c in QUAD:
        packed = jnp.zeros((SUB, LANE), F32)
        for y in range(SUB):
            line = ys[y // 2, :, (y % 2) * LANE:(y % 2) * LANE + LANE]
            slot = y % 4
            shift = (W3 * slot - W3 * c) % LANE
            line = turn(line, shift)
            if y >= 4:
                line = pltpu.roll(line, 4, 0)
            place = AND(AND(lanes8 >= W3 * slot, lanes8 < W3 * slot + W3), (sub8 >= 4) if y >= 4 else (sub8 < 4))
            packed = jnp.where(place, line, packed)
        ysend[c] = packed

    def y_copy(c):
        return remote(ysend.at[c], yrecv.at[k_me], y_send.at[c], y_recv.at[k_me], c, col)

    for c in QUAD:
        here = is_me(c, col)

        @pl.when(NOT(here))
        def _():
            y_copy(c).start()

        @pl.when(here)
        def _():
            yrecv[pl.ds(k_me, 1)] = ysend[c][None]

    for k in QUAD:
        from_col, from_row = owner(4 * row + k)

        @pl.when(NOT(is_me(from_col, from_row)))
        def _():
            remote(ysend.at[0], yrecv.at[k], y_send.at[0], y_recv.at[k], col, row).wait_recv()

    for c in QUAD:
        @pl.when(NOT(is_me(c, col)))
        def _():
            y_copy(c).wait_send()

    for k in QUAD:
        for low in QUAD:
            line = turn(yrecv[k], (LANE - low * W3) % LANE)
            for high in PAIR:
                out_ref[k * SUB + high * SIDE + low] = line[high * SIDE:high * SIDE + SIDE, :W3]


def network(x, w_e1a, w_head, *rest):
    vmem = pl.BlockSpec(memory_space=pltpu.VMEM)
    hbm = pl.BlockSpec(memory_space=pl.ANY)
    dma = pltpu.SemaphoreType.DMA
    scratch = [pltpu.VMEM(shape, F32) for shape in ((5 * SUB, SUB, LANE), (5, SUB, LANE), (SIDE, 2, SUB, LANE), (SIDE, 1, SUB, LANE), (TILE, LANE))]
    level1, level2 = 10 * LANE, 6 * HALF
    scratch += [pltpu.VMEM(shape, BF16) for shape in (
        (level1, C1P), (level1, C2), (level2, C1P), (level2, C2), (level2, C2), (LANE, C2), (LANE, C3), (HALF, C3),
        (level2, C2), (level2, C2), (TILE, C2), (level1, C1P),
        (TAP9, C1, C1), (TAP9, C1, C2), (3, C1, TILE), (RING, C2, C2))]
    scratch += [pltpu.VMEM(shape, F32) for shape in (
        (10, C3), (48, C1P), (SUB, C1P),
        (2, 3, MARGIN, TILE), (2, MARGIN, TILE), (3, MARGIN, C2), (3, 80, C3), (2, MARGIN, 1024),
        (LANE, LANE), (3072, LANE), (SIDE, SUB, TILE), (SIDE, SUB, LANE), (SIDE, SUB, LANE))]
    scratch += [dma(shape) for shape in ((3,), (RING,), (SIDE,), (SIDE,), (2,), (SIDE,), (10, 2), (10, 2), (SIDE,), (SIDE,))]
    return pl.pallas_call(
        kernel,
        out_shape=jax.ShapeDtypeStruct((W3, SIDE, W3), F32),
        in_specs=[vmem] * 13 + [hbm] * 11,
        out_specs=vmem,
        scratch_shapes=scratch,
        compiler_params=pltpu.CompilerParams(collective_id=0, has_side_effects=True, vmem_limit_bytes=67043328),
        name="unet",
    )(x, w_e1a, w_head, *rest)


def solution(mesh):
    tile_spec = P(("data", "row"), "col", None)

    def device_body(tile, *params):
        (w_enc1a, b_enc1a, w_enc1b, b_enc1b, w_enc2a, b_enc2a, w_enc2b, b_enc2b,
         w_mid_a, b_mid_a, w_mid_b, b_mid_b, w_up2, w_dec2a, b_dec2a, w_dec2b, b_dec2b,
         w_up1, w_dec1a, b_dec1a, w_dec1b, b_dec1b, w_head, b_head) = params
        biases = (b_enc1a, b_enc1b, b_enc2a, b_enc2b, b_mid_a, b_mid_b, b_dec2a, b_dec2b, b_dec1a, b_dec1b)

        def taps(weight):
            return weight.reshape(-1, weight.shape[2], weight.shape[3])

        def turned(weight):
            return jnp.swapaxes(weight, 2, 3).reshape(-1, weight.shape[2])

        weights = [taps(w) for w in (w_enc1b, w_enc2a, w_enc2b, w_mid_a, w_mid_b, w_up2, w_dec2a, w_dec2b)]
        weights += [turned(w_up1), turned(w_dec1a), taps(w_dec1b)]
        packed = network(jnp.transpose(tile, (0, 2, 1)), taps(w_enc1a), w_head.T, *biases, *weights)
        return jnp.transpose(packed, (0, 2, 1)) + b_head

    def program(image, *params):
        mapped = jax.shard_map(device_body, mesh=mesh, in_specs=(tile_spec,) + tuple([P()] * len(params)), out_specs=tile_spec, check_vma=False)
        return mapped(image, *params)

    return program
```

```python
import jax
import jax.numpy as jnp
from jax import lax
from jax.experimental import pallas as pl
from jax.experimental.pallas import tpu as pltpu
from jax.sharding import PartitionSpec as P

F32 = jnp.float32
BF16 = jnp.bfloat16
STRIPS = 16
LAST = STRIPS - 1
SIDE = 4
SUB, LANE = 8, 128
TILE, HALF = 2 * LANE, LANE // 2
C1, C2, C3, C1P = 320, 640, 1280, 384
W3 = 32
END = SUB + TILE
MARGIN = END + SUB
TAPS = range(3)
PAIR = range(2)
QUAD = range(SIDE)
TAP9 = 9
RING = 47
E2B, MA, MB, UP2, D2A, D2B, UP1, D1A, UNITS = 0, 9, 27, 63, 71, 89, 98, 100, 105
ROWS = (1, 0, 2)
NOT = jnp.logical_not
AND = jnp.logical_and
OR = jnp.logical_or
MESH_ID = pl.DeviceIdType.MESH


def dot(lhs, rhs):
    return jnp.dot(lhs, rhs, preferred_element_type=F32)


def relu(value):
    return jnp.maximum(value, 0.0)


def dot_t(lhs, rhs):
    return lax.dot_general(lhs, rhs, (((1,), (1,)), ((), ())), preferred_element_type=F32)


def cat_lanes(parts):
    return jnp.concatenate(list(parts), axis=1)


def cat_rows(parts):
    return jnp.concatenate(list(parts), axis=0)


def turn(value, amount=HALF):
    return value if amount == 0 else pltpu.roll(value, amount, 1)


def lane_mask(shape, below):
    return lax.broadcasted_iota(jnp.int32, shape, 1) < below


def column_index(rows, width):
    return lax.rem(lax.broadcasted_iota(jnp.int32, (rows, LANE), 0), width)


def kernel(x_ref, w_e1a, w_head, *refs):
    biases, refs = refs[:10], refs[10:]
    (h_e1b, h_e2a, h_e2b, h_ma, h_mb, h_up2, h_d2a, h_d2b, h_up1, h_d1a, h_d1b,
     out_ref,
     xrows, xs, xb, xh, z, act1, cat1, p1, act2, s2, p2, act3, mid, u2, act4, d2, act5,
     v_e1b, v_e2a, t_e1b, ring, bias, w_first, w_out,
     pm, pt, pl2, pl3, pd1, pool, up_f32, ys, ysend, yrecv,
     sem_w, sem_r, x_send, x_recv, h_send, h_recv, e_send, e_recv, y_send, y_recv) = refs
    col = lax.axis_index("col")
    row = lax.axis_index("row")
    data = lax.axis_index("data")

    def owner(strip):
        strip_col = strip // 4
        k = strip % 4
        return strip_col, k + (strip_col % 2) * (3 - 2 * k)

    def device(strip_col, strip_row):
        return (data, strip_col, strip_row)

    k_me = row + (col % 2) * (3 - 2 * row)
    me = 4 * col + k_me

    barrier = pltpu.get_barrier_semaphore()
    for strip in range(1, STRIPS):
        other_col, other_row = owner((me + strip) % STRIPS)
        pl.semaphore_signal(barrier, inc=1, device_id=device(other_col, other_row), device_id_type=MESH_ID)

    def whole(src, dst, index):
        return pltpu.make_async_copy(src, dst, sem_w.at[index])

    cp_e1b = whole(h_e1b, v_e1b, 0)
    cp_e2a = whole(h_e2a, v_e2a, 1)
    cp_d1b = whole(h_d1b, v_e1b, 2)

    def half(index):
        return pl.ds((index % 2) * C2, C2)

    def unit(index):
        slot = index % RING
        dst = ring.at[slot]
        if index < MA:
            src = h_e2b.at[(index % 3) * 3 + index // 3]
        elif index < MB:
            tap = (index - MA) // 2
            src = h_ma.at[ROWS[tap // 3] * 3 + tap % 3, :, half(index - MA)]
        elif index < UP2:
            local = index - MB
            tap = local // 4
            src = h_mb.at[ROWS[tap // 3] * 3 + tap % 3, half(local // 2), half(local)]
        elif index < D2A:
            local = index - UP2
            src = h_up2.at[local // 2, half(local)]
        elif index < D2B:
            local = (index - D2A) % TAP9
            src = h_d2a.at[(local % 3) * 3 + local // 3, half((D2B - 1 - index) // TAP9)]
        elif index < UP1:
            local = index - D2B
            src = h_d2b.at[(local % 3) * 3 + local // 3]
        elif index < D1A:
            src = h_up1.at[pl.ds((index - UP1) * C2, C2)]
        elif index < UNITS - 1:
            src = h_d1a.at[pl.ds((index - D1A) * C2, C2)]
        else:
            src = h_d1a.at[pl.ds((index - D1A) * C2, C1)]
            dst = ring.at[slot, pl.ds(0, C1)]
        return pltpu.make_async_copy(src, dst, sem_r.at[slot])

    def wait_units(first, last):
        for index in range(first, last):
            unit(index).wait()

    def refill(done):
        for index in range(done[0] + RING, min(done[1] + RING, UNITS)):
            unit(index).start()

    cp_e1b.start()
    cp_e2a.start()
    for index in range(MA):
        unit(index).start()

    bias[...] = jnp.zeros_like(bias)
    for index, ref in enumerate(biases):
        bias[index:index + 1, :ref.shape[0]] = ref[...].reshape(1, ref.shape[0])
    w_first[...] = jnp.zeros_like(w_first)
    for tap in range(TAP9):
        at = (tap // 3) * STRIPS + (tap % 3) * SIDE
        w_first[at:at + SIDE, :C1] = w_e1a[tap].astype(F32)
    w_out[...] = jnp.zeros_like(w_out)
    w_out[:SIDE, :C1] = w_head[...].astype(F32)

    xrows[...] = jnp.zeros_like(xrows)
    xrows[2:2 + W3, :SIDE, :W3] = x_ref[...].astype(F32)

    def pack(group, carry):
        packed = jnp.zeros((SUB, LANE), F32)
        for j in range(SUB):
            line = turn(xrows[group * SUB + j], (j % SIDE) * W3)
            packed = packed + (line if j < SIDE else pltpu.roll(line, SIDE, 0))
        xs[pl.ds(group, 1)] = packed[None]
        return carry

    lax.fori_loop(0, 5, pack, 0)
    pl.semaphore_wait(barrier, LAST)

    def build_tail(weights, base, tail):
        def body(dy, carry):
            parts = [weights[dy * 3 + dx, base:base + C1, TILE:C1].astype(F32) for dx in TAPS]
            zero = jnp.zeros((C1, HALF), F32)
            pair = cat_lanes(parts[:2])
            last = cat_lanes([parts[2], zero])
            tail[dy, :, :LANE] = pair.astype(BF16)
            tail[dy, :, LANE:TILE] = last.astype(BF16)
            return carry

        lax.fori_loop(0, 3, body, 0)


    def is_me(strip_col, strip_row):
        return AND(strip_col == col, strip_row == row)

    def remote(src, dst, send, recv, strip_col, strip_row):
        return pltpu.make_async_remote_copy(src_ref=src, dst_ref=dst, send_sem=send, recv_sem=recv,
                                            device_id=device(strip_col, strip_row), device_id_type=MESH_ID)

    for k in QUAD:
        to_col, to_row = owner(4 * row + k)
        here = is_me(to_col, to_row)
        copy = remote(xs.at[pl.ds(k, 2)], xb.at[col], x_send.at[k], x_recv.at[col], to_col, to_row)

        @pl.when(NOT(here))
        def _():
            copy.start()

        @pl.when(here)
        def _():
            xb[pl.ds(col, 1)] = xs[k:k + 2][None]

    def halo_target(strip):
        return owner(jnp.clip(strip, 0, LAST))

    for side, (strip, allowed, first) in enumerate(((4 * row - 1, row > 0, 0), (4 * row + 4, row < 3, SIDE))):
        to_col, to_row = halo_target(strip)
        here = is_me(to_col, to_row)
        copy = remote(xs.at[pl.ds(first, 1)], xh.at[col], h_send.at[side], h_recv.at[col], to_col, to_row)

        @pl.when(AND(allowed, NOT(here)))
        def _():
            copy.start()

        @pl.when(AND(allowed, here))
        def _():
            xh[pl.ds(col, 1)] = xs[first:first + 1][None]

    cp_e1b.wait()
    build_tail(v_e1b, 0, t_e1b)
    for index in range(MA, RING):
        unit(index).start()

    for c in QUAD:
        @pl.when(NOT(is_me(c, row) & (row == col)))
        def _():
            remote(xs.at[pl.ds(0, 2)], xb.at[c], x_send.at[0], x_recv.at[c], col, row).wait_recv()

    has_top = AND(k_me == 0, col > 0)
    has_bottom = AND(k_me == 3, col < 3)
    halo_row = jnp.where(has_top, col - 1, col + 1)
    for c in QUAD:
        own = AND(c == col, row == halo_row)

        @pl.when(AND(OR(has_top, has_bottom), NOT(own)))
        def _():
            remote(xs.at[pl.ds(0, 1)], xh.at[c], h_send.at[0], h_recv.at[c], col, row).wait_recv()

    for k in QUAD:
        to_col, to_row = owner(4 * row + k)

        @pl.when(NOT(is_me(to_col, to_row)))
        def _():
            remote(xs.at[pl.ds(k, 2)], xb.at[col], x_send.at[k], x_recv.at[col], to_col, to_row).wait_send()

    for side, (strip, allowed, first) in enumerate(((4 * row - 1, row > 0, 0), (4 * row + 4, row < 3, SIDE))):
        to_col, to_row = halo_target(strip)

        @pl.when(AND(allowed, NOT(is_me(to_col, to_row))))
        def _():
            remote(xs.at[pl.ds(first, 1)], xh.at[col], h_send.at[side], h_recv.at[col], to_col, to_row).wait_send()

    lanes8 = lax.broadcasted_iota(jnp.int32, (SUB, LANE), 1)
    sub8 = lax.broadcasted_iota(jnp.int32, (SUB, LANE), 0)
    z[...] = jnp.zeros_like(z)
    halo_place = (AND(has_top, lanes8 < HALF), AND(has_bottom, lanes8 >= HALF))
    for part in PAIR:
        place = AND(halo_place[part], sub8 < SIDE)
        blocks = [jnp.where(place, xh[c, 0], xb[c, part]) for c in QUAD]
        for group in QUAD:
            line = jnp.zeros((SUB, LANE), F32)
            for c in QUAD:
                inside = lanes8 // W3 == c
                line = jnp.where(inside, turn(blocks[c], (W3 * (c - group)) % LANE), line)
            for dx in TAPS:
                moved = line
                if dx == 0:
                    moved = jnp.where(lanes8 == 0, 0.0, turn(line, 1))
                elif dx == 2:
                    moved = jnp.where(lanes8 == LANE - 1, 0.0, turn(line, LANE - 1))
                for upper in range(2 - part):
                    at = (part * SUB + group + upper * SIDE) * STRIPS + dx * SIDE
                    z[at:at + SIDE, :] = moved[upper * SIDE:upper * SIDE + SIDE]

    def first_conv(pair, carry):
        weights = w_first[...].astype(BF16)
        for j in (2 * pair, 2 * pair + 1):
            taps = z[pl.ds(pl.multiple_of(j * STRIPS, STRIPS), 48), :].astype(BF16)
            value = lax.dot_general(taps, weights, (((0,), (0,)), ((), ())), preferred_element_type=F32)
            value = relu(value + bias[:1, :C1P])
            outside = OR(AND(me == 0, j == 0), AND(me == LAST, j == TAP9))
            value = jnp.where(outside, 0.0, value)
            act1[pl.ds(pl.multiple_of(j * LANE, LANE), LANE), :] = value.astype(BF16)
        return carry

    lax.fori_loop(0, 5, first_conv, 0)

    up_col, up_row = owner(jnp.maximum(me - 1, 0))
    down_col, down_row = owner(jnp.minimum(me + 1, LAST))

    def clear_borders(ref, width, height):
        @pl.when(me == 0)
        def _():
            ref[:width, :] = jnp.zeros((width, ref.shape[1]), BF16)

        @pl.when(me == LAST)
        def _():
            ref[(height + 1) * width:(height + 2) * width, :] = jnp.zeros((width, ref.shape[1]), BF16)

    for ref, width, height in ((cat1, LANE, SUB), (act5, LANE, SUB), (p1, HALF, SIDE), (act2, HALF, SIDE), (s2, HALF, SIDE),
                               (u2, HALF, SIDE), (act4, HALF, SIDE), (p2, W3, 2), (act3, W3, 2)):
        clear_borders(ref, width, height)

    def halo_copies(ref, width, height, index, lanes):
        to_up = remote(ref.at[pl.ds(width, width), lanes], ref.at[pl.ds((height + 1) * width, width), lanes],
                       e_send.at[index, 0], e_recv.at[index, 0], up_col, up_row)
        to_down = remote(ref.at[pl.ds(height * width, width), lanes], ref.at[pl.ds(0, width), lanes],
                         e_send.at[index, 1], e_recv.at[index, 1], down_col, down_row)
        return to_up, to_down

    odd = k_me % 2 == 1
    even = NOT(odd)
    far = (k_me % 2) * 3
    near = 3 - far
    ANY = (True, True)
    FAR = (even, odd)
    NEAR = (odd, even)

    def halo_start(ref, width, height, index, lanes=slice(None), sides=ANY):
        to_up, to_down = halo_copies(ref, width, height, index, lanes)

        @pl.when(AND(me > 0, sides[0]))
        def _():
            to_up.start()

        @pl.when(AND(me < LAST, sides[1]))
        def _():
            to_down.start()

    def halo_wait(ref, width, height, index, lanes=slice(None), sides=ANY):
        to_up, to_down = halo_copies(ref, width, height, index, lanes)

        @pl.when(AND(me > 0, sides[0]))
        def _():
            to_down.wait_recv()
            to_up.wait_send()

        @pl.when(AND(me < LAST, sides[1]))
        def _():
            to_up.wait_recv()
            to_down.wait_send()

    def narrow_lhs(ref, start, rows, width):
        mains = [ref[pl.ds(start + dy * width, rows), :TILE] for dy in TAPS]
        tails = [ref[pl.ds(start + dy * width, rows), TILE:C1P] for dy in TAPS]
        pair = (tails[0].astype(F32) + turn(tails[1].astype(F32))).astype(BF16)
        return cat_lanes(mains + [pair, tails[2][:, :HALF]])

    def narrow_rhs(load):
        return cat_rows([load(dy, 0, TILE) for dy in TAPS] + [load(dy, TILE, C1) for dy in TAPS])

    x_index = column_index(TILE, LANE)
    not_first = x_index > 0
    not_last = x_index < 127

    low_half = lane_mask((TILE, LANE), HALF)

    def shifted(ref, plane, left, right):
        first = left + jnp.where(not_first, ref[plane(0) + (slice(7, 263), right[0])], 0.0)
        return first + jnp.where(not_last, ref[plane(2) + (slice(9, 265), right[1])], 0.0)

    def scaled(i, step):
        return i * step if isinstance(i, int) else pl.multiple_of(i * step, step)

    def blocks_of(block):
        return slice(block * LANE, block * LANE + LANE)

    def conv_narrow(ref, bias_row, finish, chunks):
        for side, i in enumerate(chunks):
            left = narrow_lhs(ref, scaled(i, TILE), TILE, LANE)
            for dx in TAPS:
                pm[side, dx, SUB:END, :] = dot(left, narrow_rhs(lambda dy, a, b: v_e1b[dy * 3 + dx, a:b, :TILE]))
            pt[side, SUB:END, :] = dot(left, narrow_rhs(lambda dy, a, b: t_e1b[dy, a:b, :]))
        for side, i in enumerate(chunks):
            pieces = []
            for block in PAIR:
                lanes = blocks_of(block)
                value = shifted(pm, lambda dx: (side, dx), pm[side, 1, SUB:END, lanes], (lanes, lanes))
                pieces.append(relu(value + bias[bias_row:bias_row + 1, lanes]))
            value = shifted(pt, lambda dx: (side,), turn(pt[side, SUB:END, :LANE]), (blocks_of(0), blocks_of(1)))
            value = relu(value + bias[bias_row:bias_row + 1, TILE:C1P])
            pieces.append(jnp.where(low_half, value, 0.0))
            finish(i, pieces)

    def conv_cat(bias_row, finish, chunks):
        for side, i in enumerate(chunks):
            start = scaled(i, TILE)
            left = cat_lanes(cat1[pl.ds(start + dy * LANE, TILE), :] for dy in TAPS)
            right = cat_lanes(cat_rows(d1a_tap(dy * 3 + dx) for dx in TAPS) for dy in TAPS)
            pd1[side, SUB:END, :3 * C1] = dot_t(left, right)
        for side, i in enumerate(chunks):
            turned = [turn(pd1[side, SUB:END, blocks_of(2 + block)]) for block in TAPS]
            pieces = []
            for block in TAPS:
                middle = turned[block] if block == 2 else jnp.where(low_half, turned[block], turned[block + 1])
                value = shifted(pd1, lambda dx: (side,), middle, (blocks_of(block), blocks_of(5 + block) if block < 2 else slice(896, 1024)))
                value = relu(value + bias[bias_row:bias_row + 1, blocks_of(block)])
                pieces.append(value if block < 2 else jnp.where(low_half, value, 0.0))
            finish(i, pieces)

    def store_level1(ref):
        def finish(i, pieces):
            start = LANE + scaled(i, TILE)
            for block in range(3):
                ref[pl.ds(start, TILE), block * LANE:block * LANE + LANE] = pieces[block].astype(BF16)
        return finish

    def finish_s1(i, pieces):
        at = pl.ds(LANE + scaled(i, TILE), TILE)
        turned = [turn(piece) for piece in pieces]
        cat1[at, TILE:C1P] = jnp.where(low_half, 0.0, turned[0]).astype(BF16)
        for block in PAIR:
            cat1[at, blocks_of(3 + block)] = jnp.where(low_half, turned[block], turned[block + 1]).astype(BF16)
        start = HALF + scaled(i, HALF)
        for block in range(3):
            pool[:LANE, :] = jnp.maximum(pieces[block][:LANE], pieces[block][LANE:TILE])
            pooled = jnp.maximum(pool[pl.ds(0, HALF, stride=2), :], pool[pl.ds(1, HALF, stride=2), :])
            p1[pl.ds(start, HALF), block * LANE:block * LANE + LANE] = pooled.astype(BF16)

    S1_LANES = pl.ds(C1P, TILE)
    U1_LANES = pl.ds(0, C1P)
    conv_narrow(act1, 1, finish_s1, (far,))
    halo_start(p1, HALF, SIDE, 0, sides=FAR)
    conv_narrow(act1, 1, finish_s1, (near,))
    halo_start(p1, HALF, SIDE, 0, sides=NEAR)
    halo_start(cat1, LANE, SUB, 1, S1_LANES)
    conv_narrow(act1, 1, finish_s1, (1, 2))
    cp_d1b.start()

    x_index2 = column_index(TILE, HALF)
    not_first2 = x_index2 > 0
    not_last2 = x_index2 < 63

    def finish_level2(bias_row, store):
        def body(block, carry):
            lanes = pl.ds(pl.multiple_of(block * LANE, LANE), LANE)
            value = pl2[1, SUB:END, lanes] + jnp.where(not_first2, pl2[0, 7:263, lanes], 0.0)
            value = value + jnp.where(not_last2, pl2[2, 9:265, lanes], 0.0)
            store(lanes, relu(value + bias[bias_row:bias_row + 1, lanes]))
            return carry

        lax.fori_loop(0, 5, body, 0)

    def store_level2(ref, start):
        def store(lanes, value):
            ref[start:start + TILE, lanes] = value.astype(BF16)
        return store

    def store_s2(lanes, value):
        s2[HALF:C1, lanes] = value.astype(BF16)
        for i in PAIR:
            pool[:HALF, :] = jnp.maximum(value[LANE * i:LANE * i + HALF], value[LANE * i + HALF:LANE * i + LANE])
            pooled = jnp.maximum(pool[pl.ds(0, W3, stride=2), :], pool[pl.ds(1, W3, stride=2), :])
            p2[W3 + W3 * i:HALF + W3 * i, lanes] = pooled.astype(BF16)

    NTILES = ((0, TILE), (TILE, 2 * TILE), (2 * TILE, C2))
    TAIL = slice(2 * TILE, C2)

    def stack_rows(ref, rows, width, taps=TAPS):
        return cat_lanes(ref[dy * width:dy * width + rows, :] for dy in taps)

    def level2_taps(left, weights, add=False):
        def put(dx, lanes, value):
            pl2[dx, SUB:END, lanes] = pl2[dx, SUB:END, lanes] + value if add else value

        for dx in TAPS:
            for first, last in NTILES[:2]:
                lanes = slice(first, last)
                put(dx, lanes, dot(left, weights(dx, lanes)))
        pair = dot(left, cat_lanes(weights(dx, TAIL) for dx in PAIR))
        put(0, TAIL, pair[:, :LANE])
        put(1, TAIL, pair[:, LANE:])
        put(2, TAIL, dot(left, weights(2, TAIL)))

    def unit_rows(first, taps=TAPS):
        return lambda dx, lanes: cat_rows(ring[(first + dx * 3 + dy) % RING, :, lanes] for dy in taps)

    halo_wait(p1, HALF, 4, 0)
    cp_e2a.wait()

    level2_taps(narrow_lhs(p1, 0, TILE, HALF),
                lambda dx, lanes: narrow_rhs(lambda dy, r0, r1: v_e2a[dy * 3 + dx, r0:r1, lanes]))
    finish_level2(2, store_level2(act2, HALF))
    halo_start(act2, HALF, 4, 2)

    def conv640(ref, first, index, add=False):
        level2_taps(ref[HALF:HALF + TILE, :], unit_rows(first, (1,)), add)
        halo_wait(ref, HALF, SIDE, index)
        level2_taps(stack_rows(ref, TILE, HALF, (0, 2)), unit_rows(first, (0, 2)), add=True)

    wait_units(E2B, MA)
    conv640(act2, E2B, 2)
    finish_level2(3, store_s2)
    halo_start(p2, W3, 2, 3)
    halo_start(s2, HALF, 4, 4)
    refill((E2B, MA))

    x_index3 = column_index(HALF, W3)
    not_first3 = x_index3 > 0
    not_last3 = x_index3 < 31

    def finish_level3(bias_row, ref, start):
        def body(block, carry):
            lanes = pl.ds(pl.multiple_of(block * LANE, LANE), LANE)
            value = pl3[1, SUB:72, lanes] + jnp.where(not_first3, pl3[0, 7:71, lanes], 0.0)
            value = value + jnp.where(not_last3, pl3[2, 9:73, lanes], 0.0)
            ref[start:start + HALF, lanes] = relu(value + bias[bias_row:bias_row + 1, lanes]).astype(BF16)
            return carry

        lax.fori_loop(0, 10, body, 0)

    def slot_of(index):
        return index % RING

    def wide(first):
        return cat_lanes([ring[slot_of(first)], ring[slot_of(first + 1)]])

    def add_rows(dx, value):
        pl3[dx, SUB:72, :] = pl3[dx, SUB:72, :] + value

    wait_units(MA, MB)
    for dx in TAPS:
        pl3[dx, SUB:72, :] = dot(p2[W3:3 * W3, :], wide(MA + 2 * dx))
    cp_d1b.wait()
    build_tail(v_e1b, 0, t_e1b)
    halo_wait(p2, W3, 2, 3)
    left = cat_lanes([p2[:HALF, :], p2[HALF:LANE, :]])
    for dx in TAPS:
        add_rows(dx, dot(left, cat_rows([wide(MA + 6 + 2 * dx), wide(MA + 12 + 2 * dx)])))
    finish_level3(4, act3, W3)
    halo_start(act3, W3, 2, 5)
    refill((MA, MB))

    for group, dy in enumerate(ROWS):
        if group == 1:
            halo_wait(act3, W3, 2, 5)
        begin = MB + group * 12
        wait_units(begin, begin + 12)
        left = act3[dy * W3:dy * W3 + HALF, :]
        for dx in TAPS:
            first = begin + dx * SIDE
            value = dot(left, cat_rows([wide(first), wide(first + 2)]))
            if group:
                add_rows(dx, value)
            else:
                pl3[dx, SUB:72, :] = value
        refill((begin, begin + 12))
    finish_level3(5, mid, 0)

    wait_units(UP2, D2A)
    for tap in QUAD:
        p, q = tap // 2, tap % 2
        left = mid[...]
        for a, b in NTILES:
            right = cat_rows(ring[(UP2 + 2 * tap + part) % RING, :, a:b] for part in PAIR)
            part = dot(left, right)
            for i in PAIR:
                for c0 in range(a, b, LANE):
                    up_f32[pl.ds(c0 * 2 + (2 * i + p) * HALF + q, W3, stride=2), :] = part[W3 * i:W3 * i + W3, c0 - a:c0 - a + LANE]
    for block in range(5):
        u2[HALF:C1, block * LANE:block * LANE + LANE] = up_f32[block * TILE:block * TILE + TILE, :].astype(BF16)
    halo_start(u2, HALF, 4, 6)
    refill((UP2, D2A))
    halo_wait(s2, HALF, SIDE, 4)

    wait_units(D2A, D2A + TAP9)
    level2_taps(stack_rows(s2, TILE, HALF), unit_rows(D2A))
    refill((D2A, D2A + TAP9))
    wait_units(D2A + TAP9, D2B)
    conv640(u2, D2A + TAP9, 6, True)
    refill((D2A + TAP9, D2B))
    finish_level2(6, store_level2(act4, HALF))
    halo_start(act4, HALF, 4, 7)
    wait_units(D2B, UP1)
    conv640(act4, D2B, 7)
    finish_level2(7, store_level2(d2, 0))

    def half1(tap):
        return slice((tap % 2) * C1, (tap % 2) * C1 + C1)

    refill((D2B, UP1))
    wait_units(UP1, D1A)
    for tap in QUAD:
        p, q = tap // 2, tap % 2
        left = d2[...]
        up = dot_t(left, ring[(UP1 + tap // 2) % RING, half1(tap), :])
        for a, b in ((0, TILE), (TILE, C1)):
            part = up[:, a:b]
            for i in QUAD:
                for c0 in range(a, b, LANE):
                    c1 = min(b, c0 + LANE)
                    up_f32[pl.ds(c0 * SUB + (2 * i + p) * LANE + q, HALF, stride=2), :c1 - c0] = part[HALF * i:HALF * i + HALF, c0 - a:c1 - a]
    for block in TAPS:
        value = up_f32[block * 1024:block * 1024 + 1024, :].astype(BF16)
        if block < 2:
            cat1[LANE:TILE + 7 * LANE, blocks_of(block)] = value
        else:
            cat1[LANE:TILE + 7 * LANE, TILE:C1] = value[:, :HALF]
    halo_start(cat1, LANE, SUB, 8, U1_LANES)

    def d1a_tap(tap):
        return ring[(D1A + tap // 2) % RING, half1(tap), :]

    wait_units(D1A, UNITS)
    conv_cat(8, store_level1(act5), (1, 2))
    halo_wait(cat1, LANE, SUB, 1, S1_LANES)
    halo_wait(cat1, LANE, SUB, 8, U1_LANES, NEAR)
    conv_cat(8, store_level1(act5), (near,))
    halo_start(act5, LANE, SUB, TAP9, sides=NEAR)
    halo_wait(cat1, LANE, SUB, 8, U1_LANES, FAR)
    conv_cat(8, store_level1(act5), (far,))
    halo_start(act5, LANE, SUB, TAP9, sides=FAR)

    def finish_head(i, pieces):
        head = dot_t(w_out[...].astype(BF16), cat_lanes(piece.astype(BF16) for piece in pieces))
        ys[pl.ds(i, 1)] = head[None]

    conv_narrow(act5, TAP9, finish_head, (1, 2))
    halo_wait(act5, LANE, SUB, TAP9, sides=NEAR)
    conv_narrow(act5, TAP9, finish_head, (near,))
    halo_wait(act5, LANE, SUB, TAP9, sides=FAR)
    conv_narrow(act5, TAP9, finish_head, (far,))

    for c in QUAD:
        packed = jnp.zeros((SUB, LANE), F32)
        for y in range(SUB):
            line = ys[y // 2, :, (y % 2) * LANE:(y % 2) * LANE + LANE]
            slot = y % 4
            shift = (W3 * slot - W3 * c) % LANE
            line = turn(line, shift)
            if y >= 4:
                line = pltpu.roll(line, 4, 0)
            place = AND(AND(lanes8 >= W3 * slot, lanes8 < W3 * slot + W3), (sub8 >= 4) if y >= 4 else (sub8 < 4))
            packed = jnp.where(place, line, packed)
        ysend[c] = packed

    def y_copy(c):
        return remote(ysend.at[c], yrecv.at[k_me], y_send.at[c], y_recv.at[k_me], c, col)

    for c in QUAD:
        here = is_me(c, col)

        @pl.when(NOT(here))
        def _():
            y_copy(c).start()

        @pl.when(here)
        def _():
            yrecv[pl.ds(k_me, 1)] = ysend[c][None]

    for k in QUAD:
        from_col, from_row = owner(4 * row + k)

        @pl.when(NOT(is_me(from_col, from_row)))
        def _():
            remote(ysend.at[0], yrecv.at[k], y_send.at[0], y_recv.at[k], col, row).wait_recv()

    for c in QUAD:
        @pl.when(NOT(is_me(c, col)))
        def _():
            y_copy(c).wait_send()

    for k in QUAD:
        for low in QUAD:
            line = turn(yrecv[k], (LANE - low * W3) % LANE)
            for high in PAIR:
                out_ref[k * SUB + high * SIDE + low] = line[high * SIDE:high * SIDE + SIDE, :W3]


def network(x, w_e1a, w_head, *rest):
    vmem = pl.BlockSpec(memory_space=pltpu.VMEM)
    hbm = pl.BlockSpec(memory_space=pl.ANY)
    dma = pltpu.SemaphoreType.DMA
    scratch = [pltpu.VMEM(shape, F32) for shape in ((5 * SUB, SUB, LANE), (5, SUB, LANE), (SIDE, 2, SUB, LANE), (SIDE, 1, SUB, LANE), (TILE, LANE))]
    level1, level2 = 10 * LANE, 6 * HALF
    scratch += [pltpu.VMEM(shape, BF16) for shape in (
        (level1, C1P), (level1, C2), (level2, C1P), (level2, C2), (level2, C2), (LANE, C2), (LANE, C3), (HALF, C3),
        (level2, C2), (level2, C2), (TILE, C2), (level1, C1P),
        (TAP9, C1, C1), (TAP9, C1, C2), (3, C1, TILE), (RING, C2, C2))]
    scratch += [pltpu.VMEM(shape, F32) for shape in (
        (10, C3), (48, C1P), (SUB, C1P),
        (2, 3, MARGIN, TILE), (2, MARGIN, TILE), (3, MARGIN, C2), (3, 80, C3), (2, MARGIN, 1024),
        (LANE, LANE), (3072, LANE), (SIDE, SUB, TILE), (SIDE, SUB, LANE), (SIDE, SUB, LANE))]
    scratch += [dma(shape) for shape in ((3,), (RING,), (SIDE,), (SIDE,), (2,), (SIDE,), (10, 2), (10, 2), (SIDE,), (SIDE,))]
    return pl.pallas_call(
        kernel,
        out_shape=jax.ShapeDtypeStruct((W3, SIDE, W3), F32),
        in_specs=[vmem] * 13 + [hbm] * 11,
        out_specs=vmem,
        scratch_shapes=scratch,
        compiler_params=pltpu.CompilerParams(collective_id=0, has_side_effects=True, vmem_limit_bytes=67043328),
        name="unet",
    )(x, w_e1a, w_head, *rest)


def solution(mesh):
    tile_spec = P(("data", "row"), "col", None)

    def device_body(tile, *params):
        (w_enc1a, b_enc1a, w_enc1b, b_enc1b, w_enc2a, b_enc2a, w_enc2b, b_enc2b,
         w_mid_a, b_mid_a, w_mid_b, b_mid_b, w_up2, w_dec2a, b_dec2a, w_dec2b, b_dec2b,
         w_up1, w_dec1a, b_dec1a, w_dec1b, b_dec1b, w_head, b_head) = params
        biases = (b_enc1a, b_enc1b, b_enc2a, b_enc2b, b_mid_a, b_mid_b, b_dec2a, b_dec2b, b_dec1a, b_dec1b)

        def taps(weight):
            return weight.reshape(-1, weight.shape[2], weight.shape[3])

        def turned(weight):
            return jnp.swapaxes(weight, 2, 3).reshape(-1, weight.shape[2])

        weights = [taps(w) for w in (w_enc1b, w_enc2a, w_enc2b, w_mid_a, w_mid_b, w_up2, w_dec2a, w_dec2b)]
        weights += [turned(w_up1), turned(w_dec1a), taps(w_dec1b)]
        packed = network(jnp.transpose(tile, (0, 2, 1)), taps(w_enc1a), w_head.T, *biases, *weights)
        return jnp.transpose(packed, (0, 2, 1)) + b_head

    def program(image, *params):
        mapped = jax.shard_map(device_body, mesh=mesh, in_specs=(tile_spec,) + tuple([P()] * len(params)), out_specs=tile_spec, check_vma=False)
        return mapped(image, *params)

    return program
```

```python
import jax
import jax.numpy as jnp
from jax import lax
from jax.experimental import pallas as pl
from jax.experimental.pallas import tpu as pltpu
from jax.sharding import PartitionSpec as P

F32 = jnp.float32
BF16 = jnp.bfloat16
STRIPS = 16
LAST = STRIPS - 1
SIDE = 4
SUB, LANE = 8, 128
TILE, HALF = 2 * LANE, LANE // 2
C1, C2, C3, C1P = 320, 640, 1280, 384
W3 = 32
END = SUB + TILE
MARGIN = END + SUB
TAPS = range(3)
PAIR = range(2)
QUAD = range(SIDE)
TAP9 = 9
RING = 47
E2B, MA, MB, UP2, D2A, D2B, UP1, D1A, UNITS = 0, 9, 27, 63, 71, 89, 98, 100, 105
ROWS = (1, 0, 2)
NOT = jnp.logical_not
AND = jnp.logical_and
OR = jnp.logical_or
MESH_ID = pl.DeviceIdType.MESH


def dot(lhs, rhs):
    return jnp.dot(lhs, rhs, preferred_element_type=F32)


def relu(value):
    return jnp.maximum(value, 0.0)


def dot_t(lhs, rhs):
    return lax.dot_general(lhs, rhs, (((1,), (1,)), ((), ())), preferred_element_type=F32)


def cat_lanes(parts):
    return jnp.concatenate(list(parts), axis=1)


def cat_rows(parts):
    return jnp.concatenate(list(parts), axis=0)


def turn(value, amount=HALF):
    return value if amount == 0 else pltpu.roll(value, amount, 1)


def lane_mask(shape, below):
    return lax.broadcasted_iota(jnp.int32, shape, 1) < below


def column_index(rows, width):
    return lax.rem(lax.broadcasted_iota(jnp.int32, (rows, LANE), 0), width)


def kernel(x_ref, w_e1a, w_head, *refs):
    biases, refs = refs[:10], refs[10:]
    (h_e1b, h_e2a, h_e2b, h_ma, h_mb, h_up2, h_d2a, h_d2b, h_up1, h_d1a, h_d1b,
     out_ref,
     xrows, xs, xb, xh, z, act1, cat1, p1, act2, s2, p2, act3, mid, u2, act4, d2, act5,
     v_e1b, v_e2a, t_e1b, ring, bias, w_first, w_out,
     pm, pt, pl2, pl3, pd1, pool, up_f32, ys, ysend, yrecv,
     sem_w, sem_r, x_send, x_recv, h_send, h_recv, e_send, e_recv, y_send, y_recv) = refs
    col = lax.axis_index("col")
    row = lax.axis_index("row")
    data = lax.axis_index("data")

    def owner(strip):
        strip_col = strip // 4
        k = strip % 4
        return strip_col, k + (strip_col % 2) * (3 - 2 * k)

    def device(strip_col, strip_row):
        return (data, strip_col, strip_row)

    k_me = row + (col % 2) * (3 - 2 * row)
    me = 4 * col + k_me

    barrier = pltpu.get_barrier_semaphore()
    for strip in range(1, STRIPS):
        other_col, other_row = owner((me + strip) % STRIPS)
        pl.semaphore_signal(barrier, inc=1, device_id=device(other_col, other_row), device_id_type=MESH_ID)

    def whole(src, dst, index):
        return pltpu.make_async_copy(src, dst, sem_w.at[index])

    cp_e1b = whole(h_e1b, v_e1b, 0)
    cp_e2a = whole(h_e2a, v_e2a, 1)
    cp_d1b = whole(h_d1b, v_e1b, 2)

    def half(index):
        return pl.ds((index % 2) * C2, C2)

    def unit(index):
        slot = index % RING
        dst = ring.at[slot]
        if index < MA:
            src = h_e2b.at[(index % 3) * 3 + index // 3]
        elif index < MB:
            tap = (index - MA) // 2
            src = h_ma.at[ROWS[tap // 3] * 3 + tap % 3, :, half(index - MA)]
        elif index < UP2:
            local = index - MB
            tap = local // 4
            src = h_mb.at[ROWS[tap // 3] * 3 + tap % 3, half(local // 2), half(local)]
        elif index < D2A:
            local = index - UP2
            src = h_up2.at[local // 2, half(local)]
        elif index < D2B:
            local = (index - D2A) % TAP9
            src = h_d2a.at[(local % 3) * 3 + local // 3, half((D2B - 1 - index) // TAP9)]
        elif index < UP1:
            local = index - D2B
            src = h_d2b.at[(local % 3) * 3 + local // 3]
        elif index < D1A:
            src = h_up1.at[pl.ds((index - UP1) * C2, C2)]
        elif index < UNITS - 1:
            src = h_d1a.at[pl.ds((index - D1A) * C2, C2)]
        else:
            src = h_d1a.at[pl.ds((index - D1A) * C2, C1)]
            dst = ring.at[slot, pl.ds(0, C1)]
        return pltpu.make_async_copy(src, dst, sem_r.at[slot])

    def wait_units(first, last):
        for index in range(first, last):
            unit(index).wait()

    def refill(done):
        for index in range(done[0] + RING, min(done[1] + RING, UNITS)):
            unit(index).start()

    cp_e1b.start()
    cp_e2a.start()
    for index in range(MA):
        unit(index).start()

    bias[...] = jnp.zeros_like(bias)
    for index, ref in enumerate(biases):
        bias[index:index + 1, :ref.shape[0]] = ref[...].reshape(1, ref.shape[0])
    w_first[...] = jnp.zeros_like(w_first)
    for tap in range(TAP9):
        at = (tap // 3) * STRIPS + (tap % 3) * SIDE
        w_first[at:at + SIDE, :C1] = w_e1a[tap].astype(F32)
    w_out[...] = jnp.zeros_like(w_out)
    w_out[:SIDE, :C1] = w_head[...].astype(F32)

    xrows[...] = jnp.zeros_like(xrows)
    xrows[2:2 + W3, :SIDE, :W3] = x_ref[...].astype(F32)

    def pack(group, carry):
        packed = jnp.zeros((SUB, LANE), F32)
        for j in range(SUB):
            line = turn(xrows[group * SUB + j], (j % SIDE) * W3)
            packed = packed + (line if j < SIDE else pltpu.roll(line, SIDE, 0))
        xs[pl.ds(group, 1)] = packed[None]
        return carry

    lax.fori_loop(0, 5, pack, 0)
    pl.semaphore_wait(barrier, LAST)

    def build_tail(weights, base, tail):
        def body(dy, carry):
            parts = [weights[dy * 3 + dx, base:base + C1, TILE:C1].astype(F32) for dx in TAPS]
            zero = jnp.zeros((C1, HALF), F32)
            pair = cat_lanes(parts[:2])
            last = cat_lanes([parts[2], zero])
            tail[dy, :, :LANE] = pair.astype(BF16)
            tail[dy, :, LANE:TILE] = last.astype(BF16)
            return carry

        lax.fori_loop(0, 3, body, 0)


    def is_me(strip_col, strip_row):
        return AND(strip_col == col, strip_row == row)

    def remote(src, dst, send, recv, strip_col, strip_row):
        return pltpu.make_async_remote_copy(src_ref=src, dst_ref=dst, send_sem=send, recv_sem=recv,
                                            device_id=device(strip_col, strip_row), device_id_type=MESH_ID)

    for k in QUAD:
        to_col, to_row = owner(4 * row + k)
        here = is_me(to_col, to_row)
        copy = remote(xs.at[pl.ds(k, 2)], xb.at[col], x_send.at[k], x_recv.at[col], to_col, to_row)

        @pl.when(NOT(here))
        def _():
            copy.start()

        @pl.when(here)
        def _():
            xb[pl.ds(col, 1)] = xs[k:k + 2][None]

    def halo_target(strip):
        return owner(jnp.clip(strip, 0, LAST))

    for side, (strip, allowed, first) in enumerate(((4 * row - 1, row > 0, 0), (4 * row + 4, row < 3, SIDE))):
        to_col, to_row = halo_target(strip)
        here = is_me(to_col, to_row)
        copy = remote(xs.at[pl.ds(first, 1)], xh.at[col], h_send.at[side], h_recv.at[col], to_col, to_row)

        @pl.when(AND(allowed, NOT(here)))
        def _():
            copy.start()

        @pl.when(AND(allowed, here))
        def _():
            xh[pl.ds(col, 1)] = xs[first:first + 1][None]

    cp_e1b.wait()
    build_tail(v_e1b, 0, t_e1b)
    for index in range(MA, RING):
        unit(index).start()

    for c in QUAD:
        @pl.when(NOT(is_me(c, row) & (row == col)))
        def _():
            remote(xs.at[pl.ds(0, 2)], xb.at[c], x_send.at[0], x_recv.at[c], col, row).wait_recv()

    has_top = AND(k_me == 0, col > 0)
    has_bottom = AND(k_me == 3, col < 3)
    halo_row = jnp.where(has_top, col - 1, col + 1)
    for c in QUAD:
        own = AND(c == col, row == halo_row)

        @pl.when(AND(OR(has_top, has_bottom), NOT(own)))
        def _():
            remote(xs.at[pl.ds(0, 1)], xh.at[c], h_send.at[0], h_recv.at[c], col, row).wait_recv()

    for k in QUAD:
        to_col, to_row = owner(4 * row + k)

        @pl.when(NOT(is_me(to_col, to_row)))
        def _():
            remote(xs.at[pl.ds(k, 2)], xb.at[col], x_send.at[k], x_recv.at[col], to_col, to_row).wait_send()

    for side, (strip, allowed, first) in enumerate(((4 * row - 1, row > 0, 0), (4 * row + 4, row < 3, SIDE))):
        to_col, to_row = halo_target(strip)

        @pl.when(AND(allowed, NOT(is_me(to_col, to_row))))
        def _():
            remote(xs.at[pl.ds(first, 1)], xh.at[col], h_send.at[side], h_recv.at[col], to_col, to_row).wait_send()

    lanes8 = lax.broadcasted_iota(jnp.int32, (SUB, LANE), 1)
    sub8 = lax.broadcasted_iota(jnp.int32, (SUB, LANE), 0)
    z[...] = jnp.zeros_like(z)
    halo_place = (AND(has_top, lanes8 < HALF), AND(has_bottom, lanes8 >= HALF))
    for part in PAIR:
        place = AND(halo_place[part], sub8 < SIDE)
        blocks = [jnp.where(place, xh[c, 0], xb[c, part]) for c in QUAD]
        for group in QUAD:
            line = jnp.zeros((SUB, LANE), F32)
            for c in QUAD:
                inside = lanes8 // W3 == c
                line = jnp.where(inside, turn(blocks[c], (W3 * (c - group)) % LANE), line)
            for dx in TAPS:
                moved = line
                if dx == 0:
                    moved = jnp.where(lanes8 == 0, 0.0, turn(line, 1))
                elif dx == 2:
                    moved = jnp.where(lanes8 == LANE - 1, 0.0, turn(line, LANE - 1))
                for upper in range(2 - part):
                    at = (part * SUB + group + upper * SIDE) * STRIPS + dx * SIDE
                    z[at:at + SIDE, :] = moved[upper * SIDE:upper * SIDE + SIDE]

    def first_conv(pair, carry):
        weights = w_first[...].astype(BF16)
        for j in (2 * pair, 2 * pair + 1):
            taps = z[pl.ds(pl.multiple_of(j * STRIPS, STRIPS), 48), :].astype(BF16)
            value = lax.dot_general(taps, weights, (((0,), (0,)), ((), ())), preferred_element_type=F32)
            value = relu(value + bias[:1, :C1P])
            outside = OR(AND(me == 0, j == 0), AND(me == LAST, j == TAP9))
            value = jnp.where(outside, 0.0, value)
            act1[pl.ds(pl.multiple_of(j * LANE, LANE), LANE), :] = value.astype(BF16)
        return carry

    lax.fori_loop(0, 5, first_conv, 0)

    up_col, up_row = owner(jnp.maximum(me - 1, 0))
    down_col, down_row = owner(jnp.minimum(me + 1, LAST))

    def clear_borders(ref, width, height):
        @pl.when(me == 0)
        def _():
            ref[:width, :] = jnp.zeros((width, ref.shape[1]), BF16)

        @pl.when(me == LAST)
        def _():
            ref[(height + 1) * width:(height + 2) * width, :] = jnp.zeros((width, ref.shape[1]), BF16)

    for ref, width, height in ((cat1, LANE, SUB), (act5, LANE, SUB), (p1, HALF, SIDE), (act2, HALF, SIDE), (s2, HALF, SIDE),
                               (u2, HALF, SIDE), (act4, HALF, SIDE), (p2, W3, 2), (act3, W3, 2)):
        clear_borders(ref, width, height)

    def halo_copies(ref, width, height, index, lanes):
        to_up = remote(ref.at[pl.ds(width, width), lanes], ref.at[pl.ds((height + 1) * width, width), lanes],
                       e_send.at[index, 0], e_recv.at[index, 0], up_col, up_row)
        to_down = remote(ref.at[pl.ds(height * width, width), lanes], ref.at[pl.ds(0, width), lanes],
                         e_send.at[index, 1], e_recv.at[index, 1], down_col, down_row)
        return to_up, to_down

    odd = k_me % 2 == 1
    even = NOT(odd)
    far = (k_me % 2) * 3
    near = 3 - far
    ANY = (True, True)
    FAR = (even, odd)
    NEAR = (odd, even)

    def halo_start(ref, width, height, index, lanes=slice(None), sides=ANY):
        to_up, to_down = halo_copies(ref, width, height, index, lanes)

        @pl.when(AND(me > 0, sides[0]))
        def _():
            to_up.start()

        @pl.when(AND(me < LAST, sides[1]))
        def _():
            to_down.start()

    def halo_wait(ref, width, height, index, lanes=slice(None), sides=ANY):
        to_up, to_down = halo_copies(ref, width, height, index, lanes)

        @pl.when(AND(me > 0, sides[0]))
        def _():
            to_down.wait_recv()
            to_up.wait_send()

        @pl.when(AND(me < LAST, sides[1]))
        def _():
            to_up.wait_recv()
            to_down.wait_send()

    def narrow_lhs(ref, start, rows, width):
        mains = [ref[pl.ds(start + dy * width, rows), :TILE] for dy in TAPS]
        tails = [ref[pl.ds(start + dy * width, rows), TILE:C1P] for dy in TAPS]
        pair = (tails[0].astype(F32) + turn(tails[1].astype(F32))).astype(BF16)
        return cat_lanes(mains + [pair, tails[2][:, :HALF]])

    def narrow_rhs(load):
        return cat_rows([load(dy, 0, TILE) for dy in TAPS] + [load(dy, TILE, C1) for dy in TAPS])

    x_index = column_index(TILE, LANE)
    not_first = x_index > 0
    not_last = x_index < 127

    low_half = lane_mask((TILE, LANE), HALF)

    def shifted(ref, plane, left, right):
        first = left + jnp.where(not_first, ref[plane(0) + (slice(7, 263), right[0])], 0.0)
        return first + jnp.where(not_last, ref[plane(2) + (slice(9, 265), right[1])], 0.0)

    def scaled(i, step):
        return i * step if isinstance(i, int) else pl.multiple_of(i * step, step)

    def blocks_of(block):
        return slice(block * LANE, block * LANE + LANE)

    def conv_narrow(ref, bias_row, finish, chunks):
        for side, i in enumerate(chunks):
            left = narrow_lhs(ref, scaled(i, TILE), TILE, LANE)
            for dx in TAPS:
                pm[side, dx, SUB:END, :] = dot(left, narrow_rhs(lambda dy, a, b: v_e1b[dy * 3 + dx, a:b, :TILE]))
            pt[side, SUB:END, :] = dot(left, narrow_rhs(lambda dy, a, b: t_e1b[dy, a:b, :]))
        for side, i in enumerate(chunks):
            pieces = []
            for block in PAIR:
                lanes = blocks_of(block)
                value = shifted(pm, lambda dx: (side, dx), pm[side, 1, SUB:END, lanes], (lanes, lanes))
                pieces.append(relu(value + bias[bias_row:bias_row + 1, lanes]))
            value = shifted(pt, lambda dx: (side,), turn(pt[side, SUB:END, :LANE]), (blocks_of(0), blocks_of(1)))
            value = relu(value + bias[bias_row:bias_row + 1, TILE:C1P])
            pieces.append(jnp.where(low_half, value, 0.0))
            finish(i, pieces)

    def conv_cat(bias_row, finish, chunks):
        for side, i in enumerate(chunks):
            start = scaled(i, TILE)
            left = cat_lanes(cat1[pl.ds(start + dy * LANE, TILE), :] for dy in TAPS)
            right = cat_lanes(cat_rows(d1a_tap(dy * 3 + dx) for dx in TAPS) for dy in TAPS)
            pd1[side, SUB:END, :3 * C1] = dot_t(left, right)
        for side, i in enumerate(chunks):
            turned = [turn(pd1[side, SUB:END, blocks_of(2 + block)]) for block in TAPS]
            pieces = []
            for block in TAPS:
                middle = turned[block] if block == 2 else jnp.where(low_half, turned[block], turned[block + 1])
                value = shifted(pd1, lambda dx: (side,), middle, (blocks_of(block), blocks_of(5 + block) if block < 2 else slice(896, 1024)))
                value = relu(value + bias[bias_row:bias_row + 1, blocks_of(block)])
                pieces.append(value if block < 2 else jnp.where(low_half, value, 0.0))
            finish(i, pieces)

    def store_level1(ref):
        def finish(i, pieces):
            start = LANE + scaled(i, TILE)
            for block in range(3):
                ref[pl.ds(start, TILE), block * LANE:block * LANE + LANE] = pieces[block].astype(BF16)
        return finish

    def finish_s1(i, pieces):
        at = pl.ds(LANE + scaled(i, TILE), TILE)
        turned = [turn(piece) for piece in pieces]
        cat1[at, TILE:C1P] = jnp.where(low_half, 0.0, turned[0]).astype(BF16)
        for block in PAIR:
            cat1[at, blocks_of(3 + block)] = jnp.where(low_half, turned[block], turned[block + 1]).astype(BF16)
        start = HALF + scaled(i, HALF)
        for block in range(3):
            pool[:LANE, :] = jnp.maximum(pieces[block][:LANE], pieces[block][LANE:TILE])
            pooled = jnp.maximum(pool[pl.ds(0, HALF, stride=2), :], pool[pl.ds(1, HALF, stride=2), :])
            p1[pl.ds(start, HALF), block * LANE:block * LANE + LANE] = pooled.astype(BF16)

    S1_LANES = pl.ds(C1P, TILE)
    U1_LANES = pl.ds(0, C1P)
    conv_narrow(act1, 1, finish_s1, (far,))
    halo_start(p1, HALF, SIDE, 0, sides=FAR)
    conv_narrow(act1, 1, finish_s1, (near,))
    halo_start(p1, HALF, SIDE, 0, sides=NEAR)
    halo_start(cat1, LANE, SUB, 1, S1_LANES)
    conv_narrow(act1, 1, finish_s1, (1, 2))
    cp_d1b.start()

    x_index2 = column_index(TILE, HALF)
    not_first2 = x_index2 > 0
    not_last2 = x_index2 < 63

    def finish_level2(bias_row, store):
        def body(block, carry):
            lanes = pl.ds(pl.multiple_of(block * LANE, LANE), LANE)
            value = pl2[1, SUB:END, lanes] + jnp.where(not_first2, pl2[0, 7:263, lanes], 0.0)
            value = value + jnp.where(not_last2, pl2[2, 9:265, lanes], 0.0)
            store(lanes, relu(value + bias[bias_row:bias_row + 1, lanes]))
            return carry

        lax.fori_loop(0, 5, body, 0)

    def store_level2(ref, start):
        def store(lanes, value):
            ref[start:start + TILE, lanes] = value.astype(BF16)
        return store

    def store_s2(lanes, value):
        s2[HALF:C1, lanes] = value.astype(BF16)
        for i in PAIR:
            pool[:HALF, :] = jnp.maximum(value[LANE * i:LANE * i + HALF], value[LANE * i + HALF:LANE * i + LANE])
            pooled = jnp.maximum(pool[pl.ds(0, W3, stride=2), :], pool[pl.ds(1, W3, stride=2), :])
            p2[W3 + W3 * i:HALF + W3 * i, lanes] = pooled.astype(BF16)

    NTILES = ((0, TILE), (TILE, 2 * TILE), (2 * TILE, C2))
    TAIL = slice(2 * TILE, C2)

    def stack_rows(ref, rows, width, taps=TAPS):
        return cat_lanes(ref[dy * width:dy * width + rows, :] for dy in taps)

    def level2_taps(left, weights, add=False, groups=QUAD):
        if groups is not QUAD:
            left = cat_rows(left[group * HALF:group * HALF + HALF] for group in groups)

        def put(dx, lanes, value):
            if groups is QUAD:
                pl2[dx, SUB:END, lanes] = pl2[dx, SUB:END, lanes] + value if add else value
                return
            for part, group in enumerate(groups):
                at = slice(SUB + group * HALF, SUB + group * HALF + HALF)
                piece = value[part * HALF:part * HALF + HALF]
                pl2[dx, at, lanes] = pl2[dx, at, lanes] + piece if add else piece

        for dx in TAPS:
            for first, last in NTILES[:2]:
                lanes = slice(first, last)
                put(dx, lanes, dot(left, weights(dx, lanes)))
        pair = dot(left, cat_lanes(weights(dx, TAIL) for dx in PAIR))
        put(0, TAIL, pair[:, :LANE])
        put(1, TAIL, pair[:, LANE:])
        put(2, TAIL, dot(left, weights(2, TAIL)))

    def unit_rows(first, taps=TAPS):
        return lambda dx, lanes: cat_rows(ring[(first + dx * 3 + dy) % RING, :, lanes] for dy in taps)

    halo_wait(p1, HALF, 4, 0)
    cp_e2a.wait()

    def finish_groups(bias_row, ref, groups):
        def body(block, carry):
            lanes = pl.ds(pl.multiple_of(block * LANE, LANE), LANE)
            for group in groups:
                at = SUB + group * HALF
                value = pl2[1, at:at + HALF, lanes] + jnp.where(not_first2[:HALF], pl2[0, at - 1:at - 1 + HALF, lanes], 0.0)
                value = value + jnp.where(not_last2[:HALF], pl2[2, at + 1:at + 1 + HALF, lanes], 0.0)
                value = relu(value + bias[bias_row:bias_row + 1, lanes])
                ref[(group + 1) * HALF:(group + 2) * HALF, lanes] = value.astype(BF16)
            return carry

        lax.fori_loop(0, 5, body, 0)

    def edges_first(left, weights, add, bias_row, ref, index):
        for groups in ((0, 3), (1, 2)):
            level2_taps(left, weights, add, groups)
            finish_groups(bias_row, ref, groups)
            if 0 in groups:
                halo_start(ref, HALF, SIDE, index)

    edges_first(narrow_lhs(p1, 0, TILE, HALF),
                lambda dx, lanes: narrow_rhs(lambda dy, r0, r1: v_e2a[dy * 3 + dx, r0:r1, lanes]), False, 2, act2, 2)

    def conv640(ref, first, index, add=False, finish=None):
        level2_taps(ref[HALF:HALF + TILE, :], unit_rows(first, (1,)), add)
        halo_wait(ref, HALF, SIDE, index)
        left = stack_rows(ref, TILE, HALF, (0, 2))
        if finish is None:
            level2_taps(left, unit_rows(first, (0, 2)), add=True)
        else:
            edges_first(left, unit_rows(first, (0, 2)), True, *finish)

    wait_units(E2B, MA)
    conv640(act2, E2B, 2)
    finish_level2(3, store_s2)
    halo_start(p2, W3, 2, 3)
    halo_start(s2, HALF, 4, 4)
    refill((E2B, MA))

    x_index3 = column_index(HALF, W3)
    not_first3 = x_index3 > 0
    not_last3 = x_index3 < 31

    def finish_level3(bias_row, ref, start):
        def body(block, carry):
            lanes = pl.ds(pl.multiple_of(block * LANE, LANE), LANE)
            value = pl3[1, SUB:72, lanes] + jnp.where(not_first3, pl3[0, 7:71, lanes], 0.0)
            value = value + jnp.where(not_last3, pl3[2, 9:73, lanes], 0.0)
            ref[start:start + HALF, lanes] = relu(value + bias[bias_row:bias_row + 1, lanes]).astype(BF16)
            return carry

        lax.fori_loop(0, 10, body, 0)

    def slot_of(index):
        return index % RING

    def wide(first):
        return cat_lanes([ring[slot_of(first)], ring[slot_of(first + 1)]])

    def add_rows(dx, value):
        pl3[dx, SUB:72, :] = pl3[dx, SUB:72, :] + value

    wait_units(MA, MB)
    for dx in TAPS:
        pl3[dx, SUB:72, :] = dot(p2[W3:3 * W3, :], wide(MA + 2 * dx))
    cp_d1b.wait()
    build_tail(v_e1b, 0, t_e1b)
    halo_wait(p2, W3, 2, 3)
    left = cat_lanes([p2[:HALF, :], p2[HALF:LANE, :]])
    for dx in TAPS:
        add_rows(dx, dot(left, cat_rows([wide(MA + 6 + 2 * dx), wide(MA + 12 + 2 * dx)])))
    finish_level3(4, act3, W3)
    halo_start(act3, W3, 2, 5)
    refill((MA, MB))

    for group, dy in enumerate(ROWS):
        if group == 1:
            halo_wait(act3, W3, 2, 5)
        begin = MB + group * 12
        wait_units(begin, begin + 12)
        left = act3[dy * W3:dy * W3 + HALF, :]
        for dx in TAPS:
            first = begin + dx * SIDE
            value = dot(left, cat_rows([wide(first), wide(first + 2)]))
            if group:
                add_rows(dx, value)
            else:
                pl3[dx, SUB:72, :] = value
        refill((begin, begin + 12))
    finish_level3(5, mid, 0)

    wait_units(UP2, D2A)
    for tap in QUAD:
        p, q = tap // 2, tap % 2
        left = mid[...]
        for a, b in NTILES:
            right = cat_rows(ring[(UP2 + 2 * tap + part) % RING, :, a:b] for part in PAIR)
            part = dot(left, right)
            for i in PAIR:
                for c0 in range(a, b, LANE):
                    up_f32[pl.ds(c0 * 2 + (2 * i + p) * HALF + q, W3, stride=2), :] = part[W3 * i:W3 * i + W3, c0 - a:c0 - a + LANE]
    for block in range(5):
        u2[HALF:C1, block * LANE:block * LANE + LANE] = up_f32[block * TILE:block * TILE + TILE, :].astype(BF16)
    halo_start(u2, HALF, 4, 6)
    refill((UP2, D2A))
    halo_wait(s2, HALF, SIDE, 4)

    wait_units(D2A, D2A + TAP9)
    level2_taps(stack_rows(s2, TILE, HALF), unit_rows(D2A))
    refill((D2A, D2A + TAP9))
    wait_units(D2A + TAP9, D2B)
    conv640(u2, D2A + TAP9, 6, True, (6, act4, 7))
    refill((D2A + TAP9, D2B))
    wait_units(D2B, UP1)
    conv640(act4, D2B, 7)
    finish_level2(7, store_level2(d2, 0))

    def half1(tap):
        return slice((tap % 2) * C1, (tap % 2) * C1 + C1)

    refill((D2B, UP1))
    wait_units(UP1, D1A)
    for tap in QUAD:
        p, q = tap // 2, tap % 2
        left = d2[...]
        up = dot_t(left, ring[(UP1 + tap // 2) % RING, half1(tap), :])
        for a, b in ((0, TILE), (TILE, C1)):
            part = up[:, a:b]
            for i in QUAD:
                for c0 in range(a, b, LANE):
                    c1 = min(b, c0 + LANE)
                    up_f32[pl.ds(c0 * SUB + (2 * i + p) * LANE + q, HALF, stride=2), :c1 - c0] = part[HALF * i:HALF * i + HALF, c0 - a:c1 - a]
    for block in TAPS:
        value = up_f32[block * 1024:block * 1024 + 1024, :].astype(BF16)
        if block < 2:
            cat1[LANE:TILE + 7 * LANE, blocks_of(block)] = value
        else:
            cat1[LANE:TILE + 7 * LANE, TILE:C1] = value[:, :HALF]
    halo_start(cat1, LANE, SUB, 8, U1_LANES)

    def d1a_tap(tap):
        return ring[(D1A + tap // 2) % RING, half1(tap), :]

    wait_units(D1A, UNITS)
    conv_cat(8, store_level1(act5), (1, 2))
    halo_wait(cat1, LANE, SUB, 1, S1_LANES)
    halo_wait(cat1, LANE, SUB, 8, U1_LANES, NEAR)
    conv_cat(8, store_level1(act5), (near,))
    halo_start(act5, LANE, SUB, TAP9, sides=NEAR)
    halo_wait(cat1, LANE, SUB, 8, U1_LANES, FAR)
    conv_cat(8, store_level1(act5), (far,))
    halo_start(act5, LANE, SUB, TAP9, sides=FAR)

    def finish_head(i, pieces):
        head = dot_t(w_out[...].astype(BF16), cat_lanes(piece.astype(BF16) for piece in pieces))
        ys[pl.ds(i, 1)] = head[None]

    conv_narrow(act5, TAP9, finish_head, (1, 2))
    halo_wait(act5, LANE, SUB, TAP9, sides=NEAR)
    conv_narrow(act5, TAP9, finish_head, (near,))
    halo_wait(act5, LANE, SUB, TAP9, sides=FAR)
    conv_narrow(act5, TAP9, finish_head, (far,))

    for c in QUAD:
        packed = jnp.zeros((SUB, LANE), F32)
        for y in range(SUB):
            line = ys[y // 2, :, (y % 2) * LANE:(y % 2) * LANE + LANE]
            slot = y % 4
            shift = (W3 * slot - W3 * c) % LANE
            line = turn(line, shift)
            if y >= 4:
                line = pltpu.roll(line, 4, 0)
            place = AND(AND(lanes8 >= W3 * slot, lanes8 < W3 * slot + W3), (sub8 >= 4) if y >= 4 else (sub8 < 4))
            packed = jnp.where(place, line, packed)
        ysend[c] = packed

    def y_copy(c):
        return remote(ysend.at[c], yrecv.at[k_me], y_send.at[c], y_recv.at[k_me], c, col)

    for c in QUAD:
        here = is_me(c, col)

        @pl.when(NOT(here))
        def _():
            y_copy(c).start()

        @pl.when(here)
        def _():
            yrecv[pl.ds(k_me, 1)] = ysend[c][None]

    for k in QUAD:
        from_col, from_row = owner(4 * row + k)

        @pl.when(NOT(is_me(from_col, from_row)))
        def _():
            remote(ysend.at[0], yrecv.at[k], y_send.at[0], y_recv.at[k], col, row).wait_recv()

    for c in QUAD:
        @pl.when(NOT(is_me(c, col)))
        def _():
            y_copy(c).wait_send()

    for k in QUAD:
        for low in QUAD:
            line = turn(yrecv[k], (LANE - low * W3) % LANE)
            for high in PAIR:
                out_ref[k * SUB + high * SIDE + low] = line[high * SIDE:high * SIDE + SIDE, :W3]


def network(x, w_e1a, w_head, *rest):
    vmem = pl.BlockSpec(memory_space=pltpu.VMEM)
    hbm = pl.BlockSpec(memory_space=pl.ANY)
    dma = pltpu.SemaphoreType.DMA
    scratch = [pltpu.VMEM(shape, F32) for shape in ((5 * SUB, SUB, LANE), (5, SUB, LANE), (SIDE, 2, SUB, LANE), (SIDE, 1, SUB, LANE), (TILE, LANE))]
    level1, level2 = 10 * LANE, 6 * HALF
    scratch += [pltpu.VMEM(shape, BF16) for shape in (
        (level1, C1P), (level1, C2), (level2, C1P), (level2, C2), (level2, C2), (LANE, C2), (LANE, C3), (HALF, C3),
        (level2, C2), (level2, C2), (TILE, C2), (level1, C1P),
        (TAP9, C1, C1), (TAP9, C1, C2), (3, C1, TILE), (RING, C2, C2))]
    scratch += [pltpu.VMEM(shape, F32) for shape in (
        (10, C3), (48, C1P), (SUB, C1P),
        (2, 3, MARGIN, TILE), (2, MARGIN, TILE), (3, MARGIN, C2), (3, 80, C3), (2, MARGIN, 1024),
        (LANE, LANE), (3072, LANE), (SIDE, SUB, TILE), (SIDE, SUB, LANE), (SIDE, SUB, LANE))]
    scratch += [dma(shape) for shape in ((3,), (RING,), (SIDE,), (SIDE,), (2,), (SIDE,), (10, 2), (10, 2), (SIDE,), (SIDE,))]
    return pl.pallas_call(
        kernel,
        out_shape=jax.ShapeDtypeStruct((W3, SIDE, W3), F32),
        in_specs=[vmem] * 13 + [hbm] * 11,
        out_specs=vmem,
        scratch_shapes=scratch,
        compiler_params=pltpu.CompilerParams(collective_id=0, has_side_effects=True, vmem_limit_bytes=67043328),
        name="unet",
    )(x, w_e1a, w_head, *rest)


def solution(mesh):
    tile_spec = P(("data", "row"), "col", None)

    def device_body(tile, *params):
        (w_enc1a, b_enc1a, w_enc1b, b_enc1b, w_enc2a, b_enc2a, w_enc2b, b_enc2b,
         w_mid_a, b_mid_a, w_mid_b, b_mid_b, w_up2, w_dec2a, b_dec2a, w_dec2b, b_dec2b,
         w_up1, w_dec1a, b_dec1a, w_dec1b, b_dec1b, w_head, b_head) = params
        biases = (b_enc1a, b_enc1b, b_enc2a, b_enc2b, b_mid_a, b_mid_b, b_dec2a, b_dec2b, b_dec1a, b_dec1b)

        def taps(weight):
            return weight.reshape(-1, weight.shape[2], weight.shape[3])

        def turned(weight):
            return jnp.swapaxes(weight, 2, 3).reshape(-1, weight.shape[2])

        weights = [taps(w) for w in (w_enc1b, w_enc2a, w_enc2b, w_mid_a, w_mid_b, w_up2, w_dec2a, w_dec2b)]
        weights += [turned(w_up1), turned(w_dec1a), taps(w_dec1b)]
        packed = network(jnp.transpose(tile, (0, 2, 1)), taps(w_enc1a), w_head.T, *biases, *weights)
        return jnp.transpose(packed, (0, 2, 1)) + b_head

    def program(image, *params):
        mapped = jax.shard_map(device_body, mesh=mesh, in_specs=(tile_spec,) + tuple([P()] * len(params)), out_specs=tile_spec, check_vma=False)
        return mapped(image, *params)

    return program
```

```python
import jax
import jax.numpy as jnp
from jax import lax
from jax.experimental import pallas as pl
from jax.experimental.pallas import tpu as pltpu
from jax.sharding import PartitionSpec as P

F32 = jnp.float32
BF16 = jnp.bfloat16
STRIPS = 16
LAST = STRIPS - 1
SIDE = 4
SUB, LANE = 8, 128
TILE, HALF = 2 * LANE, LANE // 2
C1, C2, C3, C1P = 320, 640, 1280, 384
W3 = 32
END = SUB + TILE
MARGIN = END + SUB
TAPS = range(3)
PAIR = range(2)
QUAD = range(SIDE)
TAP9 = 9
RING = 47
E2B, MA, MB, UP2, D2A, D2B, UP1, D1A, UNITS = 0, 9, 27, 63, 71, 89, 98, 100, 105
ROWS = (1, 0, 2)
NOT = jnp.logical_not
AND = jnp.logical_and
OR = jnp.logical_or
MESH_ID = pl.DeviceIdType.MESH


def dot(lhs, rhs):
    return jnp.dot(lhs, rhs, preferred_element_type=F32)


def relu(value):
    return jnp.maximum(value, 0.0)


def dot_t(lhs, rhs):
    return lax.dot_general(lhs, rhs, (((1,), (1,)), ((), ())), preferred_element_type=F32)


def cat_lanes(parts):
    return jnp.concatenate(list(parts), axis=1)


def cat_rows(parts):
    return jnp.concatenate(list(parts), axis=0)


def turn(value, amount=HALF):
    return value if amount == 0 else pltpu.roll(value, amount, 1)


def lane_mask(shape, below):
    return lax.broadcasted_iota(jnp.int32, shape, 1) < below


def column_index(rows, width):
    return lax.rem(lax.broadcasted_iota(jnp.int32, (rows, LANE), 0), width)


def kernel(x_ref, w_e1a, w_head, *refs):
    biases, refs = refs[:10], refs[10:]
    (h_e1b, h_e2a, h_e2b, h_ma, h_mb, h_up2, h_d2a, h_d2b, h_up1, h_d1a, h_d1b,
     out_ref,
     xrows, xs, xb, xh, z, act1, cat1, p1, act2, s2, p2, act3, mid, u2, act4, d2, act5,
     v_e1b, v_e2a, t_e1b, ring, bias, w_first, w_out,
     pm, pt, pl2, pl3, pd1, pool, up_f32, ys, ysend, yrecv,
     sem_w, sem_r, x_send, x_recv, h_send, h_recv, e_send, e_recv, y_send, y_recv) = refs
    col = lax.axis_index("col")
    row = lax.axis_index("row")
    data = lax.axis_index("data")

    def owner(strip):
        strip_col = strip // 4
        k = strip % 4
        return strip_col, k + (strip_col % 2) * (3 - 2 * k)

    def device(strip_col, strip_row):
        return (data, strip_col, strip_row)

    k_me = row + (col % 2) * (3 - 2 * row)
    me = 4 * col + k_me

    barrier = pltpu.get_barrier_semaphore()
    for strip in range(1, STRIPS):
        other_col, other_row = owner((me + strip) % STRIPS)
        pl.semaphore_signal(barrier, inc=1, device_id=device(other_col, other_row), device_id_type=MESH_ID)

    def whole(src, dst, index):
        return pltpu.make_async_copy(src, dst, sem_w.at[index])

    cp_e1b = whole(h_e1b, v_e1b, 0)
    cp_e2a = whole(h_e2a, v_e2a, 1)
    cp_d1b = whole(h_d1b, v_e1b, 2)

    def half(index):
        return pl.ds((index % 2) * C2, C2)

    def unit(index):
        slot = index % RING
        dst = ring.at[slot]
        if index < MA:
            src = h_e2b.at[(index % 3) * 3 + index // 3]
        elif index < MB:
            tap = (index - MA) // 2
            src = h_ma.at[ROWS[tap // 3] * 3 + tap % 3, :, half(index - MA)]
        elif index < UP2:
            local = index - MB
            tap = local // 4
            src = h_mb.at[ROWS[tap // 3] * 3 + tap % 3, half(local // 2), half(local)]
        elif index < D2A:
            local = index - UP2
            src = h_up2.at[local // 2, half(local)]
        elif index < D2B:
            local = (index - D2A) % TAP9
            src = h_d2a.at[(local % 3) * 3 + local // 3, half((D2B - 1 - index) // TAP9)]
        elif index < UP1:
            local = index - D2B
            src = h_d2b.at[(local % 3) * 3 + local // 3]
        elif index < D1A:
            src = h_up1.at[pl.ds((index - UP1) * C2, C2)]
        elif index < UNITS - 1:
            src = h_d1a.at[pl.ds((index - D1A) * C2, C2)]
        else:
            src = h_d1a.at[pl.ds((index - D1A) * C2, C1)]
            dst = ring.at[slot, pl.ds(0, C1)]
        return pltpu.make_async_copy(src, dst, sem_r.at[slot])

    def wait_units(first, last):
        for index in range(first, last):
            unit(index).wait()

    def refill(done):
        for index in range(done[0] + RING, min(done[1] + RING, UNITS)):
            unit(index).start()

    cp_e1b.start()
    cp_e2a.start()
    for index in range(MA):
        unit(index).start()

    bias[...] = jnp.zeros_like(bias)
    for index, ref in enumerate(biases):
        bias[index:index + 1, :ref.shape[0]] = ref[...].reshape(1, ref.shape[0])
    w_first[...] = jnp.zeros_like(w_first)
    for tap in range(TAP9):
        at = (tap // 3) * STRIPS + (tap % 3) * SIDE
        w_first[at:at + SIDE, :C1] = w_e1a[tap].astype(F32)
    w_out[...] = jnp.zeros_like(w_out)
    w_out[:SIDE, :C1] = w_head[...].astype(F32)

    xrows[...] = jnp.zeros_like(xrows)
    xrows[2:2 + W3, :SIDE, :W3] = x_ref[...].astype(F32)

    def pack(group, carry):
        packed = jnp.zeros((SUB, LANE), F32)
        for j in range(SUB):
            line = turn(xrows[group * SUB + j], (j % SIDE) * W3)
            packed = packed + (line if j < SIDE else pltpu.roll(line, SIDE, 0))
        xs[pl.ds(group, 1)] = packed[None]
        return carry

    lax.fori_loop(0, 5, pack, 0)
    pl.semaphore_wait(barrier, LAST)

    def build_tail(weights, base, tail):
        def body(dy, carry):
            parts = [weights[dy * 3 + dx, base:base + C1, TILE:C1].astype(F32) for dx in TAPS]
            zero = jnp.zeros((C1, HALF), F32)
            pair = cat_lanes(parts[:2])
            last = cat_lanes([parts[2], zero])
            tail[dy, :, :LANE] = pair.astype(BF16)
            tail[dy, :, LANE:TILE] = last.astype(BF16)
            return carry

        lax.fori_loop(0, 3, body, 0)


    def is_me(strip_col, strip_row):
        return AND(strip_col == col, strip_row == row)

    def remote(src, dst, send, recv, strip_col, strip_row):
        return pltpu.make_async_remote_copy(src_ref=src, dst_ref=dst, send_sem=send, recv_sem=recv,
                                            device_id=device(strip_col, strip_row), device_id_type=MESH_ID)

    for k in QUAD:
        to_col, to_row = owner(4 * row + k)
        here = is_me(to_col, to_row)
        copy = remote(xs.at[pl.ds(k, 2)], xb.at[col], x_send.at[k], x_recv.at[col], to_col, to_row)

        @pl.when(NOT(here))
        def _():
            copy.start()

        @pl.when(here)
        def _():
            xb[pl.ds(col, 1)] = xs[k:k + 2][None]

    def halo_target(strip):
        return owner(jnp.clip(strip, 0, LAST))

    for side, (strip, allowed, first) in enumerate(((4 * row - 1, row > 0, 0), (4 * row + 4, row < 3, SIDE))):
        to_col, to_row = halo_target(strip)
        here = is_me(to_col, to_row)
        copy = remote(xs.at[pl.ds(first, 1)], xh.at[col], h_send.at[side], h_recv.at[col], to_col, to_row)

        @pl.when(AND(allowed, NOT(here)))
        def _():
            copy.start()

        @pl.when(AND(allowed, here))
        def _():
            xh[pl.ds(col, 1)] = xs[first:first + 1][None]

    cp_e1b.wait()
    build_tail(v_e1b, 0, t_e1b)
    for index in range(MA, RING):
        unit(index).start()

    for c in QUAD:
        @pl.when(NOT(is_me(c, row) & (row == col)))
        def _():
            remote(xs.at[pl.ds(0, 2)], xb.at[c], x_send.at[0], x_recv.at[c], col, row).wait_recv()

    has_top = AND(k_me == 0, col > 0)
    has_bottom = AND(k_me == 3, col < 3)
    halo_row = jnp.where(has_top, col - 1, col + 1)
    for c in QUAD:
        own = AND(c == col, row == halo_row)

        @pl.when(AND(OR(has_top, has_bottom), NOT(own)))
        def _():
            remote(xs.at[pl.ds(0, 1)], xh.at[c], h_send.at[0], h_recv.at[c], col, row).wait_recv()

    for k in QUAD:
        to_col, to_row = owner(4 * row + k)

        @pl.when(NOT(is_me(to_col, to_row)))
        def _():
            remote(xs.at[pl.ds(k, 2)], xb.at[col], x_send.at[k], x_recv.at[col], to_col, to_row).wait_send()

    for side, (strip, allowed, first) in enumerate(((4 * row - 1, row > 0, 0), (4 * row + 4, row < 3, SIDE))):
        to_col, to_row = halo_target(strip)

        @pl.when(AND(allowed, NOT(is_me(to_col, to_row))))
        def _():
            remote(xs.at[pl.ds(first, 1)], xh.at[col], h_send.at[side], h_recv.at[col], to_col, to_row).wait_send()

    lanes8 = lax.broadcasted_iota(jnp.int32, (SUB, LANE), 1)
    sub8 = lax.broadcasted_iota(jnp.int32, (SUB, LANE), 0)
    z[...] = jnp.zeros_like(z)
    halo_place = (AND(has_top, lanes8 < HALF), AND(has_bottom, lanes8 >= HALF))
    for part in PAIR:
        place = AND(halo_place[part], sub8 < SIDE)
        blocks = [jnp.where(place, xh[c, 0], xb[c, part]) for c in QUAD]
        for group in QUAD:
            line = jnp.zeros((SUB, LANE), F32)
            for c in QUAD:
                inside = lanes8 // W3 == c
                line = jnp.where(inside, turn(blocks[c], (W3 * (c - group)) % LANE), line)
            for dx in TAPS:
                moved = line
                if dx == 0:
                    moved = jnp.where(lanes8 == 0, 0.0, turn(line, 1))
                elif dx == 2:
                    moved = jnp.where(lanes8 == LANE - 1, 0.0, turn(line, LANE - 1))
                for upper in range(2 - part):
                    at = (part * SUB + group + upper * SIDE) * STRIPS + dx * SIDE
                    z[at:at + SIDE, :] = moved[upper * SIDE:upper * SIDE + SIDE]

    def first_conv(pair, carry):
        weights = w_first[...].astype(BF16)
        for j in (2 * pair, 2 * pair + 1):
            taps = z[pl.ds(pl.multiple_of(j * STRIPS, STRIPS), 48), :].astype(BF16)
            value = lax.dot_general(taps, weights, (((0,), (0,)), ((), ())), preferred_element_type=F32)
            value = relu(value + bias[:1, :C1P])
            outside = OR(AND(me == 0, j == 0), AND(me == LAST, j == TAP9))
            value = jnp.where(outside, 0.0, value)
            act1[pl.ds(pl.multiple_of(j * LANE, LANE), LANE), :] = value.astype(BF16)
        return carry

    lax.fori_loop(0, 5, first_conv, 0)

    up_col, up_row = owner(jnp.maximum(me - 1, 0))
    down_col, down_row = owner(jnp.minimum(me + 1, LAST))

    def clear_borders(ref, width, height):
        @pl.when(me == 0)
        def _():
            ref[:width, :] = jnp.zeros((width, ref.shape[1]), BF16)

        @pl.when(me == LAST)
        def _():
            ref[(height + 1) * width:(height + 2) * width, :] = jnp.zeros((width, ref.shape[1]), BF16)

    for ref, width, height in ((cat1, LANE, SUB), (act5, LANE, SUB), (p1, HALF, SIDE), (act2, HALF, SIDE), (s2, HALF, SIDE),
                               (u2, HALF, SIDE), (act4, HALF, SIDE), (p2, W3, 2), (act3, W3, 2)):
        clear_borders(ref, width, height)

    def halo_copies(ref, width, height, index, lanes):
        to_up = remote(ref.at[pl.ds(width, width), lanes], ref.at[pl.ds((height + 1) * width, width), lanes],
                       e_send.at[index, 0], e_recv.at[index, 0], up_col, up_row)
        to_down = remote(ref.at[pl.ds(height * width, width), lanes], ref.at[pl.ds(0, width), lanes],
                         e_send.at[index, 1], e_recv.at[index, 1], down_col, down_row)
        return to_up, to_down

    odd = k_me % 2 == 1
    even = NOT(odd)
    far = (k_me % 2) * 3
    near = 3 - far
    ANY = (True, True)
    FAR = (even, odd)
    NEAR = (odd, even)

    def halo_start(ref, width, height, index, lanes=slice(None), sides=ANY):
        to_up, to_down = halo_copies(ref, width, height, index, lanes)

        @pl.when(AND(me > 0, sides[0]))
        def _():
            to_up.start()

        @pl.when(AND(me < LAST, sides[1]))
        def _():
            to_down.start()

    def halo_wait(ref, width, height, index, lanes=slice(None), sides=ANY):
        to_up, to_down = halo_copies(ref, width, height, index, lanes)

        @pl.when(AND(me > 0, sides[0]))
        def _():
            to_down.wait_recv()
            to_up.wait_send()

        @pl.when(AND(me < LAST, sides[1]))
        def _():
            to_up.wait_recv()
            to_down.wait_send()

    def narrow_lhs(ref, start, rows, width):
        mains = [ref[pl.ds(start + dy * width, rows), :TILE] for dy in TAPS]
        tails = [ref[pl.ds(start + dy * width, rows), TILE:C1P] for dy in TAPS]
        pair = (tails[0].astype(F32) + turn(tails[1].astype(F32))).astype(BF16)
        return cat_lanes(mains + [pair, tails[2][:, :HALF]])

    def narrow_rhs(load):
        return cat_rows([load(dy, 0, TILE) for dy in TAPS] + [load(dy, TILE, C1) for dy in TAPS])

    x_index = column_index(TILE, LANE)
    not_first = x_index > 0
    not_last = x_index < 127

    low_half = lane_mask((TILE, LANE), HALF)

    def shifted(ref, plane, left, right):
        first = left + jnp.where(not_first, ref[plane(0) + (slice(7, 263), right[0])], 0.0)
        return first + jnp.where(not_last, ref[plane(2) + (slice(9, 265), right[1])], 0.0)

    def scaled(i, step):
        return i * step if isinstance(i, int) else pl.multiple_of(i * step, step)

    def blocks_of(block):
        return slice(block * LANE, block * LANE + LANE)

    def conv_narrow(ref, bias_row, finish, chunks):
        for side, i in enumerate(chunks):
            left = narrow_lhs(ref, scaled(i, TILE), TILE, LANE)
            for dx in TAPS:
                pm[side, dx, SUB:END, :] = dot(left, narrow_rhs(lambda dy, a, b: v_e1b[dy * 3 + dx, a:b, :TILE]))
            pt[side, SUB:END, :] = dot(left, narrow_rhs(lambda dy, a, b: t_e1b[dy, a:b, :]))
        for side, i in enumerate(chunks):
            pieces = []
            for block in PAIR:
                lanes = blocks_of(block)
                value = shifted(pm, lambda dx: (side, dx), pm[side, 1, SUB:END, lanes], (lanes, lanes))
                pieces.append(relu(value + bias[bias_row:bias_row + 1, lanes]))
            value = shifted(pt, lambda dx: (side,), turn(pt[side, SUB:END, :LANE]), (blocks_of(0), blocks_of(1)))
            value = relu(value + bias[bias_row:bias_row + 1, TILE:C1P])
            pieces.append(jnp.where(low_half, value, 0.0))
            finish(i, pieces)

    def conv_cat(bias_row, finish, chunks):
        for side, i in enumerate(chunks):
            start = scaled(i, TILE)
            left = cat_lanes(cat1[pl.ds(start + dy * LANE, TILE), :] for dy in TAPS)
            right = cat_lanes(cat_rows(d1a_tap(dy * 3 + dx) for dx in TAPS) for dy in TAPS)
            pd1[side, SUB:END, :3 * C1] = dot_t(left, right)
        for side, i in enumerate(chunks):
            turned = [turn(pd1[side, SUB:END, blocks_of(2 + block)]) for block in TAPS]
            pieces = []
            for block in TAPS:
                middle = turned[block] if block == 2 else jnp.where(low_half, turned[block], turned[block + 1])
                value = shifted(pd1, lambda dx: (side,), middle, (blocks_of(block), blocks_of(5 + block) if block < 2 else slice(896, 1024)))
                value = relu(value + bias[bias_row:bias_row + 1, blocks_of(block)])
                pieces.append(value if block < 2 else jnp.where(low_half, value, 0.0))
            finish(i, pieces)

    def store_level1(ref):
        def finish(i, pieces):
            start = LANE + scaled(i, TILE)
            for block in range(3):
                ref[pl.ds(start, TILE), block * LANE:block * LANE + LANE] = pieces[block].astype(BF16)
        return finish

    def finish_s1(i, pieces):
        at = pl.ds(LANE + scaled(i, TILE), TILE)
        turned = [turn(piece) for piece in pieces]
        cat1[at, TILE:C1P] = jnp.where(low_half, 0.0, turned[0]).astype(BF16)
        for block in PAIR:
            cat1[at, blocks_of(3 + block)] = jnp.where(low_half, turned[block], turned[block + 1]).astype(BF16)
        start = HALF + scaled(i, HALF)
        for block in range(3):
            pool[:LANE, :] = jnp.maximum(pieces[block][:LANE], pieces[block][LANE:TILE])
            pooled = jnp.maximum(pool[pl.ds(0, HALF, stride=2), :], pool[pl.ds(1, HALF, stride=2), :])
            p1[pl.ds(start, HALF), block * LANE:block * LANE + LANE] = pooled.astype(BF16)

    S1_LANES = pl.ds(C1P, TILE)
    U1_LANES = pl.ds(0, C1P)
    conv_narrow(act1, 1, finish_s1, (far,))
    halo_start(p1, HALF, SIDE, 0, sides=FAR)
    conv_narrow(act1, 1, finish_s1, (near,))
    halo_start(p1, HALF, SIDE, 0, sides=NEAR)
    halo_start(cat1, LANE, SUB, 1, S1_LANES)
    conv_narrow(act1, 1, finish_s1, (1, 2))
    cp_d1b.start()

    x_index2 = column_index(TILE, HALF)
    not_first2 = x_index2 > 0
    not_last2 = x_index2 < 63

    def finish_level2(bias_row, store):
        def body(block, carry):
            lanes = pl.ds(pl.multiple_of(block * LANE, LANE), LANE)
            value = pl2[1, SUB:END, lanes] + jnp.where(not_first2, pl2[0, 7:263, lanes], 0.0)
            value = value + jnp.where(not_last2, pl2[2, 9:265, lanes], 0.0)
            store(lanes, relu(value + bias[bias_row:bias_row + 1, lanes]))
            return carry

        lax.fori_loop(0, 5, body, 0)

    def store_level2(ref, start):
        def store(lanes, value):
            ref[start:start + TILE, lanes] = value.astype(BF16)
        return store

    def store_s2(lanes, value):
        s2[HALF:C1, lanes] = value.astype(BF16)
        for i in PAIR:
            pool[:HALF, :] = jnp.maximum(value[LANE * i:LANE * i + HALF], value[LANE * i + HALF:LANE * i + LANE])
            pooled = jnp.maximum(pool[pl.ds(0, W3, stride=2), :], pool[pl.ds(1, W3, stride=2), :])
            p2[W3 + W3 * i:HALF + W3 * i, lanes] = pooled.astype(BF16)

    NTILES = ((0, TILE), (TILE, 2 * TILE), (2 * TILE, C2))
    TAIL = slice(2 * TILE, C2)

    def stack_rows(ref, rows, width, taps=TAPS):
        return cat_lanes(ref[dy * width:dy * width + rows, :] for dy in taps)

    def level2_taps(left, weights, add=False, groups=QUAD):
        if groups is not QUAD and left.shape[0] == TILE:
            left = cat_rows(left[group * HALF:group * HALF + HALF] for group in groups)

        def put(dx, lanes, value):
            if groups is QUAD:
                pl2[dx, SUB:END, lanes] = pl2[dx, SUB:END, lanes] + value if add else value
                return
            for part, group in enumerate(groups):
                at = slice(SUB + group * HALF, SUB + group * HALF + HALF)
                piece = value[part * HALF:part * HALF + HALF]
                pl2[dx, at, lanes] = pl2[dx, at, lanes] + piece if add else piece

        for dx in TAPS:
            for first, last in NTILES[:2]:
                lanes = slice(first, last)
                put(dx, lanes, dot(left, weights(dx, lanes)))
        pair = dot(left, cat_lanes(weights(dx, TAIL) for dx in PAIR))
        put(0, TAIL, pair[:, :LANE])
        put(1, TAIL, pair[:, LANE:])
        put(2, TAIL, dot(left, weights(2, TAIL)))

    def unit_rows(first, taps=TAPS):
        return lambda dx, lanes: cat_rows(ring[(first + dx * 3 + dy) % RING, :, lanes] for dy in taps)

    halo_wait(p1, HALF, 4, 0)
    cp_e2a.wait()

    def finish_groups(bias_row, ref, groups):
        def body(block, carry):
            lanes = pl.ds(pl.multiple_of(block * LANE, LANE), LANE)
            for group in groups:
                at = SUB + group * HALF
                value = pl2[1, at:at + HALF, lanes] + jnp.where(not_first2[:HALF], pl2[0, at - 1:at - 1 + HALF, lanes], 0.0)
                value = value + jnp.where(not_last2[:HALF], pl2[2, at + 1:at + 1 + HALF, lanes], 0.0)
                value = relu(value + bias[bias_row:bias_row + 1, lanes])
                ref[(group + 1) * HALF:(group + 2) * HALF, lanes] = value.astype(BF16)
            return carry

        lax.fori_loop(0, 5, body, 0)

    def edges_first(left, weights, add, bias_row, ref, index):
        for groups in ((0, 3), (1, 2)):
            level2_taps(left, weights, add, groups)
            finish_groups(bias_row, ref, groups)
            if 0 in groups:
                halo_start(ref, HALF, SIDE, index)

    edges_first(narrow_lhs(p1, 0, TILE, HALF),
                lambda dx, lanes: narrow_rhs(lambda dy, r0, r1: v_e2a[dy * 3 + dx, r0:r1, lanes]), False, 2, act2, 2)

    def conv640(ref, first, index, add=False, finish=None):
        level2_taps(ref[HALF:HALF + TILE, :], unit_rows(first, (1,)), add)
        if finish is None:
            inner = cat_lanes([ref[HALF:HALF + LANE, :], ref[3 * HALF:3 * HALF + LANE, :]])
            level2_taps(inner, unit_rows(first, (0, 2)), True, (1, 2))
        halo_wait(ref, HALF, SIDE, index)
        left = stack_rows(ref, TILE, HALF, (0, 2))
        if finish is None:
            level2_taps(left, unit_rows(first, (0, 2)), True, (0, 3))
        else:
            edges_first(left, unit_rows(first, (0, 2)), True, *finish)

    wait_units(E2B, MA)
    conv640(act2, E2B, 2)
    finish_level2(3, store_s2)
    halo_start(p2, W3, 2, 3)
    halo_start(s2, HALF, 4, 4)
    refill((E2B, MA))

    x_index3 = column_index(HALF, W3)
    not_first3 = x_index3 > 0
    not_last3 = x_index3 < 31

    def finish_level3(bias_row, ref, start):
        def body(block, carry):
            lanes = pl.ds(pl.multiple_of(block * LANE, LANE), LANE)
            value = pl3[1, SUB:72, lanes] + jnp.where(not_first3, pl3[0, 7:71, lanes], 0.0)
            value = value + jnp.where(not_last3, pl3[2, 9:73, lanes], 0.0)
            ref[start:start + HALF, lanes] = relu(value + bias[bias_row:bias_row + 1, lanes]).astype(BF16)
            return carry

        lax.fori_loop(0, 10, body, 0)

    def slot_of(index):
        return index % RING

    def wide(first):
        return cat_lanes([ring[slot_of(first)], ring[slot_of(first + 1)]])

    def add_rows(dx, value):
        pl3[dx, SUB:72, :] = pl3[dx, SUB:72, :] + value

    wait_units(MA, MB)
    for dx in TAPS:
        pl3[dx, SUB:72, :] = dot(p2[W3:3 * W3, :], wide(MA + 2 * dx))
    cp_d1b.wait()
    build_tail(v_e1b, 0, t_e1b)
    halo_wait(p2, W3, 2, 3)
    left = cat_lanes([p2[:HALF, :], p2[HALF:LANE, :]])
    for dx in TAPS:
        add_rows(dx, dot(left, cat_rows([wide(MA + 6 + 2 * dx), wide(MA + 12 + 2 * dx)])))
    finish_level3(4, act3, W3)
    halo_start(act3, W3, 2, 5)
    refill((MA, MB))

    for group, dy in enumerate(ROWS):
        if group == 1:
            halo_wait(act3, W3, 2, 5)
        begin = MB + group * 12
        wait_units(begin, begin + 12)
        left = act3[dy * W3:dy * W3 + HALF, :]
        for dx in TAPS:
            first = begin + dx * SIDE
            value = dot(left, cat_rows([wide(first), wide(first + 2)]))
            if group:
                add_rows(dx, value)
            else:
                pl3[dx, SUB:72, :] = value
        refill((begin, begin + 12))
    finish_level3(5, mid, 0)

    wait_units(UP2, D2A)
    for tap in QUAD:
        p, q = tap // 2, tap % 2
        left = mid[...]
        for a, b in NTILES:
            right = cat_rows(ring[(UP2 + 2 * tap + part) % RING, :, a:b] for part in PAIR)
            part = dot(left, right)
            for i in PAIR:
                for c0 in range(a, b, LANE):
                    up_f32[pl.ds(c0 * 2 + (2 * i + p) * HALF + q, W3, stride=2), :] = part[W3 * i:W3 * i + W3, c0 - a:c0 - a + LANE]
    for block in range(5):
        u2[HALF:C1, block * LANE:block * LANE + LANE] = up_f32[block * TILE:block * TILE + TILE, :].astype(BF16)
    halo_start(u2, HALF, 4, 6)
    refill((UP2, D2A))
    halo_wait(s2, HALF, SIDE, 4)

    wait_units(D2A, D2A + TAP9)
    level2_taps(stack_rows(s2, TILE, HALF), unit_rows(D2A))
    refill((D2A, D2A + TAP9))
    wait_units(D2A + TAP9, D2B)
    conv640(u2, D2A + TAP9, 6, True, (6, act4, 7))
    refill((D2A + TAP9, D2B))
    wait_units(D2B, UP1)
    conv640(act4, D2B, 7)
    finish_level2(7, store_level2(d2, 0))

    def half1(tap):
        return slice((tap % 2) * C1, (tap % 2) * C1 + C1)

    refill((D2B, UP1))
    wait_units(UP1, D1A)
    for tap in QUAD:
        p, q = tap // 2, tap % 2
        left = d2[...]
        up = dot_t(left, ring[(UP1 + tap // 2) % RING, half1(tap), :])
        for a, b in ((0, TILE), (TILE, C1)):
            part = up[:, a:b]
            for i in QUAD:
                for c0 in range(a, b, LANE):
                    c1 = min(b, c0 + LANE)
                    up_f32[pl.ds(c0 * SUB + (2 * i + p) * LANE + q, HALF, stride=2), :c1 - c0] = part[HALF * i:HALF * i + HALF, c0 - a:c1 - a]
    for block in TAPS:
        value = up_f32[block * 1024:block * 1024 + 1024, :].astype(BF16)
        if block < 2:
            cat1[LANE:TILE + 7 * LANE, blocks_of(block)] = value
        else:
            cat1[LANE:TILE + 7 * LANE, TILE:C1] = value[:, :HALF]
    halo_start(cat1, LANE, SUB, 8, U1_LANES)

    def d1a_tap(tap):
        return ring[(D1A + tap // 2) % RING, half1(tap), :]

    wait_units(D1A, UNITS)
    conv_cat(8, store_level1(act5), (1, 2))
    halo_wait(cat1, LANE, SUB, 1, S1_LANES)
    halo_wait(cat1, LANE, SUB, 8, U1_LANES, NEAR)
    conv_cat(8, store_level1(act5), (near,))
    halo_start(act5, LANE, SUB, TAP9, sides=NEAR)
    halo_wait(cat1, LANE, SUB, 8, U1_LANES, FAR)
    conv_cat(8, store_level1(act5), (far,))
    halo_start(act5, LANE, SUB, TAP9, sides=FAR)

    def finish_head(i, pieces):
        head = dot_t(w_out[...].astype(BF16), cat_lanes(piece.astype(BF16) for piece in pieces))
        ys[pl.ds(i, 1)] = head[None]

    conv_narrow(act5, TAP9, finish_head, (1, 2))
    halo_wait(act5, LANE, SUB, TAP9, sides=NEAR)
    conv_narrow(act5, TAP9, finish_head, (near,))
    halo_wait(act5, LANE, SUB, TAP9, sides=FAR)
    conv_narrow(act5, TAP9, finish_head, (far,))

    for c in QUAD:
        packed = jnp.zeros((SUB, LANE), F32)
        for y in range(SUB):
            line = ys[y // 2, :, (y % 2) * LANE:(y % 2) * LANE + LANE]
            slot = y % 4
            shift = (W3 * slot - W3 * c) % LANE
            line = turn(line, shift)
            if y >= 4:
                line = pltpu.roll(line, 4, 0)
            place = AND(AND(lanes8 >= W3 * slot, lanes8 < W3 * slot + W3), (sub8 >= 4) if y >= 4 else (sub8 < 4))
            packed = jnp.where(place, line, packed)
        ysend[c] = packed

    def y_copy(c):
        return remote(ysend.at[c], yrecv.at[k_me], y_send.at[c], y_recv.at[k_me], c, col)

    for c in QUAD:
        here = is_me(c, col)

        @pl.when(NOT(here))
        def _():
            y_copy(c).start()

        @pl.when(here)
        def _():
            yrecv[pl.ds(k_me, 1)] = ysend[c][None]

    for k in QUAD:
        from_col, from_row = owner(4 * row + k)

        @pl.when(NOT(is_me(from_col, from_row)))
        def _():
            remote(ysend.at[0], yrecv.at[k], y_send.at[0], y_recv.at[k], col, row).wait_recv()

    for c in QUAD:
        @pl.when(NOT(is_me(c, col)))
        def _():
            y_copy(c).wait_send()

    for k in QUAD:
        for low in QUAD:
            line = turn(yrecv[k], (LANE - low * W3) % LANE)
            for high in PAIR:
                out_ref[k * SUB + high * SIDE + low] = line[high * SIDE:high * SIDE + SIDE, :W3]


def network(x, w_e1a, w_head, *rest):
    vmem = pl.BlockSpec(memory_space=pltpu.VMEM)
    hbm = pl.BlockSpec(memory_space=pl.ANY)
    dma = pltpu.SemaphoreType.DMA
    scratch = [pltpu.VMEM(shape, F32) for shape in ((5 * SUB, SUB, LANE), (5, SUB, LANE), (SIDE, 2, SUB, LANE), (SIDE, 1, SUB, LANE), (TILE, LANE))]
    level1, level2 = 10 * LANE, 6 * HALF
    scratch += [pltpu.VMEM(shape, BF16) for shape in (
        (level1, C1P), (level1, C2), (level2, C1P), (level2, C2), (level2, C2), (LANE, C2), (LANE, C3), (HALF, C3),
        (level2, C2), (level2, C2), (TILE, C2), (level1, C1P),
        (TAP9, C1, C1), (TAP9, C1, C2), (3, C1, TILE), (RING, C2, C2))]
    scratch += [pltpu.VMEM(shape, F32) for shape in (
        (10, C3), (48, C1P), (SUB, C1P),
        (2, 3, MARGIN, TILE), (2, MARGIN, TILE), (3, MARGIN, C2), (3, 80, C3), (2, MARGIN, 1024),
        (LANE, LANE), (3072, LANE), (SIDE, SUB, TILE), (SIDE, SUB, LANE), (SIDE, SUB, LANE))]
    scratch += [dma(shape) for shape in ((3,), (RING,), (SIDE,), (SIDE,), (2,), (SIDE,), (10, 2), (10, 2), (SIDE,), (SIDE,))]
    return pl.pallas_call(
        kernel,
        out_shape=jax.ShapeDtypeStruct((W3, SIDE, W3), F32),
        in_specs=[vmem] * 13 + [hbm] * 11,
        out_specs=vmem,
        scratch_shapes=scratch,
        compiler_params=pltpu.CompilerParams(collective_id=0, has_side_effects=True, vmem_limit_bytes=67043328),
        name="unet",
    )(x, w_e1a, w_head, *rest)


def solution(mesh):
    tile_spec = P(("data", "row"), "col", None)

    def device_body(tile, *params):
        (w_enc1a, b_enc1a, w_enc1b, b_enc1b, w_enc2a, b_enc2a, w_enc2b, b_enc2b,
         w_mid_a, b_mid_a, w_mid_b, b_mid_b, w_up2, w_dec2a, b_dec2a, w_dec2b, b_dec2b,
         w_up1, w_dec1a, b_dec1a, w_dec1b, b_dec1b, w_head, b_head) = params
        biases = (b_enc1a, b_enc1b, b_enc2a, b_enc2b, b_mid_a, b_mid_b, b_dec2a, b_dec2b, b_dec1a, b_dec1b)

        def taps(weight):
            return weight.reshape(-1, weight.shape[2], weight.shape[3])

        def turned(weight):
            return jnp.swapaxes(weight, 2, 3).reshape(-1, weight.shape[2])

        weights = [taps(w) for w in (w_enc1b, w_enc2a, w_enc2b, w_mid_a, w_mid_b, w_up2, w_dec2a, w_dec2b)]
        weights += [turned(w_up1), turned(w_dec1a), taps(w_dec1b)]
        packed = network(jnp.transpose(tile, (0, 2, 1)), taps(w_enc1a), w_head.T, *biases, *weights)
        return jnp.transpose(packed, (0, 2, 1)) + b_head

    def program(image, *params):
        mapped = jax.shard_map(device_body, mesh=mesh, in_specs=(tile_spec,) + tuple([P()] * len(params)), out_specs=tile_spec, check_vma=False)
        return mapped(image, *params)

    return program
```
